256 devices in a mesh: fft: 32 (over x_lo, z, core), scal: 8 (over x_hi, y).
Axes of the slice: x: 4 (x_hi: 2, x_lo: 2; x = x_hi * 2 + x_lo), y: 4, z: 8, core: 2. Of those that a mesh axis runs over, the one named last changes fastest.
Arguments:
- scalar_state: float32 [8, 2, 256, 256, 128], P('scal', None, 'fft'), may hold values from -12 to 12
- velocity: bfloat16 [3, 256, 256, 256], P(None, 'fft', 'scal'), may hold values from -6 to 6
- species: int32 [8], P('scal'), may hold values from 0 to 63
- kappa_table: float32 [64], replicated, may hold values from 0.1 to 1
- dealias_bound: int32 [8], P('scal'), may hold values from 64 to 85
Outputs:
- new_state: float32 [8, 2, 256, 256, 128], P('scal', None, 'fft')
- kappa: float32 [8], P('scal')
The draws below stay inside these ranges and needn't reach their ends.
All inputs are finite; a program needn't handle non-finite values.
Results may differ from the reference program's by a relative error of at most 0.0027.
Values may be sent and summed in bfloat16 or wider, within the bound.
No kernel may reach another device: no remote copies, remote signals or barrier semaphores. Data moves between devices by JAX's collectives and lax.ppermute only.
A program may use at most 128 MiB of HBM per device.

```python
import math
import jax
import jax.numpy as jnp
from jax import lax

N = 256
SPECIES = 64
SCALARS = 8


def draw_scalar_state(key, part):
    dims_shape = (SCALARS, 2, N, N, N // 2)
    key_base, key_rough, key_scale = jax.random.split(key, 3)
    values = jnp.clip(jax.random.normal(key_base, dims_shape, jnp.float32), -4.0, 4.0)
    roughness = jnp.exp(jax.random.uniform(key_rough, dims_shape, jnp.float32, math.log(0.5), math.log(1.5)))
    ky_float = jnp.arange(N, dtype=jnp.int32).astype(jnp.float32)
    envelope = jnp.sqrt(1.0 + 2.0 * ky_float / (N - 1)).reshape(1, 1, N, 1, 1)
    scalar_scale = jnp.exp(jax.random.uniform(key_scale, (SCALARS, 1, 1, 1, 1), jnp.float32, math.log(0.5), math.log(2.0)))
    return jnp.clip(values * roughness * envelope * scalar_scale, -12.0, 12.0).astype(jnp.float32)


def plant(result, rng, low, largest):
    longest = result.shape.index(max(result.shape))
    spots = []
    for shift in (0, 1):
        where = [jax.random.randint(jax.random.fold_in(rng, axis), (), 0, length) for axis, length in enumerate(result.shape)]
        where[longest] = (where[longest] + shift) % result.shape[longest]
        spots.append(tuple(where))
    return result.at[spots[0]].set(low).at[spots[1]].set(largest)


def steps_of(rng, extent, pieces, least, high):
    loudness, own = 1.0, jax.random.fold_in(rng, 6)
    for position, parts in pieces:
        draws = jnp.exp(jax.random.uniform(jax.random.fold_in(own, position), (parts,), jnp.float32, least / len(pieces), high / len(pieces)))
        loudness = loudness * jnp.repeat(draws, extent[position] // parts).reshape([-1 if axis == position else 1 for axis in range(len(extent))])
    return loudness


def normal_values(key, dims, spread, most, cuts=(), held_as=jnp.bfloat16):
    drawn = jax.random.normal(key, dims, jnp.float32) * spread
    if len(cuts) > 0:
        drawn = steps_of(key, dims, cuts, -0.22, 0.18) * drawn
    return jnp.clip(drawn, min=-most, max=most).astype(held_as)


def setup_inputs(seed: int = 0) -> dict:
    keys = jax.random.split(jax.random.key(seed), 6)
    return {
        "scalar_state": draw_scalar_state(jax.random.fold_in(keys[5], 71), 0),
        "velocity": normal_values(keys[1], (3, N, N, N), 1.0, 6.0, ((1, 32), (2, 8))),
        "species": plant(jax.random.randint(keys[2], (SCALARS,), 0, SPECIES), jax.random.fold_in(keys[2], 1), 0, SPECIES - 1).astype(jnp.int32),
        "kappa_table": jnp.clip(jnp.exp(jax.random.uniform(keys[3], (SPECIES,), jnp.float32, math.log(0.1), math.log(1.0))), 0.1, 1.0),
        "dealias_bound": plant(jax.random.randint(keys[4], (SCALARS,), N // 4, N // 3 + 1), jax.random.fold_in(keys[4], 1), N // 4, (N // 3 + 1) - 1).astype(jnp.int32),
    }


cfl_number = 0.2

def twiddle(size_in, size_out, length):
    row_index = jnp.arange(size_in, dtype=jnp.int32)[:, None]
    col_index = jnp.arange(size_out, dtype=jnp.int32)[None, :]
    angles = (row_index * col_index % length).astype(jnp.float32) * (2.0 * math.pi / length)
    norming = 1.0 / math.sqrt(length)
    return (jnp.cos(angles) * norming, jnp.sin(angles) * norming)

def build_tables(length):
    half_len = length // 2
    full_cos, full_sin = twiddle(length, length, length)
    inv_cos, inv_sin = twiddle(half_len, length, length)
    weight = jnp.where(jnp.arange(half_len, dtype=jnp.int32) == 0, 1.0, 2.0).astype(jnp.float32)[:, None]
    fwd_cos, fwd_sin = twiddle(length, half_len, length)
    listed = (full_cos, full_sin, inv_cos * weight, inv_sin * weight, fwd_cos, fwd_sin)
    return tuple((matrix.astype(jnp.bfloat16) for matrix in listed))

def product(formula, operand, matrix):
    return jnp.einsum(formula, operand.astype(jnp.float32), matrix.astype(jnp.float32), precision=lax.Precision.HIGHEST)

def complex_section(real_part, imag_part, cos_matrix, sin_matrix, formula, inverse):
    real_cos = product(formula, real_part, cos_matrix)
    real_sin = product(formula, real_part, sin_matrix)
    imag_cos = product(formula, imag_part, cos_matrix)
    imag_sin = product(formula, imag_part, sin_matrix)
    if inverse:
        return (real_cos - imag_sin, real_sin + imag_cos)
    return (real_cos + imag_sin, imag_cos - real_sin)

def reference(scalar_state, velocity, species, kappa_table, dealias_bound):
    scalar_count = scalar_state.shape[0]
    table_count = kappa_table.shape[0]
    length = scalar_state.shape[2]
    half_len = length // 2
    full_cos, full_sin, inv_cos, inv_sin, fwd_cos, fwd_sin = build_tables(length)
    index_full = jnp.arange(length, dtype=jnp.int32)
    signed = jnp.where(index_full < half_len, index_full, index_full - length).astype(jnp.float32)
    ky_wave = signed[:, None, None]
    kz_wave = signed[None, :, None]
    kx_wave = jnp.arange(half_len, dtype=jnp.int32).astype(jnp.float32)[None, None, :]
    ksquare = kx_wave * kx_wave + ky_wave * ky_wave + kz_wave * kz_wave
    weight = jnp.where(kx_wave == 0.0, 1.0, 2.0).astype(jnp.float32)
    cell_count = float(length) ** 3
    step_size = cfl_number * 2.0 * math.pi / length

    def z_inverse(real_part, imag_part):
        z_section = complex_section(real_part, imag_part, full_cos, full_sin, 'ykx,kz->yzx', True)
        return (z_section[0].astype(jnp.bfloat16), z_section[1].astype(jnp.bfloat16))

    def rest_inverse(real_part, imag_part):
        y_section = complex_section(real_part, imag_part, full_cos, full_sin, 'yzx,yw->zwx', True)
        y_real = y_section[0].astype(jnp.bfloat16)
        y_imag = y_section[1].astype(jnp.bfloat16)
        return product('zwk,kx->zwx', y_real, inv_cos) - product('zwk,kx->zwx', y_imag, inv_sin)

    def gradient_set(real_part, imag_part):
        whole_real, whole_imag = z_inverse(real_part.astype(jnp.bfloat16), imag_part.astype(jnp.bfloat16))
        deriv_real, deriv_imag = z_inverse((-kz_wave * imag_part).astype(jnp.bfloat16), (kz_wave * real_part).astype(jnp.bfloat16))
        results = []
        for wavenumber in (kx_wave, ky_wave):
            grad_real = (-wavenumber * whole_imag.astype(jnp.float32)).astype(jnp.bfloat16)
            grad_imag = (wavenumber * whole_real.astype(jnp.float32)).astype(jnp.bfloat16)
            results.append(rest_inverse(grad_real, grad_imag))
        results.append(rest_inverse(deriv_real, deriv_imag))
        return results

    def advect(gradients):
        total = velocity[0].astype(jnp.float32) * gradients[0]
        total = total + velocity[1].astype(jnp.float32) * gradients[1]
        total = total + velocity[2].astype(jnp.float32) * gradients[2]
        return total.astype(jnp.bfloat16)

    def forward_field(physical):
        real_x = product('zyx,xk->zyk', physical, fwd_cos).astype(jnp.bfloat16)
        imag_x = (-product('zyx,xk->zyk', physical, fwd_sin)).astype(jnp.bfloat16)
        y_section = complex_section(real_x, imag_x, full_cos, full_sin, 'zyk,yw->wzk', False)
        y_real = y_section[0].astype(jnp.bfloat16)
        y_imag = y_section[1].astype(jnp.bfloat16)
        return complex_section(y_real, y_imag, full_cos, full_sin, 'wzk,zv->wvk', False)
    updated_list = []
    kappa_list = []
    for scalar in range(scalar_count):
        start_real = scalar_state[scalar, 0]
        start_imag = scalar_state[scalar, 1]
        energy = start_real * start_real + start_imag * start_imag
        variance = jnp.sum(weight * energy) / cell_count
        mean_grad = jnp.sum(weight * ksquare * energy) / cell_count
        gradients = gradient_set(start_real, start_imag)
        peak_value = jnp.max(jnp.sqrt(gradients[0] * gradients[0] + gradients[1] * gradients[1] + gradients[2] * gradients[2]))
        base_kappa = jnp.sum(jnp.where(species[scalar] == jnp.arange(table_count, dtype=jnp.int32), kappa_table, 0.0))
        kappa_value = base_kappa * peak_value * jnp.sqrt(variance) / (mean_grad + 1e-06)
        factor = jnp.exp(-kappa_value * ksquare * step_size)
        bound = dealias_bound[scalar].astype(jnp.float32)
        dealias_mask = (ksquare <= bound * bound).astype(jnp.float32)
        first_real, first_imag = forward_field(advect(gradients))
        first_real = -dealias_mask * first_real
        first_imag = -dealias_mask * first_imag
        mid_real = factor * (start_real + step_size * first_real)
        mid_imag = factor * (start_imag + step_size * first_imag)
        second_real, second_imag = forward_field(advect(gradient_set(mid_real, mid_imag)))
        second_real = -dealias_mask * second_real
        second_imag = -dealias_mask * second_imag
        new_real = factor * start_real + 0.5 * step_size * (factor * first_real + second_real)
        new_imag = factor * start_imag + 0.5 * step_size * (factor * first_imag + second_imag)
        updated_list.append(jnp.stack([new_real, new_imag]))
        kappa_list.append(kappa_value)
    return (jnp.stack(updated_list), jnp.stack(kappa_list))
```

```python
import math

import jax
import jax.numpy as jnp
import numpy as np
from jax import lax
from jax.experimental import pallas as pl
from jax.experimental.pallas import tpu as pltpu
from jax.sharding import PartitionSpec as P

N = 256
HALF = 128
PEERS = 32
ROWS = N // PEERS
GROUP = 4
KEPT = 96
LIMIT = 86
PACKED = ROWS * KEPT
PITCH = 2 * N + 8
STEP = 0.2 * 2.0 * math.pi / N
CELLS = float(N) ** 3
F32 = jnp.float32
BF16 = jnp.bfloat16


def tables():
    index = np.arange(N)
    angles = (index[:, None] * index[None, :] % N).astype(np.float32) * np.float32(2.0 * math.pi / N)
    cos = np.cos(angles) * np.float32(1.0 / math.sqrt(N))
    sin = np.sin(angles) * np.float32(1.0 / math.sqrt(N))
    weight = np.where(np.arange(HALF) == 0, 1.0, 2.0).astype(np.float32)[:, None]
    inverse = np.block([[cos, -sin], [sin, cos]])
    forward = np.block([[cos, sin], [-sin, cos]])
    order = np.arange(2 * N).reshape(2, PEERS, ROWS).transpose(1, 0, 2).reshape(-1)
    x_inv = np.concatenate([-weight * sin[:HALF], -weight * cos[:HALF]], axis=0)
    keep = (np.arange(HALF) < LIMIT).astype(np.float32)[None, :]
    x_fwd = np.concatenate([cos[:, :HALF] * keep, -sin[:, :HALF] * keep], axis=1)
    listed = {
        "z_inv": inverse,
        "y_inv": inverse[:, order],
        "x_inv": x_inv,
        "x_fwd": x_fwd,
        "y_fwd": forward[order, :],
        "z_fwd": forward[:, order],
    }
    return {name: jnp.asarray(value.astype(np.float32)).astype(BF16) for name, value in listed.items()}


def dot(left, right):
    return jnp.dot(left, right, preferred_element_type=F32)


def iota(shape, dim):
    return lax.broadcasted_iota(jnp.int32, shape, dim)


def signed(index):
    return jnp.where(index < HALF, index, index - N).astype(F32)


def z_rows(real_part, imag_part, kz_wave):
    both = jnp.concatenate([real_part, imag_part], axis=0)
    waves = jnp.concatenate([kz_wave, kz_wave], axis=0)
    return jnp.concatenate([both.astype(BF16), (waves * both).astype(BF16)], axis=1)


def send_planes(out_ref, whole_ref, deriv_ref):
    def one_peer(peer, carry):
        for local in range(ROWS):
            for at, ref in ((0, whole_ref), (HALF, deriv_ref)):
                start = peer * ROWS + local
                real_part = ref[pl.ds(start, ROWS, stride=PITCH), :]
                imag_part = ref[pl.ds(start + N, ROWS, stride=PITCH), :]
                tile = jnp.concatenate([real_part, imag_part], axis=0).astype(BF16)
                out_ref[peer, local, :, at : at + HALF] = tile
        return carry

    lax.fori_loop(0, PEERS, one_peer, 0)


def z_inverse(local, rows, table_ref, whole_ref, deriv_ref):
    found = dot(table_ref[...], rows)
    start = pl.multiple_of(local * PITCH, 8)
    whole_ref[pl.ds(start, 2 * N), :] = found[:, :HALF]
    deriv_ref[pl.ds(start, 2 * N), :] = found[:, HALF:]


def waves_of(info_ref, local):
    ky_wave = signed(info_ref[0] + local)
    kz_wave = signed(iota((N, HALF), 0))
    kx_wave = iota((N, HALF), 1).astype(F32)
    return kz_wave, kx_wave * kx_wave + ky_wave * ky_wave + kz_wave * kz_wave


def start_kernel(info_ref, state_ref, table_ref, out_ref, stats_ref, whole_ref, deriv_ref):
    step = pl.program_id(0)

    @pl.when(step == 0)
    def _():
        stats_ref[...] = jnp.zeros_like(stats_ref)

    for pos in range(GROUP):
        local = step * GROUP + pos
        kz_wave, ksquare = waves_of(info_ref, local)
        real_part = state_ref[0, pos]
        imag_part = state_ref[1, pos]
        weight = jnp.where(iota((N, HALF), 1) == 0, 1.0, 2.0)
        energy = weight * (real_part * real_part + imag_part * imag_part)
        stats_ref[0] += jnp.sum(energy.reshape(N // 8, 8, HALF), axis=0)
        stats_ref[1] += jnp.sum((ksquare * energy).reshape(N // 8, 8, HALF), axis=0)
        z_inverse(local, z_rows(real_part, imag_part, kz_wave), table_ref, whole_ref, deriv_ref)

    @pl.when(step == pl.num_programs(0) - 1)
    def _():
        send_planes(out_ref, whole_ref, deriv_ref)


def in_three(value):
    high = value.astype(BF16).astype(F32)
    rest = value - high
    middle = rest.astype(BF16).astype(F32)
    return high, middle, (rest - middle).astype(BF16).astype(F32)


def packed_four(parts):
    lane = iota((2 * ROWS, HALF), 1)
    turned = [parts[0]] + [pltpu.roll(parts[k], HALF - 32 * k, 1) for k in (1, 2, 3)]
    return [jnp.where(lane < HALF - 32 * (k + 1), turned[k], turned[k + 1]) for k in (0, 1, 2)]


def unpacked_four(packed):
    lane = iota((2 * N, HALF), 1)
    first, second, third = (packed[:, k * HALF : (k + 1) * HALF] for k in (0, 1, 2))
    return [
        first,
        pltpu.roll(jnp.where(lane >= 96, first, second), 32, 1),
        pltpu.roll(jnp.where(lane >= 64, second, third), 64, 1),
        pltpu.roll(third, 96, 1),
    ]


def grid_kernel(
    planes_ref, speed_ref, stats_ref, y_inv_ref, x_inv_ref, x_fwd_ref, y_fwd_ref, out_ref, sums_ref, peak_ref
):
    step = pl.program_id(0)
    pair = planes_ref.shape[1]
    count = 2 * N

    @pl.when(step == 0)
    def _():
        peak_ref[...] = jnp.zeros_like(peak_ref)

    row = iota((count, HALF), 0)
    ky_wave = signed(row // (2 * ROWS) * ROWS + row % ROWS)
    kx_wave = iota((N, HALF), 1).astype(F32)
    came = [planes_ref[:, k].reshape(count, N) for k in range(pair)]
    scaled = [(ky_wave * part[:, :HALF].astype(F32)).astype(BF16) for part in came]
    y_section = dot(y_inv_ref[...], jnp.concatenate(came + scaled, axis=1))
    x_rows = []
    for k in range(pair):
        starts = (k * N, pair * N + k * HALF, k * N + HALF)
        for which, at in enumerate(starts):
            halves = [y_section[part * N : (part + 1) * N, at : at + HALF] for part in (0, 1)]
            if which == 0:
                halves = [kx_wave * half for half in halves]
            x_rows.append(jnp.concatenate(halves, axis=1).astype(BF16))
    gradients = dot(jnp.concatenate(x_rows, axis=0), x_inv_ref[...])
    fields = []
    for k in range(pair):
        parts = [gradients[(3 * k + d) * N : (3 * k + d + 1) * N] for d in range(3)]
        total = speed_ref[0, k].astype(F32) * parts[0]
        total = total + speed_ref[1, k].astype(F32) * parts[1]
        total = total + speed_ref[2, k].astype(F32) * parts[2]
        fields.append(total.astype(BF16))
        square = parts[0] * parts[0] + parts[1] * parts[1] + parts[2] * parts[2]
        peak_ref[...] = jnp.maximum(peak_ref[...], jnp.max(square.reshape(N // 8, 8, N), axis=0))
    x_section = dot(jnp.concatenate(fields, axis=0), x_fwd_ref[...]).astype(BF16)
    columns = []
    for k in range(pair):
        part = x_section[k * N : (k + 1) * N]
        columns.append(jnp.concatenate([part[:, :HALF], part[:, HALF:]], axis=0))
    sums = dot(y_fwd_ref[...], jnp.concatenate(columns, axis=1))
    for k in range(pair):
        start = pl.multiple_of((step * pair + k) * PITCH, 8)
        sums_ref[pl.ds(start, count), :] = sums[:, k * HALF : (k + 1) * HALF]

    @pl.when(step == pl.num_programs(0) - 1)
    def _():
        shape = (2 * ROWS, HALF)
        peak = jnp.sqrt(jnp.max(peak_ref[...], keepdims=True))
        pieces = []
        for value in (jnp.sum(stats_ref[0], keepdims=True), jnp.sum(stats_ref[1], keepdims=True), peak):
            pieces.extend(in_three(jnp.broadcast_to(value, shape)))
        line = jnp.zeros(shape, F32)
        for k, piece in enumerate(pieces):
            line = jnp.where((iota(shape, 0) == 0) & (iota(shape, 1) == LIMIT + k), piece, line)

        def one_peer(peer, carry):
            for group in range(ROWS // GROUP):
                parts = []
                for pos in range(GROUP):
                    start = peer * 2 * ROWS + group * GROUP + pos
                    real_part = sums_ref[pl.ds(start, ROWS, stride=PITCH), :]
                    imag_part = sums_ref[pl.ds(start + ROWS, ROWS, stride=PITCH), :]
                    parts.append(jnp.concatenate([real_part, imag_part], axis=0))
                if group == 0:
                    parts[0] = parts[0] + line
                for k, tile in enumerate(packed_four(parts)):
                    at = (group * 3 + k) * HALF
                    out_ref[peer, :, at : at + HALF] = tile.astype(BF16)
            return carry

        lax.fori_loop(0, PEERS, one_peer, 0)


def tendency(came_ref, table_ref):
    packed = dot(table_ref[...], came_ref[...].reshape(2 * N, GROUP * KEPT))
    return [(part[:N], part[N:]) for part in unpacked_four(packed)]


def middle_kernel(
    info_ref,
    came_ref,
    state_ref,
    base_ref,
    z_fwd_ref,
    z_inv_ref,
    out_ref,
    kept_ref,
    kappa_ref,
    whole_ref,
    deriv_ref,
):
    step = pl.program_id(0)

    @pl.when(step == 0)
    def _():
        shape = (PEERS, 2 * ROWS, HALF)
        found = jnp.where(iota(shape, 1) == 0, came_ref[:, :, :HALF].astype(F32), 0.0)
        lane = iota(shape, 2)

        def piece(which):
            low = LIMIT + 3 * which
            inside = jnp.where((lane >= low) & (lane < low + 3), found, 0.0)
            return jnp.sum(jnp.sum(inside, axis=1), axis=1, keepdims=True)

        def spread(value):
            return jnp.broadcast_to(value, (8, HALF))

        variance = spread(jnp.sum(piece(0), axis=0, keepdims=True)) / CELLS
        mean_grad = spread(jnp.sum(piece(1), axis=0, keepdims=True)) / CELLS
        peak = spread(jnp.max(piece(2), axis=0, keepdims=True))
        match = iota(base_ref.shape, 1) == info_ref[2]
        base = spread(jnp.sum(jnp.where(match, base_ref[...], 0.0), axis=1, keepdims=True))
        kappa_ref[...] = base * peak * jnp.sqrt(variance) / (mean_grad + 1e-06)

    kappa = kappa_ref[0:1, :]
    bound = (info_ref[1] * info_ref[1]).astype(F32)
    for pos, (sum_real, sum_imag) in enumerate(tendency(came_ref, z_fwd_ref)):
        local = step * GROUP + pos
        kz_wave, ksquare = waves_of(info_ref, local)
        factor = jnp.exp(-kappa * ksquare * STEP)
        inside = ksquare <= bound
        first = [jnp.where(inside, -part, 0.0) for part in (sum_real, sum_imag)]
        middle = []
        for part in (0, 1):
            start = state_ref[part, pos]
            middle.append(factor * (start + STEP * first[part]))
            kept_ref[part, pos] = factor * start + (0.5 * STEP) * (factor * first[part])
        z_inverse(local, z_rows(*middle, kz_wave), z_inv_ref, whole_ref, deriv_ref)

    @pl.when(step == pl.num_programs(0) - 1)
    def _():
        send_planes(out_ref, whole_ref, deriv_ref)


def final_kernel(info_ref, came_ref, kept_ref, z_fwd_ref, out_ref):
    step = pl.program_id(0)
    bound = (info_ref[1] * info_ref[1]).astype(F32)
    for pos, sums in enumerate(tendency(came_ref, z_fwd_ref)):
        _, ksquare = waves_of(info_ref, step * GROUP + pos)
        for part in (0, 1):
            second = jnp.where(ksquare <= bound, -sums[part], 0.0)
            out_ref[part, pos] = kept_ref[part, pos] + (0.5 * STEP) * second


def whole(shape):
    return pl.BlockSpec(shape, lambda step: (0,) * len(shape))


SCALARS = pl.BlockSpec(memory_space=pltpu.SMEM)
HELD = pl.BlockSpec((2, GROUP, N, HALF), lambda step: (0, step, 0, 0))
CAME = pl.BlockSpec((PEERS, 2 * ROWS, GROUP * KEPT), lambda step: (0, 0, step))
TABLE = whole((2 * N, 2 * N))
SMALL = whole((N, N))
PLANES = (PEERS, ROWS, 2 * ROWS, N)
PAIR = 2
STATE = (2, ROWS, N, HALF)


def params():
    return pltpu.CompilerParams(dimension_semantics=("arbitrary",))


def shaped(shape, dtype):
    return jax.ShapeDtypeStruct(shape, dtype)


def turned():
    return pltpu.VMEM((ROWS * PITCH, HALF), F32)


def gathered(velocity):
    groups = lax.axis_size("scal")
    me = lax.axis_index("scal")
    ring = 4

    def moved(x, change):
        return lax.ppermute(x, "scal", [(s, change(s)) for s in range(groups)])

    def beside(shift):
        return lambda s: s // ring * ring + (s + shift) % ring

    across = moved(velocity, lambda s: (s + ring) % groups)
    out = jnp.zeros((*velocity.shape[:2], N, N), velocity.dtype)
    high, low = me // ring, me % ring
    half = velocity.shape[1] // 2

    def placed(out, x, owner, first=0):
        return lax.dynamic_update_slice(out, x, (0, first, owner * x.shape[2], 0))

    for x, own in ((velocity, high), (across, 1 - high)):
        up = moved(x, beside(1))
        down = moved(x, beside(-1))
        far_up = moved(up[:, :half], beside(1))
        far_down = moved(down[:, half:], beside(-1))
        start = own * ring
        out = placed(out, x, start + low)
        out = placed(out, up, start + (low + ring - 1) % ring)
        out = placed(out, down, start + (low + 1) % ring)
        out = placed(out, far_up, start + (low + 2) % ring)
        out = placed(out, far_down, start + (low + 2) % ring, half)
    return out


def exchanged(x):
    return lax.all_to_all(x, "fft", 0, 0, tiled=True)


def body(scalar_state, velocity, species, kappa_table, dealias_bound):
    table = tables()
    state = scalar_state[0]
    ky_first = lax.axis_index("fft").astype(jnp.int32) * ROWS
    info = jnp.stack([ky_first, dealias_bound[0], species[0]])
    speeds = gathered(velocity)

    planes, stats = pl.pallas_call(
        start_kernel,
        grid=(ROWS // GROUP,),
        in_specs=[SCALARS, HELD, TABLE],
        out_specs=[whole(PLANES), whole((2, 8, HALF))],
        out_shape=[shaped(PLANES, BF16), shaped((2, 8, HALF), F32)],
        scratch_shapes=[turned(), turned()],
        compiler_params=params(),
        name="start",
    )(info, state, table["z_inv"])

    def grid_side(planes):
        sent = (PEERS, 2 * ROWS, PACKED)
        return pl.pallas_call(
            grid_kernel,
            grid=(ROWS // PAIR,),
            in_specs=[
                pl.BlockSpec((PEERS, PAIR, 2 * ROWS, N), lambda step: (0, step, 0, 0)),
                pl.BlockSpec((3, PAIR, N, N), lambda step: (0, step, 0, 0)),
                whole((2, 8, HALF)),
                TABLE,
                SMALL,
                SMALL,
                TABLE,
            ],
            out_specs=whole(sent),
            out_shape=shaped(sent, BF16),
            scratch_shapes=[turned(), pltpu.VMEM((8, N), F32)],
            compiler_params=params(),
            name="grid",
        )(planes, speeds, stats, table["y_inv"], table["x_inv"], table["x_fwd"], table["y_fwd"])

    came = exchanged(grid_side(exchanged(planes)))
    planes, kept, kappa = pl.pallas_call(
        middle_kernel,
        grid=(ROWS // GROUP,),
        in_specs=[SCALARS, CAME, HELD, whole((1, kappa_table.shape[0])), TABLE, TABLE],
        out_specs=[whole(PLANES), HELD, whole((8, HALF))],
        out_shape=[shaped(PLANES, BF16), shaped(STATE, F32), shaped((8, HALF), F32)],
        scratch_shapes=[turned(), turned()],
        compiler_params=params(),
        name="middle",
    )(info, came, state, kappa_table[None], table["z_fwd"], table["z_inv"])
    came = exchanged(grid_side(exchanged(planes)))
    updated = pl.pallas_call(
        final_kernel,
        grid=(ROWS // GROUP,),
        in_specs=[SCALARS, CAME, HELD, TABLE],
        out_specs=HELD,
        out_shape=shaped(STATE, F32),
        compiler_params=params(),
        name="final",
    )(info, came, kept, table["z_fwd"])
    return (updated[None], kappa[0, :1])


def solution(mesh):
    placed = (
        P("scal", None, "fft", None, None),
        P(None, "fft", "scal", None),
        P("scal"),
        P(),
        P("scal"),
    )
    return jax.shard_map(
        body,
        mesh=mesh,
        in_specs=placed,
        out_specs=(P("scal", None, "fft", None, None), P("scal")),
        check_vma=False,
    )
```

```python
import math

import jax
import jax.numpy as jnp
import numpy as np
from jax import lax
from jax.experimental import pallas as pl
from jax.experimental.pallas import tpu as pltpu
from jax.sharding import PartitionSpec as P

N = 256
HALF = 128
PEERS = 32
ROWS = N // PEERS
GROUP = 4
KEPT = 96
LIMIT = 86
PACKED = ROWS * KEPT
PITCH = 2 * N + 8
STEP = 0.2 * 2.0 * math.pi / N
CELLS = float(N) ** 3
F32 = jnp.float32
BF16 = jnp.bfloat16


def tables():
    index = np.arange(N)
    angles = (index[:, None] * index[None, :] % N).astype(np.float32) * np.float32(2.0 * math.pi / N)
    cos = np.cos(angles) * np.float32(1.0 / math.sqrt(N))
    sin = np.sin(angles) * np.float32(1.0 / math.sqrt(N))
    weight = np.where(np.arange(HALF) == 0, 1.0, 2.0).astype(np.float32)[:, None]
    inverse = np.block([[cos, -sin], [sin, cos]])
    forward = np.block([[cos, sin], [-sin, cos]])
    order = np.arange(2 * N).reshape(2, PEERS, ROWS).transpose(1, 0, 2).reshape(-1)
    x_inv = np.concatenate([-weight * sin[:HALF], -weight * cos[:HALF]], axis=0)
    keep = (np.arange(HALF) < LIMIT).astype(np.float32)[None, :]
    x_fwd = np.concatenate([cos[:, :HALF] * keep, -sin[:, :HALF] * keep], axis=1)
    listed = {
        "z_inv": inverse,
        "y_inv": inverse[:, order],
        "x_inv": x_inv,
        "x_fwd": x_fwd,
        "y_fwd": forward[order, :],
        "z_fwd": forward[:, order],
    }
    return {name: jnp.asarray(value.astype(np.float32)).astype(BF16) for name, value in listed.items()}


def dot(left, right):
    return jnp.dot(left, right, preferred_element_type=F32)


def iota(shape, dim):
    return lax.broadcasted_iota(jnp.int32, shape, dim)


def signed(index):
    return jnp.where(index < HALF, index, index - N).astype(F32)


def z_rows(real_part, imag_part, kz_wave):
    both = jnp.concatenate([real_part, imag_part], axis=0)
    waves = jnp.concatenate([kz_wave, kz_wave], axis=0)
    return jnp.concatenate([both.astype(BF16), (waves * both).astype(BF16)], axis=1)


def send_planes(out_ref, whole_ref, deriv_ref):
    def one_peer(peer, carry):
        for local in range(ROWS):
            for at, ref in ((0, whole_ref), (HALF, deriv_ref)):
                start = peer * ROWS + local
                real_part = ref[pl.ds(start, ROWS, stride=PITCH), :]
                imag_part = ref[pl.ds(start + N, ROWS, stride=PITCH), :]
                tile = jnp.concatenate([real_part, imag_part], axis=0).astype(BF16)
                out_ref[peer, local, :, at : at + HALF] = tile
        return carry

    lax.fori_loop(0, PEERS, one_peer, 0)


def z_inverse(local, rows, table_ref, whole_ref, deriv_ref):
    found = dot(table_ref[...], rows)
    start = pl.multiple_of(local * PITCH, 8)
    whole_ref[pl.ds(start, 2 * N), :] = found[:, :HALF]
    deriv_ref[pl.ds(start, 2 * N), :] = found[:, HALF:]


def waves_of(local):
    ky_wave = signed(lax.axis_index("fft").astype(jnp.int32) * ROWS + local)
    kz_wave = signed(iota((N, HALF), 0))
    kx_wave = iota((N, HALF), 1).astype(F32)
    return kz_wave, kx_wave * kx_wave + ky_wave * ky_wave + kz_wave * kz_wave


def start_kernel(state_ref, table_ref, out_ref, stats_ref, whole_ref, deriv_ref):
    step = pl.program_id(0)
    rows = state_ref.shape[1]

    @pl.when(step == 0)
    def _():
        stats_ref[...] = jnp.zeros_like(stats_ref)

    for pos in range(rows):
        local = step * rows + pos
        kz_wave, ksquare = waves_of(local)
        real_part = state_ref[0, pos]
        imag_part = state_ref[1, pos]
        weight = jnp.where(iota((N, HALF), 1) == 0, 1.0, 2.0)
        energy = weight * (real_part * real_part + imag_part * imag_part)
        stats_ref[0] += jnp.sum(energy.reshape(N // 8, 8, HALF), axis=0)
        stats_ref[1] += jnp.sum((ksquare * energy).reshape(N // 8, 8, HALF), axis=0)
        z_inverse(local, z_rows(real_part, imag_part, kz_wave), table_ref, whole_ref, deriv_ref)

    @pl.when(step == pl.num_programs(0) - 1)
    def _():
        send_planes(out_ref, whole_ref, deriv_ref)


def in_three(value):
    high = value.astype(BF16).astype(F32)
    rest = value - high
    middle = rest.astype(BF16).astype(F32)
    return high, middle, (rest - middle).astype(BF16).astype(F32)


def packed_four(parts):
    lane = iota((2 * ROWS, HALF), 1)
    turned = [parts[0]] + [pltpu.roll(parts[k], HALF - 32 * k, 1) for k in (1, 2, 3)]
    return [jnp.where(lane < HALF - 32 * (k + 1), turned[k], turned[k + 1]) for k in (0, 1, 2)]


def unpacked_four(packed):
    lane = iota((2 * N, HALF), 1)
    first, second, third = (packed[:, k * HALF : (k + 1) * HALF] for k in (0, 1, 2))
    return [
        first,
        pltpu.roll(jnp.where(lane >= 96, first, second), 32, 1),
        pltpu.roll(jnp.where(lane >= 64, second, third), 64, 1),
        pltpu.roll(third, 96, 1),
    ]


def grid_kernel(
    planes_ref, speed_ref, stats_ref, y_inv_ref, x_inv_ref, x_fwd_ref, y_fwd_ref, out_ref, sums_ref, peak_ref
):
    count = 2 * N
    peak_ref[...] = jnp.zeros_like(peak_ref)
    row = iota((count, HALF), 0)
    ky_wave = signed(row // (2 * ROWS) * ROWS + row % ROWS)
    kx_wave = iota((N, HALF), 1).astype(F32)

    def one_pair(step, carry):
        came = [planes_ref[:, step * PAIR + k].reshape(count, N) for k in range(PAIR)]
        scaled = [(ky_wave * part[:, :HALF].astype(F32)).astype(BF16) for part in came]
        y_section = dot(y_inv_ref[...], jnp.concatenate(came + scaled, axis=1))
        x_rows = []
        for k in range(PAIR):
            starts = (k * N, PAIR * N + k * HALF, k * N + HALF)
            for which, at in enumerate(starts):
                halves = [y_section[part * N : (part + 1) * N, at : at + HALF] for part in (0, 1)]
                if which == 0:
                    halves = [kx_wave * half for half in halves]
                x_rows.append(jnp.concatenate(halves, axis=1).astype(BF16))
        gradients = dot(jnp.concatenate(x_rows, axis=0), x_inv_ref[...])
        fields = []
        for k in range(PAIR):
            parts = [gradients[(3 * k + d) * N : (3 * k + d + 1) * N] for d in range(3)]
            total = speed_ref[0, step * PAIR + k].astype(F32) * parts[0]
            total = total + speed_ref[1, step * PAIR + k].astype(F32) * parts[1]
            total = total + speed_ref[2, step * PAIR + k].astype(F32) * parts[2]
            fields.append(total.astype(BF16))
            square = parts[0] * parts[0] + parts[1] * parts[1] + parts[2] * parts[2]
            peak_ref[...] = jnp.maximum(peak_ref[...], jnp.max(square.reshape(N // 8, 8, N), axis=0))
        x_section = dot(jnp.concatenate(fields, axis=0), x_fwd_ref[...]).astype(BF16)
        columns = []
        for k in range(PAIR):
            part = x_section[k * N : (k + 1) * N]
            columns.append(jnp.concatenate([part[:, :HALF], part[:, HALF:]], axis=0))
        sums = dot(y_fwd_ref[...], jnp.concatenate(columns, axis=1))
        for k in range(PAIR):
            start = pl.multiple_of((step * PAIR + k) * PITCH, 8)
            sums_ref[pl.ds(start, count), :] = sums[:, k * HALF : (k + 1) * HALF]
        return carry

    lax.fori_loop(0, ROWS // PAIR, one_pair, 0)
    shape = (2 * ROWS, HALF)
    peak = jnp.sqrt(jnp.max(peak_ref[...], keepdims=True))
    pieces = []
    for value in (jnp.sum(stats_ref[0], keepdims=True), jnp.sum(stats_ref[1], keepdims=True), peak):
        pieces.extend(in_three(jnp.broadcast_to(value, shape)))
    line = jnp.zeros(shape, F32)
    for k, piece in enumerate(pieces):
        line = jnp.where((iota(shape, 0) == 0) & (iota(shape, 1) == LIMIT + k), piece, line)

    def one_peer(peer, carry):
        for group in range(ROWS // GROUP):
            parts = []
            for pos in range(GROUP):
                start = peer * 2 * ROWS + group * GROUP + pos
                real_part = sums_ref[pl.ds(start, ROWS, stride=PITCH), :]
                imag_part = sums_ref[pl.ds(start + ROWS, ROWS, stride=PITCH), :]
                parts.append(jnp.concatenate([real_part, imag_part], axis=0))
            if group == 0:
                parts[0] = parts[0] + line
            for k, tile in enumerate(packed_four(parts)):
                at = (group * 3 + k) * HALF
                out_ref[peer, :, at : at + HALF] = tile.astype(BF16)
        return carry

    lax.fori_loop(0, PEERS, one_peer, 0)


def tendency(came_ref, table_ref, group):
    at = group * GROUP * KEPT
    packed = dot(table_ref[...], came_ref[:, :, at : at + GROUP * KEPT].reshape(2 * N, GROUP * KEPT))
    return [(part[:N], part[N:]) for part in unpacked_four(packed)]


def middle_kernel(
    bound_ref,
    species_ref,
    came_ref,
    state_ref,
    base_ref,
    z_fwd_ref,
    z_inv_ref,
    out_ref,
    kept_ref,
    kappa_ref,
    whole_ref,
    deriv_ref,
):
    shape = (PEERS, 2 * ROWS, HALF)
    found = jnp.where(iota(shape, 1) == 0, came_ref[:, :, :HALF].astype(F32), 0.0)
    lane = iota(shape, 2)

    def piece(which):
        low = LIMIT + 3 * which
        inside = jnp.where((lane >= low) & (lane < low + 3), found, 0.0)
        return jnp.sum(jnp.sum(inside, axis=1), axis=1, keepdims=True)

    def spread(value):
        return jnp.broadcast_to(value, (8, HALF))

    variance = spread(jnp.sum(piece(0), axis=0, keepdims=True)) / CELLS
    mean_grad = spread(jnp.sum(piece(1), axis=0, keepdims=True)) / CELLS
    peak = spread(jnp.max(piece(2), axis=0, keepdims=True))
    match = iota(base_ref.shape, 1) == species_ref[0]
    base = spread(jnp.sum(jnp.where(match, base_ref[...], 0.0), axis=1, keepdims=True))
    kappa_ref[...] = base * peak * jnp.sqrt(variance) / (mean_grad + 1e-06)
    kappa = kappa_ref[0:1, :]
    bound = (bound_ref[0] * bound_ref[0]).astype(F32)
    for group in range(ROWS // GROUP):
        for pos, (sum_real, sum_imag) in enumerate(tendency(came_ref, z_fwd_ref, group)):
            local = group * GROUP + pos
            kz_wave, ksquare = waves_of(local)
            factor = jnp.exp(-kappa * ksquare * STEP)
            inside = ksquare <= bound
            first = [jnp.where(inside, -part, 0.0) for part in (sum_real, sum_imag)]
            middle = []
            for part in (0, 1):
                start = state_ref[part, local]
                middle.append(factor * (start + STEP * first[part]))
                kept_ref[part, local] = factor * start + (0.5 * STEP) * (factor * first[part])
            z_inverse(local, z_rows(*middle, kz_wave), z_inv_ref, whole_ref, deriv_ref)
    send_planes(out_ref, whole_ref, deriv_ref)


def final_kernel(bound_ref, came_ref, kept_ref, z_fwd_ref, out_ref):
    bound = (bound_ref[0] * bound_ref[0]).astype(F32)
    for group in range(ROWS // GROUP):
        for pos, sums in enumerate(tendency(came_ref, z_fwd_ref, group)):
            local = group * GROUP + pos
            _, ksquare = waves_of(local)
            for part in (0, 1):
                second = jnp.where(ksquare <= bound, -sums[part], 0.0)
                out_ref[part, local] = kept_ref[part, local] + (0.5 * STEP) * second


SCALARS = pl.BlockSpec(memory_space=pltpu.SMEM)
NEAR = pl.BlockSpec(memory_space=pltpu.VMEM)
PLANES = (PEERS, ROWS, 2 * ROWS, N)
SENT = (PEERS, 2 * ROWS, PACKED)
STATE = (2, ROWS, N, HALF)
PAIR = 2
AHEAD = 2


def params(mebibytes):
    return pltpu.CompilerParams(vmem_limit_bytes=mebibytes * 2**20)


def shaped(shape, dtype):
    return jax.ShapeDtypeStruct(shape, dtype)


def near(x):
    return pltpu.with_memory_space_constraint(x, pltpu.VMEM)


def turned():
    return pltpu.VMEM((ROWS * PITCH, HALF), F32)


def gathered(velocity):
    groups = lax.axis_size("scal")
    me = lax.axis_index("scal")
    ring = 4

    def moved(x, change):
        return lax.ppermute(x, "scal", [(s, change(s)) for s in range(groups)])

    def beside(shift):
        return lambda s: s // ring * ring + (s + shift) % ring

    across = moved(velocity, lambda s: (s + ring) % groups)
    out = jnp.zeros((*velocity.shape[:2], N, N), velocity.dtype)
    high, low = me // ring, me % ring
    half = velocity.shape[1] // 2

    def placed(out, x, owner, first=0):
        return lax.dynamic_update_slice(out, x, (0, first, owner * x.shape[2], 0))

    for x, own in ((velocity, high), (across, 1 - high)):
        up = moved(x, beside(1))
        down = moved(x, beside(-1))
        far_up = moved(up[:, :half], beside(1))
        far_down = moved(down[:, half:], beside(-1))
        start = own * ring
        out = placed(out, x, start + low)
        out = placed(out, up, start + (low + ring - 1) % ring)
        out = placed(out, down, start + (low + 1) % ring)
        out = placed(out, far_up, start + (low + 2) % ring)
        out = placed(out, far_down, start + (low + 2) % ring, half)
    return out


def exchanged(x):
    return lax.all_to_all(x, "fft", 0, 0, tiled=True)


def start_call(state, table):
    return pl.pallas_call(
        start_kernel,
        grid=(ROWS // AHEAD,),
        in_specs=[pl.BlockSpec((2, AHEAD, N, HALF), lambda step: (0, step, 0, 0)), NEAR],
        out_specs=[NEAR, NEAR],
        out_shape=[pltpu.VMEM(PLANES, BF16), pltpu.VMEM((2, 8, HALF), F32)],
        scratch_shapes=[turned(), turned()],
        compiler_params=params(24),
        name="start",
    )(state, near(table["z_inv"]))


def grid_call(planes, speeds, stats, table):
    return pl.pallas_call(
        grid_kernel,
        in_specs=[NEAR] * 7,
        out_specs=NEAR,
        out_shape=pltpu.VMEM(SENT, BF16),
        scratch_shapes=[turned(), pltpu.VMEM((8, N), F32)],
        compiler_params=params(24),
        name="grid",
    )(
        *(near(x) for x in (planes, speeds, stats)),
        *(near(table[name]) for name in ("y_inv", "x_inv", "x_fwd", "y_fwd")),
    )


def middle_call(bound, species, came, state, kappa_table, table):
    return pl.pallas_call(
        middle_kernel,
        in_specs=[SCALARS, SCALARS] + [NEAR] * 5,
        out_specs=[NEAR] * 3,
        out_shape=[pltpu.VMEM(PLANES, BF16), pltpu.VMEM(STATE, F32), shaped((8, HALF), F32)],
        scratch_shapes=[turned(), turned()],
        compiler_params=params(24),
        name="middle",
    )(
        bound,
        species,
        near(came),
        near(state),
        kappa_table[None],
        near(table["z_fwd"]),
        near(table["z_inv"]),
    )


def final_call(bound, came, kept, table):
    return pl.pallas_call(
        final_kernel,
        in_specs=[SCALARS] + [NEAR] * 3,
        out_specs=NEAR,
        out_shape=shaped(STATE, F32),
        compiler_params=params(16),
        name="final",
    )(bound, near(came), near(kept), near(table["z_fwd"]))


def body(scalar_state, velocity, species, kappa_table, dealias_bound):
    table = tables()
    state = scalar_state[0]
    speeds = gathered(velocity)
    planes, stats = start_call(state, table)
    came = exchanged(grid_call(exchanged(planes), speeds, stats, table))
    planes, kept, kappa = middle_call(dealias_bound, species, came, state, kappa_table, table)
    came = exchanged(grid_call(exchanged(planes), speeds, stats, table))
    return (final_call(dealias_bound, came, kept, table)[None], kappa[0, :1])


def solution(mesh):
    placed = (
        P("scal", None, "fft", None, None),
        P(None, "fft", "scal", None),
        P("scal"),
        P(),
        P("scal"),
    )
    return jax.shard_map(
        body,
        mesh=mesh,
        in_specs=placed,
        out_specs=(P("scal", None, "fft", None, None), P("scal")),
        check_vma=False,
    )
```

```python
import math

import jax
import jax.numpy as jnp
import numpy as np
from jax import lax
from jax.experimental import pallas as pl
from jax.experimental.pallas import tpu as pltpu
from jax.sharding import PartitionSpec as P

N = 256
HALF = 128
PEERS = 32
ROWS = N // PEERS
GROUP = 4
KEPT = 96
LIMIT = 86
PACKED = ROWS * KEPT
PITCH = 2 * N + 8
STEP = 0.2 * 2.0 * math.pi / N
CELLS = float(N) ** 3
F32 = jnp.float32
BF16 = jnp.bfloat16


def tables():
    index = np.arange(N)
    angles = (index[:, None] * index[None, :] % N).astype(np.float32) * np.float32(2.0 * math.pi / N)
    cos = np.cos(angles) * np.float32(1.0 / math.sqrt(N))
    sin = np.sin(angles) * np.float32(1.0 / math.sqrt(N))
    weight = np.where(np.arange(HALF) == 0, 1.0, 2.0).astype(np.float32)[:, None]
    inverse = np.block([[cos, -sin], [sin, cos]])
    forward = np.block([[cos, sin], [-sin, cos]])
    order = np.arange(2 * N).reshape(2, PEERS, ROWS).transpose(1, 0, 2).reshape(-1)
    x_inv = np.concatenate([-weight * sin[:HALF], -weight * cos[:HALF]], axis=0)
    keep = (np.arange(HALF) < LIMIT).astype(np.float32)[None, :]
    x_fwd = np.concatenate([cos[:, :HALF] * keep, -sin[:, :HALF] * keep], axis=1)
    listed = {
        "z_inv": inverse,
        "y_inv": inverse[:, order],
        "x_inv": x_inv,
        "x_fwd": x_fwd,
        "y_fwd": forward[order, :],
        "z_fwd": forward[:, order],
    }
    return {name: jnp.asarray(value.astype(np.float32)).astype(BF16) for name, value in listed.items()}


def dot(left, right):
    return jnp.dot(left, right, preferred_element_type=F32)


def iota(shape, dim):
    return lax.broadcasted_iota(jnp.int32, shape, dim)


def signed(index):
    return jnp.where(index < HALF, index, index - N).astype(F32)


def z_rows(real_part, imag_part, kz_wave):
    both = jnp.concatenate([real_part, imag_part], axis=0)
    waves = jnp.concatenate([kz_wave, kz_wave], axis=0)
    return jnp.concatenate([both.astype(BF16), (waves * both).astype(BF16)], axis=1)


def send_planes(first, count, planes_ref, whole_ref, deriv_ref):
    def some_peers(step, carry):
        for turn in range(UNROLL):
            peer = first + step * UNROLL + turn
            for local in range(ROWS):
                for at, ref in ((0, whole_ref), (HALF, deriv_ref)):
                    start = peer * ROWS + local
                    real_part = ref[pl.ds(start, ROWS, stride=PITCH), :]
                    imag_part = ref[pl.ds(start + N, ROWS, stride=PITCH), :]
                    tile = jnp.concatenate([real_part, imag_part], axis=0).astype(BF16)
                    planes_ref[peer, local, :, at : at + HALF] = tile
        return carry

    lax.fori_loop(0, count // UNROLL, some_peers, 0)


def z_inverse(local, rows, table_ref, whole_ref, deriv_ref):
    found = dot(table_ref[...], rows)
    start = pl.multiple_of(local * PITCH, 8)
    whole_ref[pl.ds(start, 2 * N), :] = found[:, :HALF]
    deriv_ref[pl.ds(start, 2 * N), :] = found[:, HALF:]


def waves_of(local):
    ky_wave = signed(lax.axis_index("fft").astype(jnp.int32) * ROWS + local)
    kz_wave = signed(iota((N, HALF), 0))
    kx_wave = iota((N, HALF), 1).astype(F32)
    return kz_wave, kx_wave * kx_wave + ky_wave * ky_wave + kz_wave * kz_wave


def copy_of(source, target, sem):
    return pltpu.make_async_copy(source, target, sem)


def start_kernel(
    state_hbm, table_hbm, out_hbm, stats_ref, state_ref, table_ref, planes_ref, whole_ref, deriv_ref, in_sems, out_sems
):
    loads = [copy_of(table_hbm, table_ref, in_sems.at[ROWS])]
    loads += [copy_of(state_hbm.at[:, k], state_ref.at[:, k], in_sems.at[k]) for k in range(ROWS)]
    for load in loads:
        load.start()
    stats_ref[...] = jnp.zeros_like(stats_ref)
    loads[0].wait()

    def one_row(local, carry):
        copy_of(state_hbm.at[:, local], state_ref.at[:, local], in_sems.at[local]).wait()
        kz_wave, ksquare = waves_of(local)
        real_part = state_ref[0, local]
        imag_part = state_ref[1, local]
        weight = jnp.where(iota((N, HALF), 1) == 0, 1.0, 2.0)
        energy = weight * (real_part * real_part + imag_part * imag_part)
        stats_ref[0] += jnp.sum(energy.reshape(N // 8, 8, HALF), axis=0)
        stats_ref[1] += jnp.sum((ksquare * energy).reshape(N // 8, 8, HALF), axis=0)
        z_inverse(local, z_rows(real_part, imag_part, kz_wave), table_ref, whole_ref, deriv_ref)
        return carry

    lax.fori_loop(0, ROWS, one_row, 0, unroll=2)

    def leaving(k):
        part = pl.ds(k * CHUNK, CHUNK)
        return copy_of(planes_ref.at[part], out_hbm.at[part], out_sems.at[k])

    def one_chunk(k, carry):
        send_planes(k * CHUNK, CHUNK, planes_ref, whole_ref, deriv_ref)
        leaving(k).start()
        return carry

    lax.fori_loop(0, PEERS // CHUNK, one_chunk, 0)
    for k in range(PEERS // CHUNK):
        leaving(k).wait()


def in_three(value):
    high = value.astype(BF16).astype(F32)
    rest = value - high
    middle = rest.astype(BF16).astype(F32)
    return high, middle, (rest - middle).astype(BF16).astype(F32)


def packed_four(parts):
    lane = iota((2 * ROWS, HALF), 1)
    turned = [parts[0]] + [pltpu.roll(parts[k], HALF - 32 * k, 1) for k in (1, 2, 3)]
    return [jnp.where(lane < HALF - 32 * (k + 1), turned[k], turned[k + 1]) for k in (0, 1, 2)]


def unpacked_four(packed):
    lane = iota((2 * N, HALF), 1)
    first, second, third = (packed[:, k * HALF : (k + 1) * HALF] for k in (0, 1, 2))
    return [
        first,
        pltpu.roll(jnp.where(lane >= 96, first, second), 32, 1),
        pltpu.roll(jnp.where(lane >= 64, second, third), 64, 1),
        pltpu.roll(third, 96, 1),
    ]


def grid_kernel(
    scalars,
    planes_hbm,
    speed_ref,
    stats_ref,
    y_inv_hbm,
    x_inv_hbm,
    x_fwd_hbm,
    y_fwd_hbm,
    out_ref,
    y_inv_ref,
    x_inv_ref,
    x_fwd_ref,
    y_fwd_ref,
    sums_ref,
    peak_ref,
    sems,
    planes_ref=None,
    planes_sems=None,
):
    count = 2 * N

    def came_pair(step):
        part = pl.ds(step * PAIR, PAIR)
        return copy_of(planes_hbm.at[:, part], planes_ref.at[:, part], planes_sems.at[step])

    loads = [
        copy_of(source, target, sems.at[k])
        for k, (source, target) in enumerate(
            (
                (y_inv_hbm, y_inv_ref),
                (x_inv_hbm, x_inv_ref),
                (x_fwd_hbm, x_fwd_ref),
                (y_fwd_hbm, y_fwd_ref),
            )
        )
    ]
    far = planes_ref is not None
    loads[0].start()
    if far:
        came_pair(0).start()
    for load in loads[1:]:
        load.start()
    if far:
        for k in range(1, ROWS // PAIR):
            came_pair(k).start()
    else:
        planes_ref = planes_hbm
    peak_ref[...] = jnp.zeros_like(peak_ref)
    row = iota((count, HALF), 0)
    ky_wave = signed(row // (2 * ROWS) * ROWS + row % ROWS)
    kx_wave = iota((N, HALF), 1).astype(F32)

    def one_pair(step, carry):
        if far:
            came_pair(step).wait()
        came = [planes_ref[:, step * PAIR + k].reshape(count, N) for k in range(PAIR)]
        scaled = [(ky_wave * part[:, :HALF].astype(F32)).astype(BF16) for part in came]
        pl.when(step == 0)(loads[0].wait)
        y_section = dot(y_inv_ref[...], jnp.concatenate(came + scaled, axis=1))
        x_rows = []
        for k in range(PAIR):
            starts = (k * N, PAIR * N + k * HALF, k * N + HALF)
            for which, at in enumerate(starts):
                halves = [y_section[part * N : (part + 1) * N, at : at + HALF] for part in (0, 1)]
                if which == 0:
                    halves = [kx_wave * half for half in halves]
                x_rows.append(jnp.concatenate(halves, axis=1).astype(BF16))
        for load in loads[1:]:
            pl.when(step == 0)(load.wait)
        gradients = dot(jnp.concatenate(x_rows, axis=0), x_inv_ref[...])
        fields = []
        for k in range(PAIR):
            parts = [gradients[(3 * k + d) * N : (3 * k + d + 1) * N] for d in range(3)]
            total = speed_ref[0, step * PAIR + k].astype(F32) * parts[0]
            total = total + speed_ref[1, step * PAIR + k].astype(F32) * parts[1]
            total = total + speed_ref[2, step * PAIR + k].astype(F32) * parts[2]
            fields.append(total.astype(BF16))
            square = parts[0] * parts[0] + parts[1] * parts[1] + parts[2] * parts[2]
            peak_ref[...] = jnp.maximum(peak_ref[...], jnp.max(square.reshape(N // 8, 8, N), axis=0))
        x_section = dot(jnp.concatenate(fields, axis=0), x_fwd_ref[...]).astype(BF16)
        columns = []
        for k in range(PAIR):
            part = x_section[k * N : (k + 1) * N]
            columns.append(jnp.concatenate([part[:, :HALF], part[:, HALF:]], axis=0))
        sums = dot(y_fwd_ref[...], jnp.concatenate(columns, axis=1))
        for k in range(PAIR):
            start = pl.multiple_of((step * PAIR + k) * PITCH, 8)
            sums_ref[pl.ds(start, count), :] = sums[:, k * HALF : (k + 1) * HALF]
        return carry

    lax.fori_loop(0, ROWS // PAIR, one_pair, 0)
    shape = (2 * ROWS, HALF)
    peak = jnp.sqrt(jnp.max(peak_ref[...], keepdims=True))
    pieces = []
    for value in (jnp.sum(stats_ref[0], keepdims=True), jnp.sum(stats_ref[1], keepdims=True), peak):
        pieces.extend(in_three(jnp.broadcast_to(value, shape)))
    line = jnp.zeros(shape, F32)
    for k, piece in enumerate(pieces):
        line = jnp.where((iota(shape, 0) == 0) & (iota(shape, 1) == LIMIT + k), piece, line)

    def some_peers(step, carry):
        for turn in range(SENDS):
            peer = step * SENDS + turn
            for group in range(ROWS // GROUP):
                parts = []
                for pos in range(GROUP):
                    start = peer * 2 * ROWS + group * GROUP + pos
                    real_part = sums_ref[pl.ds(start, ROWS, stride=PITCH), :]
                    imag_part = sums_ref[pl.ds(start + ROWS, ROWS, stride=PITCH), :]
                    parts.append(jnp.concatenate([real_part, imag_part], axis=0))
                if group == 0:
                    parts[0] = parts[0] + line
                for k, tile in enumerate(packed_four(parts)):
                    at = (group * 3 + k) * HALF
                    out_ref[peer, :, at : at + HALF] = tile.astype(BF16)
        return carry

    lax.fori_loop(0, PEERS // SENDS, some_peers, 0)


def tendency(came_ref, table_ref, group):
    at = group * GROUP * KEPT
    packed = dot(table_ref[...], came_ref[:, :, at : at + GROUP * KEPT].reshape(2 * N, GROUP * KEPT))
    return [(part[:N], part[N:]) for part in unpacked_four(packed)]


def middle_kernel(
    bound_ref,
    species_ref,
    base_ref,
    came_ref,
    state_hbm,
    z_fwd_hbm,
    z_inv_hbm,
    out_ref,
    kept_hbm,
    kappa_ref,
    state_ref,
    z_fwd_ref,
    z_inv_ref,
    kept_ref,
    whole_ref,
    deriv_ref,
    in_sems,
    out_sems,
):
    loads = [
        copy_of(source, target, in_sems.at[k])
        for k, (source, target) in enumerate(
            ((z_fwd_hbm, z_fwd_ref), (state_hbm, state_ref), (z_inv_hbm, z_inv_ref))
        )
    ]
    for load in loads:
        load.start()
    shape = (PEERS, 2 * ROWS, HALF)
    found = jnp.where(iota(shape, 1) == 0, came_ref[:, :, :HALF].astype(F32), 0.0)
    lane = iota(shape, 2)

    def piece(which):
        low = LIMIT + 3 * which
        inside = jnp.where((lane >= low) & (lane < low + 3), found, 0.0)
        return jnp.sum(jnp.sum(inside, axis=1), axis=1, keepdims=True)

    def spread(value):
        return jnp.broadcast_to(value, (8, HALF))

    variance = spread(jnp.sum(piece(0), axis=0, keepdims=True)) / CELLS
    mean_grad = spread(jnp.sum(piece(1), axis=0, keepdims=True)) / CELLS
    peak = spread(jnp.max(piece(2), axis=0, keepdims=True))
    base = base_ref[species_ref[0]]
    found = base * peak * jnp.sqrt(variance) / (mean_grad + 1e-06)
    kappa_ref[0] = jnp.max(found)
    kappa = found[0:1, :]
    bound = (bound_ref[0] * bound_ref[0]).astype(F32)
    loads[0].wait()
    saves = []
    for group in range(ROWS // GROUP):
        parts = tendency(came_ref, z_fwd_ref, group)
        if group == 0:
            loads[1].wait()
        for pos, (sum_real, sum_imag) in enumerate(parts):
            local = group * GROUP + pos
            kz_wave, ksquare = waves_of(local)
            factor = jnp.exp(-kappa * ksquare * STEP)
            inside = ksquare <= bound
            first = [jnp.where(inside, -part, 0.0) for part in (sum_real, sum_imag)]
            middle = []
            for part in (0, 1):
                start = state_ref[part, local]
                middle.append(factor * (start + STEP * first[part]))
                kept_ref[part, local] = factor * start + (0.5 * STEP) * (factor * first[part])
            if local == 0:
                loads[2].wait()
            z_inverse(local, z_rows(*middle, kz_wave), z_inv_ref, whole_ref, deriv_ref)
        rows = pl.ds(group * GROUP, GROUP)
        saves.append(copy_of(kept_ref.at[:, rows], kept_hbm.at[:, rows], out_sems.at[group]))
        saves[-1].start()
    send_planes(0, PEERS, out_ref, whole_ref, deriv_ref)
    for save in saves:
        save.wait()


def final_kernel(bound_ref, came_ref, kept_hbm, z_fwd_hbm, out_hbm, kept_ref, z_fwd_ref, out_ref, in_sems, out_sems):
    loads = [copy_of(z_fwd_hbm, z_fwd_ref, in_sems.at[0]), copy_of(kept_hbm, kept_ref, in_sems.at[1])]
    for load in loads:
        load.start()
    bound = (bound_ref[0] * bound_ref[0]).astype(F32)
    loads[0].wait()
    saves = []
    for group in range(ROWS // GROUP):
        parts = tendency(came_ref, z_fwd_ref, group)
        if group == 0:
            loads[1].wait()
        for pos, sums in enumerate(parts):
            local = group * GROUP + pos
            _, ksquare = waves_of(local)
            for part in (0, 1):
                second = jnp.where(ksquare <= bound, -sums[part], 0.0)
                out_ref[part, local] = kept_ref[part, local] + (0.5 * STEP) * second
            saves.append(copy_of(out_ref.at[:, local], out_hbm.at[:, local], out_sems.at[local]))
            saves[-1].start()
    for save in saves:
        save.wait()


SCALARS = pl.BlockSpec(memory_space=pltpu.SMEM)
NEAR = pl.BlockSpec(memory_space=pltpu.VMEM)
FAR = pl.BlockSpec(memory_space=pltpu.HBM)
PLANES = (PEERS, ROWS, 2 * ROWS, N)
SENT = (PEERS, 2 * ROWS, PACKED)
STATE = (2, ROWS, N, HALF)
PAIR = 4
CHUNK = 8
UNROLL = 2
SENDS = 4


def params(mebibytes):
    return pltpu.CompilerParams(vmem_limit_bytes=mebibytes * 2**20)


def shaped(shape, dtype):
    return jax.ShapeDtypeStruct(shape, dtype)


def near(x):
    return pltpu.with_memory_space_constraint(x, pltpu.VMEM)


def far(x):
    return pltpu.with_memory_space_constraint(x, pltpu.HBM)


def sems(count):
    return pltpu.SemaphoreType.DMA((count,))


def turned():
    return pltpu.VMEM((ROWS * PITCH, HALF), F32)


BIG = pltpu.VMEM((2 * N, 2 * N), BF16)
SMALL = pltpu.VMEM((N, N), BF16)
HELD = pltpu.VMEM(STATE, F32)


def gathered(velocity):
    groups = lax.axis_size("scal")
    me = lax.axis_index("scal")
    ring = 4

    def moved(x, change):
        return lax.ppermute(x, "scal", [(s, change(s)) for s in range(groups)])

    def beside(shift):
        return lambda s: s // ring * ring + (s + shift) % ring

    across = moved(velocity, lambda s: (s + ring) % groups)
    out = jnp.zeros((*velocity.shape[:2], N, N), velocity.dtype)
    high, low = me // ring, me % ring
    half = velocity.shape[1] // 2

    def placed(out, x, owner, first=0):
        return lax.dynamic_update_slice(out, x, (0, first, owner * x.shape[2], 0))

    for x, own in ((velocity, high), (across, 1 - high)):
        up = moved(x, beside(1))
        down = moved(x, beside(-1))
        far_up = moved(up[:, :half], beside(1))
        far_down = moved(down[:, half:], beside(-1))
        start = own * ring
        out = placed(out, x, start + low)
        out = placed(out, up, start + (low + ring - 1) % ring)
        out = placed(out, down, start + (low + 1) % ring)
        out = placed(out, far_up, start + (low + 2) % ring)
        out = placed(out, far_down, start + (low + 2) % ring, half)
    return out


def exchanged(x):
    return lax.all_to_all(x, "fft", 0, 0, tiled=True)


def start_call(state, table):
    return pl.pallas_call(
        start_kernel,
        in_specs=[FAR, FAR],
        out_specs=[FAR, NEAR],
        out_shape=[pltpu.HBM(PLANES, BF16), pltpu.VMEM((2, 8, HALF), F32)],
        scratch_shapes=[HELD, BIG, pltpu.VMEM(PLANES, BF16), turned(), turned(), sems(ROWS + 1), sems(PEERS // CHUNK)],
        compiler_params=params(24),
        name="start",
    )(far(state), far(table["z_inv"]))


def grid_call(scalars, planes, speeds, stats, table, apart):
    scratch = [BIG, SMALL, SMALL, BIG, turned(), pltpu.VMEM((8, N), F32), sems(4)]
    if apart:
        scratch += [pltpu.VMEM(PLANES, BF16), sems(ROWS // PAIR)]
    return pl.pallas_call(
        grid_kernel,
        in_specs=[(SCALARS,) * len(scalars), FAR if apart else NEAR, NEAR, NEAR] + [FAR] * 4,
        out_specs=NEAR,
        out_shape=pltpu.VMEM(SENT, BF16),
        scratch_shapes=scratch,
        compiler_params=params(24),
        name="grid",
    )(
        scalars,
        far(planes) if apart else near(planes),
        near(speeds),
        near(stats),
        *(far(table[name]) for name in ("y_inv", "x_inv", "x_fwd", "y_fwd")),
    )


def middle_call(bound, species, kappa_table, came, state, table):
    return pl.pallas_call(
        middle_kernel,
        in_specs=[SCALARS] * 3 + [NEAR] + [FAR] * 3,
        out_specs=[NEAR, FAR, SCALARS],
        out_shape=[pltpu.VMEM(PLANES, BF16), pltpu.HBM(STATE, F32), shaped((1,), F32)],
        scratch_shapes=[HELD, BIG, BIG, HELD, turned(), turned(), sems(3), sems(ROWS // GROUP)],
        compiler_params=params(24),
        name="middle",
    )(bound, species, kappa_table, near(came), far(state), far(table["z_fwd"]), far(table["z_inv"]))


def final_call(bound, came, kept, table):
    return pl.pallas_call(
        final_kernel,
        in_specs=[SCALARS, NEAR, FAR, FAR],
        out_specs=FAR,
        out_shape=pltpu.HBM(STATE, F32),
        scratch_shapes=[HELD, BIG, HELD, sems(2), sems(ROWS)],
        compiler_params=params(24),
        name="final",
    )(bound, near(came), far(kept), far(table["z_fwd"]))


def body(scalar_state, velocity, species, kappa_table, dealias_bound):
    table = tables()
    state = scalar_state[0]
    speeds = gathered(velocity)
    planes, stats = start_call(state, table)
    scalars = (dealias_bound, species, kappa_table)
    came = exchanged(grid_call(scalars, exchanged(planes), speeds, stats, table, True))
    planes, kept, kappa = middle_call(dealias_bound, species, kappa_table, came, state, table)
    came = exchanged(grid_call((), exchanged(planes), speeds, stats, table, False))
    return (final_call(dealias_bound, came, kept, table)[None], kappa)


def solution(mesh):
    placed = (
        P("scal", None, "fft", None, None),
        P(None, "fft", "scal", None),
        P("scal"),
        P(),
        P("scal"),
    )
    return jax.shard_map(
        body,
        mesh=mesh,
        in_specs=placed,
        out_specs=(P("scal", None, "fft", None, None), P("scal")),
        check_vma=False,
    )
```

```python
import math

import jax
import jax.numpy as jnp
import numpy as np
from jax import lax
from jax.experimental import pallas as pl
from jax.experimental.pallas import tpu as pltpu
from jax.sharding import PartitionSpec as P

N = 256
HALF = 128
PEERS = 32
ROWS = N // PEERS
GROUP = 4
KEPT = 96
LIMIT = 86
PACKED = ROWS * KEPT
PITCH = 2 * N + 8
STEP = 0.2 * 2.0 * math.pi / N
CELLS = float(N) ** 3
F32 = jnp.float32
BF16 = jnp.bfloat16


def tables():
    index = np.arange(N)
    angles = (index[:, None] * index[None, :] % N).astype(np.float32) * np.float32(2.0 * math.pi / N)
    cos = np.cos(angles) * np.float32(1.0 / math.sqrt(N))
    sin = np.sin(angles) * np.float32(1.0 / math.sqrt(N))
    weight = np.where(np.arange(HALF) == 0, 1.0, 2.0).astype(np.float32)[:, None]
    inverse = np.block([[cos, -sin], [sin, cos]])
    forward = np.block([[cos, sin], [-sin, cos]])
    order = np.arange(2 * N).reshape(2, PEERS, ROWS).transpose(1, 0, 2).reshape(-1)
    x_inv = np.concatenate([-weight * sin[:HALF], -weight * cos[:HALF]], axis=0)
    keep = (np.arange(HALF) < LIMIT).astype(np.float32)[None, :]
    x_fwd = np.concatenate([cos[:, :HALF] * keep, -sin[:, :HALF] * keep], axis=1)
    listed = {
        "z_inv": inverse,
        "y_inv": inverse[:, order],
        "x_inv": x_inv,
        "x_fwd": x_fwd,
        "y_fwd": forward[order, :],
        "z_fwd": forward[:, order],
    }
    return {name: jnp.asarray(value.astype(np.float32)).astype(BF16) for name, value in listed.items()}


def dot(left, right):
    return jnp.dot(left, right, preferred_element_type=F32)


def iota(shape, dim):
    return lax.broadcasted_iota(jnp.int32, shape, dim)


def signed(index):
    return jnp.where(index < HALF, index, index - N).astype(F32)


def z_rows(real_part, imag_part, kz_wave):
    both = jnp.concatenate([real_part, imag_part], axis=0)
    waves = jnp.concatenate([kz_wave, kz_wave], axis=0)
    return jnp.concatenate([both.astype(BF16), (waves * both).astype(BF16)], axis=1)


def send_planes(first, count, planes_ref, whole_ref, deriv_ref):
    def some_peers(step, carry):
        for turn in range(UNROLL):
            peer = first + step * UNROLL + turn
            for local in range(ROWS):
                for at, ref in ((0, whole_ref), (HALF, deriv_ref)):
                    start = peer * ROWS + local
                    real_part = ref[pl.ds(start, ROWS, stride=PITCH), :]
                    imag_part = ref[pl.ds(start + N, ROWS, stride=PITCH), :]
                    tile = jnp.concatenate([real_part, imag_part], axis=0).astype(BF16)
                    planes_ref[peer, local, :, at : at + HALF] = tile
        return carry

    lax.fori_loop(0, count // UNROLL, some_peers, 0)


def z_inverse(local, rows, table_ref, whole_ref, deriv_ref):
    found = dot(table_ref[...], rows)
    start = pl.multiple_of(local * PITCH, 8)
    whole_ref[pl.ds(start, 2 * N), :] = found[:, :HALF]
    deriv_ref[pl.ds(start, 2 * N), :] = found[:, HALF:]


def waves_of(local):
    ky_wave = signed(lax.axis_index("fft").astype(jnp.int32) * ROWS + local)
    kz_wave = signed(iota((N, HALF), 0))
    kx_wave = iota((N, HALF), 1).astype(F32)
    return kz_wave, kx_wave * kx_wave + ky_wave * ky_wave + kz_wave * kz_wave


def copy_of(source, target, sem):
    return pltpu.make_async_copy(source, target, sem)


def start_kernel(
    state_hbm, table_hbm, out_hbm, stats_ref, state_ref, table_ref, planes_ref, whole_ref, deriv_ref, in_sems, out_sems
):
    loads = [copy_of(table_hbm, table_ref, in_sems.at[ROWS])]
    loads += [copy_of(state_hbm.at[:, k], state_ref.at[:, k], in_sems.at[k]) for k in range(ROWS)]
    for load in loads:
        load.start()
    stats_ref[...] = jnp.zeros_like(stats_ref)
    loads[0].wait()

    def one_row(local, carry):
        copy_of(state_hbm.at[:, local], state_ref.at[:, local], in_sems.at[local]).wait()
        kz_wave, ksquare = waves_of(local)
        real_part = state_ref[0, local]
        imag_part = state_ref[1, local]
        weight = jnp.where(iota((N, HALF), 1) == 0, 1.0, 2.0)
        energy = weight * (real_part * real_part + imag_part * imag_part)
        stats_ref[0] += jnp.sum(energy.reshape(N // 8, 8, HALF), axis=0)
        stats_ref[1] += jnp.sum((ksquare * energy).reshape(N // 8, 8, HALF), axis=0)
        z_inverse(local, z_rows(real_part, imag_part, kz_wave), table_ref, whole_ref, deriv_ref)
        return carry

    lax.fori_loop(0, ROWS, one_row, 0)

    def leaving(k):
        part = pl.ds(k * CHUNK, CHUNK)
        return copy_of(planes_ref.at[part], out_hbm.at[part], out_sems.at[k])

    def one_chunk(k, carry):
        send_planes(k * CHUNK, CHUNK, planes_ref, whole_ref, deriv_ref)
        leaving(k).start()
        return carry

    lax.fori_loop(0, PEERS // CHUNK, one_chunk, 0)
    for k in range(PEERS // CHUNK):
        leaving(k).wait()


def in_three(value):
    high = value.astype(BF16).astype(F32)
    rest = value - high
    middle = rest.astype(BF16).astype(F32)
    return high, middle, (rest - middle).astype(BF16).astype(F32)


def packed_four(parts):
    lane = iota((2 * ROWS, HALF), 1)
    turned = [parts[0]] + [pltpu.roll(parts[k], HALF - 32 * k, 1) for k in (1, 2, 3)]
    return [jnp.where(lane < HALF - 32 * (k + 1), turned[k], turned[k + 1]) for k in (0, 1, 2)]


def unpacked_four(packed):
    lane = iota((2 * N, HALF), 1)
    first, second, third = (packed[:, k * HALF : (k + 1) * HALF] for k in (0, 1, 2))
    return [
        first,
        pltpu.roll(jnp.where(lane >= 96, first, second), 32, 1),
        pltpu.roll(jnp.where(lane >= 64, second, third), 64, 1),
        pltpu.roll(third, 96, 1),
    ]


def grid_kernel(scalars, planes_hbm, speed_ref, stats_ref, held, out_ref, passed, sums_ref, peak_ref, *apart):
    count = 2 * N
    if apart:
        planes_ref, planes_sems, sems = apart

        def came_plane(k):
            return copy_of(planes_hbm.at[:, k], planes_ref.at[:, k], planes_sems.at[k])

        loads = [copy_of(source, target, sems.at[k]) for k, (source, target) in enumerate(zip(held, passed))]
        loads[0].start()
        for k in range(PAIR):
            came_plane(k).start()
        for load in loads[1:4]:
            load.start()
        for k in range(PAIR, ROWS):
            came_plane(k).start()
        for load in loads[4:]:
            load.start()
        held = passed
    else:
        planes_ref = planes_hbm
    y_inv_ref, x_inv_ref, x_fwd_ref, y_fwd_ref = held[:4]
    peak_ref[...] = jnp.zeros_like(peak_ref)
    row = iota((count, HALF), 0)
    ky_wave = signed(row // (2 * ROWS) * ROWS + row % ROWS)
    kx_wave = iota((N, HALF), 1).astype(F32)

    def one_pair(step, carry):
        if apart:
            for k in range(PAIR):
                came_plane(step * PAIR + k).wait()
        came = [planes_ref[:, step * PAIR + k].reshape(count, N) for k in range(PAIR)]
        scaled = [(ky_wave * part[:, :HALF].astype(F32)).astype(BF16) for part in came]
        if apart:
            pl.when(step == 0)(loads[0].wait)
        y_section = dot(y_inv_ref[...], jnp.concatenate(came + scaled, axis=1))
        x_rows = []
        for k in range(PAIR):
            starts = (k * N, PAIR * N + k * HALF, k * N + HALF)
            for which, at in enumerate(starts):
                halves = [y_section[part * N : (part + 1) * N, at : at + HALF] for part in (0, 1)]
                if which == 0:
                    halves = [kx_wave * half for half in halves]
                x_rows.append(jnp.concatenate(halves, axis=1).astype(BF16))
        if apart:
            for load in loads[1:4]:
                pl.when(step == 0)(load.wait)
        gradients = dot(jnp.concatenate(x_rows, axis=0), x_inv_ref[...])
        fields = []
        for k in range(PAIR):
            parts = [gradients[(3 * k + d) * N : (3 * k + d + 1) * N] for d in range(3)]
            total = speed_ref[0, step * PAIR + k].astype(F32) * parts[0]
            total = total + speed_ref[1, step * PAIR + k].astype(F32) * parts[1]
            total = total + speed_ref[2, step * PAIR + k].astype(F32) * parts[2]
            fields.append(total.astype(BF16))
            square = parts[0] * parts[0] + parts[1] * parts[1] + parts[2] * parts[2]
            peak_ref[...] = jnp.maximum(peak_ref[...], jnp.max(square.reshape(N // 8, 8, N), axis=0))
        x_section = dot(jnp.concatenate(fields, axis=0), x_fwd_ref[...]).astype(BF16)
        columns = []
        for k in range(PAIR):
            part = x_section[k * N : (k + 1) * N]
            columns.append(jnp.concatenate([part[:, :HALF], part[:, HALF:]], axis=0))
        sums = dot(y_fwd_ref[...], jnp.concatenate(columns, axis=1))
        for k in range(PAIR):
            start = pl.multiple_of((step * PAIR + k) * PITCH, 8)
            sums_ref[pl.ds(start, count), :] = sums[:, k * HALF : (k + 1) * HALF]
        return carry

    lax.fori_loop(0, ROWS // PAIR, one_pair, 0)
    shape = (2 * ROWS, HALF)
    peak = jnp.sqrt(jnp.max(peak_ref[...], keepdims=True))
    pieces = []
    for value in (jnp.sum(stats_ref[0], keepdims=True), jnp.sum(stats_ref[1], keepdims=True), peak):
        pieces.extend(in_three(jnp.broadcast_to(value, shape)))
    line = jnp.zeros(shape, F32)
    for k, piece in enumerate(pieces):
        line = jnp.where((iota(shape, 0) == 0) & (iota(shape, 1) == LIMIT + k), piece, line)

    def some_peers(step, carry):
        for turn in range(SENDS):
            peer = step * SENDS + turn
            for group in range(ROWS // GROUP):
                parts = []
                for pos in range(GROUP):
                    start = peer * 2 * ROWS + group * GROUP + pos
                    real_part = sums_ref[pl.ds(start, ROWS, stride=PITCH), :]
                    imag_part = sums_ref[pl.ds(start + ROWS, ROWS, stride=PITCH), :]
                    parts.append(jnp.concatenate([real_part, imag_part], axis=0))
                if group == 0:
                    parts[0] = parts[0] + line
                for k, tile in enumerate(packed_four(parts)):
                    at = (group * 3 + k) * HALF
                    out_ref[peer, :, at : at + HALF] = tile.astype(BF16)
        return carry

    lax.fori_loop(0, PEERS // SENDS, some_peers, 0)
    if apart:
        for load in loads[4:]:
            load.wait()


def tendency(came_ref, table_ref, group):
    at = group * GROUP * KEPT
    packed = dot(table_ref[...], came_ref[:, :, at : at + GROUP * KEPT].reshape(2 * N, GROUP * KEPT))
    return [(part[:N], part[N:]) for part in unpacked_four(packed)]


def middle_kernel(
    bound_ref,
    species_ref,
    base_ref,
    came_ref,
    state_ref,
    z_fwd_ref,
    z_inv_ref,
    out_ref,
    kept_ref,
    kappa_ref,
    whole_ref,
    deriv_ref,
):
    shape = (PEERS, 2 * ROWS, HALF)
    found = jnp.where(iota(shape, 1) == 0, came_ref[:, :, :HALF].astype(F32), 0.0)
    lane = iota(shape, 2)

    def piece(which):
        low = LIMIT + 3 * which
        inside = jnp.where((lane >= low) & (lane < low + 3), found, 0.0)
        return jnp.sum(jnp.sum(inside, axis=1), axis=1, keepdims=True)

    def spread(value):
        return jnp.broadcast_to(value, (8, HALF))

    variance = spread(jnp.sum(piece(0), axis=0, keepdims=True)) / CELLS
    mean_grad = spread(jnp.sum(piece(1), axis=0, keepdims=True)) / CELLS
    peak = spread(jnp.max(piece(2), axis=0, keepdims=True))
    base = base_ref[species_ref[0]]
    found = base * peak * jnp.sqrt(variance) / (mean_grad + 1e-06)
    kappa_ref[0] = jnp.max(found)
    kappa = found[0:1, :]
    bound = (bound_ref[0] * bound_ref[0]).astype(F32)
    for group in range(ROWS // GROUP):
        parts = tendency(came_ref, z_fwd_ref, group)
        for pos, (sum_real, sum_imag) in enumerate(parts):
            local = group * GROUP + pos
            kz_wave, ksquare = waves_of(local)
            factor = jnp.exp(-kappa * ksquare * STEP)
            inside = ksquare <= bound
            first = [jnp.where(inside, -part, 0.0) for part in (sum_real, sum_imag)]
            middle = []
            for part in (0, 1):
                start = state_ref[part, local]
                middle.append(factor * (start + STEP * first[part]))
                kept_ref[part, local] = factor * start + (0.5 * STEP) * (factor * first[part])
            z_inverse(local, z_rows(*middle, kz_wave), z_inv_ref, whole_ref, deriv_ref)
    send_planes(0, PEERS, out_ref, whole_ref, deriv_ref)


def final_kernel(bound_ref, came_ref, kept_ref, z_fwd_ref, out_hbm, out_ref, out_sems):
    bound = (bound_ref[0] * bound_ref[0]).astype(F32)
    saves = []
    for group in range(ROWS // GROUP):
        parts = tendency(came_ref, z_fwd_ref, group)
        for pos, sums in enumerate(parts):
            local = group * GROUP + pos
            _, ksquare = waves_of(local)
            for part in (0, 1):
                second = jnp.where(ksquare <= bound, -sums[part], 0.0)
                out_ref[part, local] = kept_ref[part, local] + (0.5 * STEP) * second
            saves.append(copy_of(out_ref.at[:, local], out_hbm.at[:, local], out_sems.at[local]))
            saves[-1].start()
    for save in saves:
        save.wait()


SCALARS = pl.BlockSpec(memory_space=pltpu.SMEM)
NEAR = pl.BlockSpec(memory_space=pltpu.VMEM)
FAR = pl.BlockSpec(memory_space=pltpu.HBM)
PLANES = (PEERS, ROWS, 2 * ROWS, N)
SENT = (PEERS, 2 * ROWS, PACKED)
STATE = (2, ROWS, N, HALF)
PAIR = 4
CHUNK = 8
UNROLL = 2
SENDS = 4


def params(mebibytes):
    return pltpu.CompilerParams(vmem_limit_bytes=mebibytes * 2**20)


def shaped(shape, dtype):
    return jax.ShapeDtypeStruct(shape, dtype)


def near(x):
    return pltpu.with_memory_space_constraint(x, pltpu.VMEM)


def far(x):
    return pltpu.with_memory_space_constraint(x, pltpu.HBM)


def sems(count):
    return pltpu.SemaphoreType.DMA((count,))


def turned():
    return pltpu.VMEM((ROWS * PITCH, HALF), F32)


BIG = pltpu.VMEM((2 * N, 2 * N), BF16)
SMALL = pltpu.VMEM((N, N), BF16)
HELD = pltpu.VMEM(STATE, F32)


def gathered(velocity):
    groups = lax.axis_size("scal")
    me = lax.axis_index("scal")
    ring = 4

    def moved(x, change):
        return lax.ppermute(x, "scal", [(s, change(s)) for s in range(groups)])

    def beside(shift):
        return lambda s: s // ring * ring + (s + shift) % ring

    across = moved(velocity, lambda s: (s + ring) % groups)
    out = jnp.zeros((*velocity.shape[:2], N, N), velocity.dtype)
    high, low = me // ring, me % ring
    half = velocity.shape[1] // 2

    def placed(out, x, owner, first=0):
        return lax.dynamic_update_slice(out, x, (0, first, owner * x.shape[2], 0))

    for x, own in ((velocity, high), (across, 1 - high)):
        up = moved(x, beside(1))
        down = moved(x, beside(-1))
        far_up = moved(up[:, :half], beside(1))
        far_down = moved(down[:, half:], beside(-1))
        start = own * ring
        out = placed(out, x, start + low)
        out = placed(out, up, start + (low + ring - 1) % ring)
        out = placed(out, down, start + (low + 1) % ring)
        out = placed(out, far_up, start + (low + 2) % ring)
        out = placed(out, far_down, start + (low + 2) % ring, half)
    return out


def exchanged(x):
    return lax.all_to_all(x, "fft", 0, 0, tiled=True)


def start_call(state, table):
    return pl.pallas_call(
        start_kernel,
        in_specs=[FAR, FAR],
        out_specs=[FAR, NEAR],
        out_shape=[pltpu.HBM(PLANES, BF16), pltpu.VMEM((2, 8, HALF), F32)],
        scratch_shapes=[HELD, BIG, pltpu.VMEM(PLANES, BF16), turned(), turned(), sems(ROWS + 1), sems(PEERS // CHUNK)],
        compiler_params=params(24),
        name="start",
    )(far(state), far(table["z_inv"]))


def grid_call(scalars, planes, speeds, stats, held, apart):
    scratch = [turned(), pltpu.VMEM((8, N), F32)]
    passed = held if apart else ()
    if apart:
        scratch += [pltpu.VMEM(PLANES, BF16), sems(ROWS), sems(len(held))]
    spec, place = (FAR, far) if apart else (NEAR, near)
    return pl.pallas_call(
        grid_kernel,
        in_specs=[(SCALARS,) * len(scalars), spec, NEAR, NEAR, (spec,) * len(held)],
        out_specs=[NEAR, (NEAR,) * len(passed)],
        out_shape=[pltpu.VMEM(SENT, BF16), tuple(pltpu.VMEM(x.shape, x.dtype) for x in passed)],
        scratch_shapes=scratch,
        compiler_params=params(24),
        name="grid",
    )(scalars, place(planes), near(speeds), near(stats), tuple(place(x) for x in held))


def middle_call(scalars, came, state, z_fwd, z_inv):
    return pl.pallas_call(
        middle_kernel,
        in_specs=[SCALARS] * 3 + [NEAR] * 4,
        out_specs=[NEAR, NEAR, SCALARS],
        out_shape=[pltpu.VMEM(PLANES, BF16), pltpu.VMEM(STATE, F32), shaped((1,), F32)],
        scratch_shapes=[turned(), turned()],
        compiler_params=params(24),
        name="middle",
    )(*scalars, *(near(x) for x in (came, state, z_fwd, z_inv)))


def final_call(bound, came, kept, z_fwd):
    return pl.pallas_call(
        final_kernel,
        in_specs=[SCALARS, NEAR, NEAR, NEAR],
        out_specs=FAR,
        out_shape=pltpu.HBM(STATE, F32),
        scratch_shapes=[HELD, sems(ROWS)],
        compiler_params=params(24),
        name="final",
    )(bound, near(came), near(kept), near(z_fwd))


def body(scalar_state, velocity, species, kappa_table, dealias_bound):
    table = tables()
    state = scalar_state[0]
    speeds = gathered(velocity)
    planes, stats = start_call(state, table)
    scalars = (dealias_bound, species, kappa_table)
    held = tuple(table[name] for name in ("y_inv", "x_inv", "x_fwd", "y_fwd", "z_fwd", "z_inv")) + (state,)
    sent, held = grid_call(scalars, exchanged(planes), speeds, stats, held, True)
    *grid_tables, z_fwd, z_inv, state = held
    planes, kept, kappa = middle_call(scalars, exchanged(sent), state, z_fwd, z_inv)
    sent, _ = grid_call((), exchanged(planes), speeds, stats, tuple(grid_tables), False)
    return (final_call(dealias_bound, exchanged(sent), kept, z_fwd)[None], kappa)


def solution(mesh):
    placed = (
        P("scal", None, "fft", None, None),
        P(None, "fft", "scal", None),
        P("scal"),
        P(),
        P("scal"),
    )
    return jax.shard_map(
        body,
        mesh=mesh,
        in_specs=placed,
        out_specs=(P("scal", None, "fft", None, None), P("scal")),
        check_vma=False,
    )
```

```python
import math

import jax
import jax.numpy as jnp
import numpy as np
from jax import lax
from jax.experimental import pallas as pl
from jax.experimental.pallas import tpu as pltpu
from jax.sharding import PartitionSpec as P

N = 256
HALF = 128
PEERS = 32
ROWS = N // PEERS
GROUP = 4
KEPT = 96
LIMIT = 86
PACKED = ROWS * KEPT
PITCH = 2 * N + 4
STEP = 0.2 * 2.0 * math.pi / N
CELLS = float(N) ** 3
F32 = jnp.float32
BF16 = jnp.bfloat16


def tables():
    def cos_sin(rows, columns):
        angles = (rows[:, None] * columns[None, :] % N).astype(np.float32) * np.float32(2.0 * math.pi / N)
        scale = np.float32(1.0 / math.sqrt(N))
        return np.cos(angles) * scale, np.sin(angles) * scale

    def inverse(rows, columns):
        cos, sin = cos_sin(rows, columns)
        return np.block([[cos, -sin], [sin, cos]])

    def forward(rows, columns):
        cos, sin = cos_sin(rows, columns)
        return np.block([[cos, sin], [-sin, cos]])

    def order(peers):
        return np.arange(2 * peers * ROWS).reshape(2, peers, ROWS).transpose(1, 0, 2).reshape(-1)

    index, low = np.arange(N), np.arange(HALF)
    cos, sin = cos_sin(index, low)
    weight = np.where(low == 0, 1.0, 2.0).astype(np.float32)[:, None]
    keep = (low < LIMIT).astype(np.float32)[None, :]
    halves = order(PEERS // 2)
    listed = {
        "z_inv": np.stack([inverse(2 * low + turn, low) for turn in (0, 1)]),
        "y_inv": np.stack([inverse(2 * low + turn, low)[:, halves] for turn in (0, 1)]),
        "x_inv": np.concatenate([-weight * sin.T, -weight * cos.T], axis=0),
        "x_fwd": np.concatenate([cos * keep, -sin * keep], axis=1),
        "y_fwd": np.stack([forward(low, 2 * low + turn)[halves] for turn in (0, 1)]),
        "z_fwd": forward(index, index)[:, order(PEERS)],
    }
    return {name: jnp.asarray(value.astype(np.float32)).astype(BF16) for name, value in listed.items()}


def both_turns(x):
    low, high = x[: x.shape[0] // 2], x[x.shape[0] // 2 :]
    return low + high, low - high


def dot(left, right):
    return jnp.dot(left, right, preferred_element_type=F32)


def iota(shape, dim):
    return lax.broadcasted_iota(jnp.int32, shape, dim)


def signed(index):
    return jnp.where(index < HALF, index, index - N).astype(F32)


def z_rows(real_part, imag_part, kz_wave):
    columns = [
        [jnp.concatenate(pair, axis=0).astype(BF16) for pair in zip(both_turns(real), both_turns(imag))]
        for real, imag in ((real_part, imag_part), (kz_wave * real_part, kz_wave * imag_part))
    ]
    return [jnp.concatenate(pair, axis=1) for pair in zip(*columns)]


def send_planes(first, count, planes_ref, whole_ref, deriv_ref):
    def some_peers(step, carry):
        for turn in range(UNROLL):
            peer = first + step * UNROLL + turn
            for local in range(ROWS):
                for at, ref in ((0, whole_ref), (HALF, deriv_ref)):
                    start = local % 2 * N + peer * (ROWS // 2) + local // 2
                    real_part = ref[pl.ds(start, ROWS, stride=PITCH), :]
                    imag_part = ref[pl.ds(start + HALF, ROWS, stride=PITCH), :]
                    tile = jnp.concatenate([real_part, imag_part], axis=0).astype(BF16)
                    planes_ref[peer, local, :, at : at + HALF] = tile
        return carry

    lax.fori_loop(0, count // UNROLL, some_peers, 0)


def row_of(block, shift=0):
    return block * PITCH + shift if isinstance(block, int) else pl.multiple_of(block * PITCH + shift, 4)


def z_inverse(local, rows, table_ref, whole_ref, deriv_ref):
    for turn in (0, 1):
        found = dot(table_ref[turn], rows[turn])
        part = pl.ds(row_of(local, turn * N), N)
        whole_ref[part, :] = found[:, :HALF]
        deriv_ref[part, :] = found[:, HALF:]


def waves_of(local):
    ky_wave = signed(lax.axis_index("fft").astype(jnp.int32) * ROWS + local)
    kz_wave = signed(iota((N, HALF), 0))
    kx_wave = iota((N, HALF), 1).astype(F32)
    return kz_wave, kx_wave * kx_wave + ky_wave * ky_wave + kz_wave * kz_wave


def copy_of(source, target, sem):
    return pltpu.make_async_copy(source, target, sem)


def start_kernel(
    state_hbm, table_hbm, out_hbm, stats_ref, state_ref, table_ref, planes_ref, whole_ref, deriv_ref, in_sems, out_sems
):
    loads = [copy_of(table_hbm, table_ref, in_sems.at[ROWS])]
    loads += [copy_of(state_hbm.at[:, k], state_ref.at[:, k], in_sems.at[k]) for k in range(ROWS)]
    for load in loads:
        load.start()
    stats_ref[...] = jnp.zeros_like(stats_ref)
    loads[0].wait()

    def one_row(local, carry):
        copy_of(state_hbm.at[:, local], state_ref.at[:, local], in_sems.at[local]).wait()
        kz_wave, ksquare = waves_of(local)
        real_part = state_ref[0, local]
        imag_part = state_ref[1, local]
        weight = jnp.where(iota((N, HALF), 1) == 0, 1.0, 2.0)
        energy = weight * (real_part * real_part + imag_part * imag_part)
        stats_ref[0] += jnp.sum(energy.reshape(N // 8, 8, HALF), axis=0)
        stats_ref[1] += jnp.sum((ksquare * energy).reshape(N // 8, 8, HALF), axis=0)
        z_inverse(local, z_rows(real_part, imag_part, kz_wave), table_ref, whole_ref, deriv_ref)
        return carry

    lax.fori_loop(0, ROWS, one_row, 0)

    def leaving(k):
        part = pl.ds(k * CHUNK, CHUNK)
        return copy_of(planes_ref.at[part], out_hbm.at[part], out_sems.at[k])

    def one_chunk(k, carry):
        send_planes(k * CHUNK, CHUNK, planes_ref, whole_ref, deriv_ref)
        leaving(k).start()
        return carry

    lax.fori_loop(0, PEERS // CHUNK, one_chunk, 0)
    for k in range(PEERS // CHUNK):
        leaving(k).wait()


def in_three(value):
    high = value.astype(BF16).astype(F32)
    rest = value - high
    middle = rest.astype(BF16).astype(F32)
    return high, middle, (rest - middle).astype(BF16).astype(F32)


def packed_four(parts):
    lane = iota((2 * ROWS, HALF), 1)
    turned = [parts[0]] + [pltpu.roll(parts[k], HALF - 32 * k, 1) for k in (1, 2, 3)]
    return [jnp.where(lane < HALF - 32 * (k + 1), turned[k], turned[k + 1]) for k in (0, 1, 2)]


def unpacked_four(packed):
    lane = iota((2 * N, HALF), 1)
    first, second, third = (packed[:, k * HALF : (k + 1) * HALF] for k in (0, 1, 2))
    return [
        first,
        pltpu.roll(jnp.where(lane >= 96, first, second), 32, 1),
        pltpu.roll(jnp.where(lane >= 64, second, third), 64, 1),
        pltpu.roll(third, 96, 1),
    ]


def grid_kernel(scalars, planes_hbm, speed_ref, stats_ref, held, out_ref, passed, sums_ref, peak_ref, *apart):
    count = 2 * N
    if apart:
        planes_ref, planes_sems, sems = apart

        def came_plane(k):
            return copy_of(planes_hbm.at[:, k], planes_ref.at[:, k], planes_sems.at[k])

        loads = [copy_of(source, target, sems.at[k]) for k, (source, target) in enumerate(zip(held, passed))]
        loads[0].start()
        for k in range(PAIR):
            came_plane(k).start()
        for load in loads[1:4]:
            load.start()
        for k in range(PAIR, ROWS):
            came_plane(k).start()
        for load in loads[4:]:
            load.start()
        held = passed
    else:
        planes_ref = planes_hbm
    y_inv_ref, x_inv_ref, x_fwd_ref, y_fwd_ref = held[:4]
    peak_ref[...] = jnp.zeros_like(peak_ref)
    row = iota((count, HALF), 0)
    ky_wave = signed(row // (2 * ROWS) * ROWS + row % ROWS).astype(BF16)
    kx_wave = iota((HALF, HALF), 1).astype(F32)

    def one_pair(step, carry):
        if apart:
            for k in range(PAIR):
                came_plane(step * PAIR + k).wait()
            for load in loads[:4]:
                pl.when(step == 0)(load.wait)
        came = [planes_ref[:, step * PAIR + k].reshape(count, N) for k in range(PAIR)]
        scaled = [ky_wave * part[:, :HALF] for part in came]
        pairs = both_turns(jnp.concatenate(came + scaled, axis=1))
        y_section = [dot(y_inv_ref[turn], pairs[turn]) for turn in (0, 1)]
        x_rows = []
        for k in range(PAIR):
            starts = (k * N, PAIR * N + k * HALF, k * N + HALF)
            for which, at in enumerate(starts):
                for found in y_section:
                    halves = [found[part * HALF : (part + 1) * HALF, at : at + HALF] for part in (0, 1)]
                    if which == 0:
                        halves = [kx_wave * half for half in halves]
                    x_rows.append(jnp.concatenate(halves, axis=1).astype(BF16))
        gradients = dot(jnp.concatenate(x_rows, axis=0), x_inv_ref[...])
        fields = []
        for k in range(PAIR):
            parts = [gradients[(3 * k + d) * N : (3 * k + d + 1) * N] for d in range(3)]
            total = speed_ref[0, step * PAIR + k].astype(F32) * parts[0]
            total = total + speed_ref[1, step * PAIR + k].astype(F32) * parts[1]
            total = total + speed_ref[2, step * PAIR + k].astype(F32) * parts[2]
            fields.append(total.astype(BF16))
            square = parts[0] * parts[0] + parts[1] * parts[1] + parts[2] * parts[2]
            peak_ref[...] = jnp.maximum(peak_ref[...], jnp.max(square.reshape(N // 8, 8, N), axis=0))
        x_section = dot(jnp.concatenate(fields, axis=0), x_fwd_ref[...]).astype(BF16)
        sums = []
        for turn in (0, 1):
            columns = []
            for k in range(PAIR):
                part = x_section[k * N + turn * HALF : k * N + (turn + 1) * HALF]
                columns.append(jnp.concatenate([part[:, :HALF], part[:, HALF:]], axis=0))
            sums.append(dot(y_fwd_ref[turn], jnp.concatenate(columns, axis=1)))
        for k in range(PAIR):
            even, odd = (found[:, k * HALF : (k + 1) * HALF] for found in sums)
            sums_ref[pl.ds(row_of(step * PAIR + k), N), :] = even + odd
            sums_ref[pl.ds(row_of(step * PAIR + k, N), N), :] = even - odd
        return carry

    lax.fori_loop(0, ROWS // PAIR, one_pair, 0)
    shape = (2 * ROWS, HALF)
    peak = jnp.sqrt(jnp.max(peak_ref[...], keepdims=True))
    pieces = []
    for value in (jnp.sum(stats_ref[0], keepdims=True), jnp.sum(stats_ref[1], keepdims=True), peak):
        pieces.extend(in_three(jnp.broadcast_to(value, shape)))
    line = jnp.zeros(shape, F32)
    for k, piece in enumerate(pieces):
        line = jnp.where((iota(shape, 0) == 0) & (iota(shape, 1) == LIMIT + k), piece, line)

    def some_peers(step, carry):
        for turn in range(SENDS):
            peer = step * SENDS + turn
            for group in range(ROWS // GROUP):
                parts = []
                for pos in range(GROUP):
                    start = peer * 2 * ROWS + group * GROUP + pos
                    real_part = sums_ref[pl.ds(start, ROWS, stride=PITCH), :]
                    imag_part = sums_ref[pl.ds(start + ROWS, ROWS, stride=PITCH), :]
                    parts.append(jnp.concatenate([real_part, imag_part], axis=0))
                if group == 0:
                    parts[0] = parts[0] + line
                for k, tile in enumerate(packed_four(parts)):
                    at = (group * 3 + k) * HALF
                    out_ref[peer, :, at : at + HALF] = tile.astype(BF16)
        return carry

    lax.fori_loop(0, PEERS // SENDS, some_peers, 0)
    if apart:
        for load in loads[4:]:
            load.wait()


def tendency(came_ref, table_ref, group):
    at = group * GROUP * KEPT
    packed = dot(table_ref[...], came_ref[:, :, at : at + GROUP * KEPT].reshape(2 * N, GROUP * KEPT))
    return [(part[:N], part[N:]) for part in unpacked_four(packed)]


def middle_kernel(
    bound_ref,
    species_ref,
    base_ref,
    came_ref,
    state_ref,
    z_fwd_ref,
    z_inv_ref,
    out_ref,
    kept_ref,
    kappa_ref,
    whole_ref,
    deriv_ref,
):
    shape = (PEERS, 2 * ROWS, HALF)
    found = jnp.where(iota(shape, 1) == 0, came_ref[:, :, :HALF].astype(F32), 0.0)
    lane = iota(shape, 2)

    def piece(which):
        low = LIMIT + 3 * which
        inside = jnp.where((lane >= low) & (lane < low + 3), found, 0.0)
        return jnp.sum(jnp.sum(inside, axis=1), axis=1, keepdims=True)

    def spread(value):
        return jnp.broadcast_to(value, (8, HALF))

    variance = spread(jnp.sum(piece(0), axis=0, keepdims=True)) / CELLS
    mean_grad = spread(jnp.sum(piece(1), axis=0, keepdims=True)) / CELLS
    peak = spread(jnp.max(piece(2), axis=0, keepdims=True))
    base = base_ref[species_ref[0]]
    found = base * peak * jnp.sqrt(variance) / (mean_grad + 1e-06)
    kappa_ref[0] = jnp.max(found)
    kappa = found[0:1, :]
    bound = (bound_ref[0] * bound_ref[0]).astype(F32)
    for group in range(ROWS // GROUP):
        parts = tendency(came_ref, z_fwd_ref, group)
        for pos, (sum_real, sum_imag) in enumerate(parts):
            local = group * GROUP + pos
            kz_wave, ksquare = waves_of(local)
            factor = jnp.exp(-kappa * ksquare * STEP)
            inside = ksquare <= bound
            first = [jnp.where(inside, -part, 0.0) for part in (sum_real, sum_imag)]
            middle = []
            for part in (0, 1):
                start = state_ref[part, local]
                middle.append(factor * (start + STEP * first[part]))
                kept_ref[part, local] = factor * start + (0.5 * STEP) * (factor * first[part])
            z_inverse(local, z_rows(*middle, kz_wave), z_inv_ref, whole_ref, deriv_ref)
    send_planes(0, PEERS, out_ref, whole_ref, deriv_ref)


def final_kernel(bound_ref, came_ref, kept_ref, z_fwd_ref, out_hbm, out_ref, out_sems):
    bound = (bound_ref[0] * bound_ref[0]).astype(F32)
    saves = []
    for group in range(ROWS // GROUP):
        parts = tendency(came_ref, z_fwd_ref, group)
        for pos, sums in enumerate(parts):
            local = group * GROUP + pos
            _, ksquare = waves_of(local)
            for part in (0, 1):
                second = jnp.where(ksquare <= bound, -sums[part], 0.0)
                out_ref[part, local] = kept_ref[part, local] + (0.5 * STEP) * second
            saves.append(copy_of(out_ref.at[:, local], out_hbm.at[:, local], out_sems.at[local]))
            saves[-1].start()
    for save in saves:
        save.wait()


SCALARS = pl.BlockSpec(memory_space=pltpu.SMEM)
NEAR = pl.BlockSpec(memory_space=pltpu.VMEM)
FAR = pl.BlockSpec(memory_space=pltpu.HBM)
PLANES = (PEERS, ROWS, 2 * ROWS, N)
SENT = (PEERS, 2 * ROWS, PACKED)
STATE = (2, ROWS, N, HALF)
PAIR = 4
CHUNK = 8
UNROLL = 2
SENDS = 4


def params(mebibytes):
    return pltpu.CompilerParams(vmem_limit_bytes=mebibytes * 2**20)


def shaped(shape, dtype):
    return jax.ShapeDtypeStruct(shape, dtype)


def near(x):
    return pltpu.with_memory_space_constraint(x, pltpu.VMEM)


def far(x):
    return pltpu.with_memory_space_constraint(x, pltpu.HBM)


def sems(count):
    return pltpu.SemaphoreType.DMA((count,))


def turned():
    return pltpu.VMEM((ROWS * PITCH, HALF), F32)


BIG = pltpu.VMEM((2, N, N), BF16)
HELD = pltpu.VMEM(STATE, F32)


def gathered(velocity):
    groups = lax.axis_size("scal")
    me = lax.axis_index("scal")
    ring = 4
    high, low = me // ring, me % ring
    planes, rows = velocity.shape[1], velocity.shape[2] // 2
    velocity = velocity.reshape(3, planes, rows, 2, N).swapaxes(2, 3)

    def moved(x, change):
        return lax.ppermute(x, "scal", [(s, change(s)) for s in range(groups)])

    def beside(shift):
        return lambda s: s // ring * ring + (s + shift) % ring

    across = moved(velocity, lambda s: (s + ring) % groups)
    out = jnp.zeros((3, planes, 2, HALF, N), velocity.dtype)
    half = planes // 2

    def placed(out, x, owner, first=0):
        return lax.dynamic_update_slice(out, x, (0, first, 0, owner * rows, 0))

    for x, own in ((velocity, high), (across, 1 - high)):
        up = moved(x, beside(1))
        down = moved(x, beside(-1))
        far_up = moved(up[:, :half], beside(1))
        far_down = moved(down[:, half:], beside(-1))
        start = own * ring
        out = placed(out, x, start + low)
        out = placed(out, up, start + (low + ring - 1) % ring)
        out = placed(out, down, start + (low + 1) % ring)
        out = placed(out, far_up, start + (low + 2) % ring)
        out = placed(out, far_down, start + (low + 2) % ring, half)
    return out.reshape(3, planes, N, N)


def exchanged(x):
    return lax.all_to_all(x, "fft", 0, 0, tiled=True)


def start_call(state, table):
    return pl.pallas_call(
        start_kernel,
        in_specs=[FAR, FAR],
        out_specs=[FAR, NEAR],
        out_shape=[pltpu.HBM(PLANES, BF16), pltpu.VMEM((2, 8, HALF), F32)],
        scratch_shapes=[HELD, BIG, pltpu.VMEM(PLANES, BF16), turned(), turned(), sems(ROWS + 1), sems(PEERS // CHUNK)],
        compiler_params=params(24),
        name="start",
    )(far(state), far(table["z_inv"]))


def grid_call(scalars, planes, speeds, stats, held, apart):
    scratch = [turned(), pltpu.VMEM((8, N), F32)]
    passed = held if apart else ()
    if apart:
        scratch += [pltpu.VMEM(PLANES, BF16), sems(ROWS), sems(len(held))]
    spec, place = (FAR, far) if apart else (NEAR, near)
    return pl.pallas_call(
        grid_kernel,
        in_specs=[(SCALARS,) * len(scalars), spec, NEAR, NEAR, (spec,) * len(held)],
        out_specs=[NEAR, (NEAR,) * len(passed)],
        out_shape=[pltpu.VMEM(SENT, BF16), tuple(pltpu.VMEM(x.shape, x.dtype) for x in passed)],
        scratch_shapes=scratch,
        compiler_params=params(24),
        name="grid",
    )(scalars, place(planes), near(speeds), near(stats), tuple(place(x) for x in held))


def middle_call(scalars, came, state, z_fwd, z_inv):
    return pl.pallas_call(
        middle_kernel,
        in_specs=[SCALARS] * 3 + [NEAR] * 4,
        out_specs=[NEAR, NEAR, SCALARS],
        out_shape=[pltpu.VMEM(PLANES, BF16), pltpu.VMEM(STATE, F32), shaped((1,), F32)],
        scratch_shapes=[turned(), turned()],
        compiler_params=params(24),
        name="middle",
    )(*scalars, *(near(x) for x in (came, state, z_fwd, z_inv)))


def final_call(bound, came, kept, z_fwd):
    return pl.pallas_call(
        final_kernel,
        in_specs=[SCALARS, NEAR, NEAR, NEAR],
        out_specs=FAR,
        out_shape=pltpu.HBM(STATE, F32),
        scratch_shapes=[HELD, sems(ROWS)],
        compiler_params=params(24),
        name="final",
    )(bound, near(came), near(kept), near(z_fwd))


def body(scalar_state, velocity, species, kappa_table, dealias_bound):
    table = tables()
    state = scalar_state[0]
    speeds = gathered(velocity)
    planes, stats = start_call(state, table)
    scalars = (dealias_bound, species, kappa_table)
    held = tuple(table[name] for name in ("y_inv", "x_inv", "x_fwd", "y_fwd", "z_fwd", "z_inv")) + (state,)
    sent, held = grid_call(scalars, exchanged(planes), speeds, stats, held, True)
    *grid_tables, z_fwd, z_inv, state = held
    planes, kept, kappa = middle_call(scalars, exchanged(sent), state, z_fwd, z_inv)
    sent, _ = grid_call((), exchanged(planes), speeds, stats, tuple(grid_tables), False)
    return (final_call(dealias_bound, exchanged(sent), kept, z_fwd)[None], kappa)


def solution(mesh):
    placed = (
        P("scal", None, "fft", None, None),
        P(None, "fft", "scal", None),
        P("scal"),
        P(),
        P("scal"),
    )
    return jax.shard_map(
        body,
        mesh=mesh,
        in_specs=placed,
        out_specs=(P("scal", None, "fft", None, None), P("scal")),
        check_vma=False,
    )
```

```python
import math

import jax
import jax.numpy as jnp
import numpy as np
from jax import lax
from jax.experimental import pallas as pl
from jax.experimental.pallas import tpu as pltpu
from jax.sharding import PartitionSpec as P

N = 256
HALF = 128
PEERS = 32
ROWS = N // PEERS
KEPT = 88
LIMIT = 86
BLOCKS = ROWS * KEPT // HALF
PITCH = 2 * N + 4
STEP = 0.2 * 2.0 * math.pi / N
CELLS = float(N) ** 3
F32 = jnp.float32
BF16 = jnp.bfloat16


def tables():
    def cos_sin(rows, columns):
        angles = (rows[:, None] * columns[None, :] % N).astype(np.float32) * np.float32(2.0 * math.pi / N)
        scale = np.float32(1.0 / math.sqrt(N))
        return np.cos(angles) * scale, np.sin(angles) * scale

    def inverse(rows, columns):
        cos, sin = cos_sin(rows, columns)
        return np.block([[cos, -sin], [sin, cos]])

    def forward(rows, columns):
        cos, sin = cos_sin(rows, columns)
        return np.block([[cos, sin], [-sin, cos]])

    def order(peers):
        return np.arange(2 * peers * ROWS).reshape(2, peers, ROWS).transpose(1, 0, 2).reshape(-1)

    index, low = np.arange(N), np.arange(HALF)
    cos, sin = cos_sin(index, low)
    weight = np.where(low == 0, 1.0, 2.0).astype(np.float32)[:, None]
    keep = (low < LIMIT).astype(np.float32)[None, :]
    halves = order(PEERS // 2)
    listed = {
        "z_inv": np.stack([inverse(2 * low + turn, low) for turn in (0, 1)]),
        "y_inv": np.stack([inverse(2 * low + turn, low)[:, halves] for turn in (0, 1)]),
        "x_inv": np.concatenate([-weight * sin.T, -weight * cos.T], axis=0),
        "x_fwd": np.concatenate([cos * keep, -sin * keep], axis=1),
        "y_fwd": np.stack([forward(low, 2 * low + turn)[halves] for turn in (0, 1)]),
        "z_fwd": forward(index, index)[:, order(PEERS)],
    }
    return {name: jnp.asarray(value.astype(np.float32)).astype(BF16) for name, value in listed.items()}


def both_turns(x):
    low, high = x[: x.shape[0] // 2], x[x.shape[0] // 2 :]
    return low + high, low - high


def dot(left, right):
    return jnp.dot(left, right, preferred_element_type=F32)


def iota(shape, dim):
    return lax.broadcasted_iota(jnp.int32, shape, dim)


def signed(index):
    return jnp.where(index < HALF, index, index - N).astype(F32)


def z_rows(real_part, imag_part, kz_wave):
    columns = [
        [jnp.concatenate(pair, axis=0).astype(BF16) for pair in zip(both_turns(real), both_turns(imag))]
        for real, imag in ((real_part, imag_part), (kz_wave * real_part, kz_wave * imag_part))
    ]
    return [jnp.concatenate(pair, axis=1) for pair in zip(*columns)]


def send_planes(first, count, planes_ref, whole_ref, deriv_ref):
    def some_peers(step, carry):
        for turn in range(UNROLL):
            peer = first + step * UNROLL + turn
            for local in range(ROWS):
                for at, ref in ((0, whole_ref), (HALF, deriv_ref)):
                    start = local % 2 * N + peer * (ROWS // 2) + local // 2
                    real_part = ref[pl.ds(start, ROWS, stride=PITCH), :]
                    imag_part = ref[pl.ds(start + HALF, ROWS, stride=PITCH), :]
                    tile = jnp.concatenate([real_part, imag_part], axis=0).astype(BF16)
                    planes_ref[peer, local, :, at : at + HALF] = tile
        return carry

    lax.fori_loop(0, count // UNROLL, some_peers, 0)


def row_of(block, shift=0):
    return block * PITCH + shift if isinstance(block, int) else pl.multiple_of(block * PITCH + shift, 4)


def z_inverse(local, rows, table_ref, whole_ref, deriv_ref):
    for turn in (0, 1):
        found = dot(table_ref[turn], rows[turn])
        part = pl.ds(row_of(local, turn * N), N)
        whole_ref[part, :] = found[:, :HALF]
        deriv_ref[part, :] = found[:, HALF:]


def waves_of(local):
    ky_wave = signed(lax.axis_index("fft").astype(jnp.int32) * ROWS + local)
    kz_wave = signed(iota((N, HALF), 0))
    kx_wave = iota((N, HALF), 1).astype(F32)
    return kz_wave, kx_wave * kx_wave + ky_wave * ky_wave + kz_wave * kz_wave


def copy_of(source, target, sem):
    return pltpu.make_async_copy(source, target, sem)


def start_kernel(
    state_hbm, table_hbm, out_hbm, stats_ref, state_ref, table_ref, planes_ref, whole_ref, deriv_ref, in_sems, out_sems
):
    loads = [copy_of(table_hbm, table_ref, in_sems.at[ROWS])]
    loads += [copy_of(state_hbm.at[:, k], state_ref.at[:, k], in_sems.at[k]) for k in range(ROWS)]
    for load in loads:
        load.start()
    stats_ref[...] = jnp.zeros_like(stats_ref)
    loads[0].wait()

    def one_row(local, carry):
        copy_of(state_hbm.at[:, local], state_ref.at[:, local], in_sems.at[local]).wait()
        kz_wave, ksquare = waves_of(local)
        real_part = state_ref[0, local]
        imag_part = state_ref[1, local]
        weight = jnp.where(iota((N, HALF), 1) == 0, 1.0, 2.0)
        energy = weight * (real_part * real_part + imag_part * imag_part)
        stats_ref[0] += jnp.sum(energy.reshape(N // 8, 8, HALF), axis=0)
        stats_ref[1] += jnp.sum((ksquare * energy).reshape(N // 8, 8, HALF), axis=0)
        z_inverse(local, z_rows(real_part, imag_part, kz_wave), table_ref, whole_ref, deriv_ref)
        return carry

    lax.fori_loop(0, ROWS, one_row, 0)

    def leaving(k):
        part = pl.ds(k * CHUNK, CHUNK)
        return copy_of(planes_ref.at[part], out_hbm.at[part], out_sems.at[k])

    def one_chunk(k, carry):
        send_planes(k * CHUNK, CHUNK, planes_ref, whole_ref, deriv_ref)
        leaving(k).start()
        return carry

    lax.fori_loop(0, PEERS // CHUNK, one_chunk, 0)
    for k in range(PEERS // CHUNK):
        leaving(k).wait()


def in_three(value):
    high = value.astype(BF16).astype(F32)
    rest = value - high
    middle = rest.astype(BF16).astype(F32)
    return high, middle, (rest - middle).astype(BF16).astype(F32)


def place_of(row):
    return row * KEPT // HALF, row * KEPT % HALF


def packed(parts):
    lane = iota((2 * ROWS, HALF), 1)
    blocks = [None] * (BLOCKS + 1)
    for row, part in enumerate(parts):
        block, shift = place_of(row)
        turned = pltpu.roll(part, shift, 1) if shift else part
        blocks[block] = turned if shift == 0 else jnp.where(lane < shift, blocks[block], turned)
        if shift + KEPT > HALF:
            blocks[block + 1] = turned
    real_part, imag_part = blocks[BLOCKS][:ROWS], blocks[BLOCKS][ROWS:]
    blocks[BLOCKS] = jnp.where(lane[:ROWS] < HALF // 2, real_part, pltpu.roll(imag_part, HALF // 2, 1))
    return blocks


def unpacked(blocks):
    lane = iota((2 * N, HALF), 1)
    parts = []
    for row in range(ROWS):
        block, shift = place_of(row)
        part = blocks[block]
        if shift + KEPT > HALF:
            part = jnp.where(lane >= shift, part, blocks[block + 1])
        parts.append(pltpu.roll(part, HALF - shift, 1) if shift else part)
    return parts


def grid_kernel(scalars, planes_hbm, speed_ref, stats_ref, held, out_ref, passed, sums_ref, peak_ref, *apart):
    count = 2 * N
    if apart:
        planes_ref, planes_sems, sems = apart

        def came_plane(k):
            return copy_of(planes_hbm.at[:, k], planes_ref.at[:, k], planes_sems.at[k])

        loads = [copy_of(source, target, sems.at[k]) for k, (source, target) in enumerate(zip(held, passed))]
        loads[0].start()
        for k in range(PAIR):
            came_plane(k).start()
        for load in loads[1:4]:
            load.start()
        for k in range(PAIR, ROWS):
            came_plane(k).start()
        for load in loads[4:]:
            load.start()
        held = passed
    else:
        planes_ref = planes_hbm
    y_inv_ref, x_inv_ref, x_fwd_ref, y_fwd_ref = held[:4]
    peak_ref[...] = jnp.zeros_like(peak_ref)
    row = iota((count, HALF), 0)
    ky_wave = signed(row // (2 * ROWS) * ROWS + row % ROWS).astype(BF16)
    kx_wave = iota((HALF, HALF), 1).astype(F32)

    def one_pair(step, carry):
        if apart:
            for k in range(PAIR):
                came_plane(step * PAIR + k).wait()
            for load in loads[:4]:
                pl.when(step == 0)(load.wait)
        came = [planes_ref[:, step * PAIR + k].reshape(count, N) for k in range(PAIR)]
        scaled = [ky_wave * part[:, :HALF] for part in came]
        pairs = both_turns(jnp.concatenate(came + scaled, axis=1))
        y_section = [dot(y_inv_ref[turn], pairs[turn]) for turn in (0, 1)]
        x_rows = []
        for k in range(PAIR):
            starts = (k * N, PAIR * N + k * HALF, k * N + HALF)
            for which, at in enumerate(starts):
                for found in y_section:
                    halves = [found[part * HALF : (part + 1) * HALF, at : at + HALF] for part in (0, 1)]
                    if which == 0:
                        halves = [kx_wave * half for half in halves]
                    x_rows.append(jnp.concatenate(halves, axis=1).astype(BF16))
        gradients = dot(jnp.concatenate(x_rows, axis=0), x_inv_ref[...])
        fields = []
        for k in range(PAIR):
            parts = [gradients[(3 * k + d) * N : (3 * k + d + 1) * N] for d in range(3)]
            total = speed_ref[0, step * PAIR + k].astype(F32) * parts[0]
            total = total + speed_ref[1, step * PAIR + k].astype(F32) * parts[1]
            total = total + speed_ref[2, step * PAIR + k].astype(F32) * parts[2]
            fields.append(total.astype(BF16))
            square = parts[0] * parts[0] + parts[1] * parts[1] + parts[2] * parts[2]
            peak_ref[...] = jnp.maximum(peak_ref[...], jnp.max(square.reshape(N // 8, 8, N), axis=0))
        x_section = dot(jnp.concatenate(fields, axis=0), x_fwd_ref[...]).astype(BF16)
        sums = []
        for turn in (0, 1):
            columns = []
            for k in range(PAIR):
                part = x_section[k * N + turn * HALF : k * N + (turn + 1) * HALF]
                columns.append(jnp.concatenate([part[:, :HALF], part[:, HALF:]], axis=0))
            sums.append(dot(y_fwd_ref[turn], jnp.concatenate(columns, axis=1)))
        for k in range(PAIR):
            even, odd = (found[:, k * HALF : (k + 1) * HALF] for found in sums)
            sums_ref[pl.ds(row_of(step * PAIR + k), N), :] = even + odd
            sums_ref[pl.ds(row_of(step * PAIR + k, N), N), :] = even - odd
        return carry

    lax.fori_loop(0, ROWS // PAIR, one_pair, 0)
    shape = (2 * ROWS, HALF)
    peak = jnp.sqrt(jnp.max(peak_ref[...], keepdims=True))
    pieces = []
    for value in (jnp.sum(stats_ref[0], keepdims=True), jnp.sum(stats_ref[1], keepdims=True), peak):
        pieces.extend(in_three(jnp.broadcast_to(value, shape)))
    line = jnp.zeros(shape, F32)
    for k, piece in enumerate(pieces):
        line = jnp.where((iota(shape, 0) == k) & (iota(shape, 1) == LIMIT), piece, line)

    def some_peers(step, carry):
        for turn in range(SENDS):
            peer = step * SENDS + turn
            parts = []
            for row in range(ROWS):
                start = peer * 2 * ROWS + row
                real_part = sums_ref[pl.ds(start, ROWS, stride=PITCH), :]
                imag_part = sums_ref[pl.ds(start + ROWS, ROWS, stride=PITCH), :]
                parts.append(jnp.concatenate([real_part, imag_part], axis=0))
            parts[0] = parts[0] + line
            for k, block in enumerate(packed(parts)):
                at = 2 * ROWS * k
                out_ref[peer, at : at + block.shape[0], :] = block.astype(BF16)
        return carry

    lax.fori_loop(0, PEERS // SENDS, some_peers, 0)
    if apart:
        for load in loads[4:]:
            load.wait()


def tendency(came_ref, table_ref):
    count = 2 * ROWS
    blocks = [came_ref[:, k * count : (k + 1) * count, :] for k in range(BLOCKS)]
    last = came_ref[:, BLOCKS * count :, :].astype(F32)
    blocks.append(jnp.concatenate([last, pltpu.roll(last, HALF // 2, 2)], axis=1).astype(BF16))
    sums = dot(table_ref[...], jnp.concatenate([block.reshape(2 * N, HALF) for block in blocks], axis=1))
    parts = unpacked([sums[:, k * HALF : (k + 1) * HALF] for k in range(BLOCKS + 1)])
    return [(part[:N], part[N:]) for part in parts]


def middle_kernel(
    bound_ref,
    species_ref,
    base_ref,
    came_ref,
    state_ref,
    z_fwd_ref,
    z_inv_ref,
    out_ref,
    kept_ref,
    kappa_ref,
    whole_ref,
    deriv_ref,
):
    shape = (PEERS, 2 * ROWS, HALF)
    found = jnp.where(iota(shape, 2) == LIMIT, came_ref[:, : 2 * ROWS, :].astype(F32), 0.0)
    piece_row = iota(shape, 1)

    def piece(which):
        inside = jnp.where((piece_row >= 3 * which) & (piece_row < 3 * which + 3), found, 0.0)
        return jnp.sum(jnp.sum(inside, axis=1), axis=1, keepdims=True)

    def spread(value):
        return jnp.broadcast_to(value, (8, HALF))

    variance = spread(jnp.sum(piece(0), axis=0, keepdims=True)) / CELLS
    mean_grad = spread(jnp.sum(piece(1), axis=0, keepdims=True)) / CELLS
    peak = spread(jnp.max(piece(2), axis=0, keepdims=True))
    base = base_ref[species_ref[0]]
    found = base * peak * jnp.sqrt(variance) / (mean_grad + 1e-06)
    kappa_ref[0] = jnp.max(found)
    kappa = found[0:1, :]
    bound = (bound_ref[0] * bound_ref[0]).astype(F32)
    for local, (sum_real, sum_imag) in enumerate(tendency(came_ref, z_fwd_ref)):
        kz_wave, ksquare = waves_of(local)
        factor = jnp.exp(-kappa * ksquare * STEP)
        inside = ksquare <= bound
        first = [jnp.where(inside, -part, 0.0) for part in (sum_real, sum_imag)]
        middle = []
        for part in (0, 1):
            start = state_ref[part, local]
            middle.append(factor * (start + STEP * first[part]))
            kept_ref[part, local] = factor * start + (0.5 * STEP) * (factor * first[part])
        z_inverse(local, z_rows(*middle, kz_wave), z_inv_ref, whole_ref, deriv_ref)
    send_planes(0, PEERS, out_ref, whole_ref, deriv_ref)


def final_kernel(bound_ref, came_ref, kept_ref, z_fwd_ref, out_hbm, out_ref, out_sems):
    bound = (bound_ref[0] * bound_ref[0]).astype(F32)
    saves = []
    for local, sums in enumerate(tendency(came_ref, z_fwd_ref)):
        _, ksquare = waves_of(local)
        for part in (0, 1):
            second = jnp.where(ksquare <= bound, -sums[part], 0.0)
            out_ref[part, local] = kept_ref[part, local] + (0.5 * STEP) * second
        saves.append(copy_of(out_ref.at[:, local], out_hbm.at[:, local], out_sems.at[local]))
        saves[-1].start()
    for save in saves:
        save.wait()


SCALARS = pl.BlockSpec(memory_space=pltpu.SMEM)
NEAR = pl.BlockSpec(memory_space=pltpu.VMEM)
FAR = pl.BlockSpec(memory_space=pltpu.HBM)
PLANES = (PEERS, ROWS, 2 * ROWS, N)
SENT = (PEERS, 2 * ROWS * KEPT * ROWS // HALF, HALF)
STATE = (2, ROWS, N, HALF)
PAIR = 4
CHUNK = 8
UNROLL = 4
SENDS = 32


def params(mebibytes):
    return pltpu.CompilerParams(vmem_limit_bytes=mebibytes * 2**20)


def shaped(shape, dtype):
    return jax.ShapeDtypeStruct(shape, dtype)


def near(x):
    return pltpu.with_memory_space_constraint(x, pltpu.VMEM)


def far(x):
    return pltpu.with_memory_space_constraint(x, pltpu.HBM)


def sems(count):
    return pltpu.SemaphoreType.DMA((count,))


def turned():
    return pltpu.VMEM((ROWS * PITCH, HALF), F32)


BIG = pltpu.VMEM((2, N, N), BF16)
HELD = pltpu.VMEM(STATE, F32)


def gathered(velocity):
    groups = lax.axis_size("scal")
    me = lax.axis_index("scal")
    ring = 4
    high, low = me // ring, me % ring
    planes, rows = velocity.shape[1], velocity.shape[2] // 2
    velocity = velocity.reshape(3, planes, rows, 2, N).swapaxes(2, 3)

    def moved(x, change):
        return lax.ppermute(x, "scal", [(s, change(s)) for s in range(groups)])

    def beside(shift):
        return lambda s: s // ring * ring + (s + shift) % ring

    across = moved(velocity, lambda s: (s + ring) % groups)
    out = jnp.zeros((3, planes, 2, HALF, N), velocity.dtype)
    half = planes // 2

    def placed(out, x, owner, first=0):
        return lax.dynamic_update_slice(out, x, (0, first, 0, owner * rows, 0))

    for x, own in ((velocity, high), (across, 1 - high)):
        up = moved(x, beside(1))
        down = moved(x, beside(-1))
        far_up = moved(up[:, :half], beside(1))
        far_down = moved(down[:, half:], beside(-1))
        start = own * ring
        out = placed(out, x, start + low)
        out = placed(out, up, start + (low + ring - 1) % ring)
        out = placed(out, down, start + (low + 1) % ring)
        out = placed(out, far_up, start + (low + 2) % ring)
        out = placed(out, far_down, start + (low + 2) % ring, half)
    return out.reshape(3, planes, N, N)


def exchanged(x):
    return lax.all_to_all(x, "fft", 0, 0, tiled=True)


def start_call(state, table):
    return pl.pallas_call(
        start_kernel,
        in_specs=[FAR, FAR],
        out_specs=[FAR, NEAR],
        out_shape=[pltpu.HBM(PLANES, BF16), pltpu.VMEM((2, 8, HALF), F32)],
        scratch_shapes=[HELD, BIG, pltpu.VMEM(PLANES, BF16), turned(), turned(), sems(ROWS + 1), sems(PEERS // CHUNK)],
        compiler_params=params(24),
        name="start",
    )(far(state), far(table["z_inv"]))


def grid_call(scalars, planes, speeds, stats, held, apart):
    scratch = [turned(), pltpu.VMEM((8, N), F32)]
    passed = held if apart else ()
    if apart:
        scratch += [pltpu.VMEM(PLANES, BF16), sems(ROWS), sems(len(held))]
    spec, place = (FAR, far) if apart else (NEAR, near)
    return pl.pallas_call(
        grid_kernel,
        in_specs=[(SCALARS,) * len(scalars), spec, NEAR, NEAR, (spec,) * len(held)],
        out_specs=[NEAR, (NEAR,) * len(passed)],
        out_shape=[pltpu.VMEM(SENT, BF16), tuple(pltpu.VMEM(x.shape, x.dtype) for x in passed)],
        scratch_shapes=scratch,
        compiler_params=params(24),
        name="grid",
    )(scalars, place(planes), near(speeds), near(stats), tuple(place(x) for x in held))


def middle_call(scalars, came, state, z_fwd, z_inv):
    return pl.pallas_call(
        middle_kernel,
        in_specs=[SCALARS] * 3 + [NEAR] * 4,
        out_specs=[NEAR, NEAR, SCALARS],
        out_shape=[pltpu.VMEM(PLANES, BF16), pltpu.VMEM(STATE, F32), shaped((1,), F32)],
        scratch_shapes=[turned(), turned()],
        compiler_params=params(24),
        name="middle",
    )(*scalars, *(near(x) for x in (came, state, z_fwd, z_inv)))


def final_call(bound, came, kept, z_fwd):
    return pl.pallas_call(
        final_kernel,
        in_specs=[SCALARS, NEAR, NEAR, NEAR],
        out_specs=FAR,
        out_shape=pltpu.HBM(STATE, F32),
        scratch_shapes=[HELD, sems(ROWS)],
        compiler_params=params(24),
        name="final",
    )(bound, near(came), near(kept), near(z_fwd))


def body(scalar_state, velocity, species, kappa_table, dealias_bound):
    table = tables()
    state = scalar_state[0]
    speeds = gathered(velocity)
    planes, stats = start_call(state, table)
    scalars = (dealias_bound, species, kappa_table)
    held = tuple(table[name] for name in ("y_inv", "x_inv", "x_fwd", "y_fwd", "z_fwd", "z_inv")) + (state,)
    sent, held = grid_call(scalars, exchanged(planes), speeds, stats, held, True)
    *grid_tables, z_fwd, z_inv, state = held
    planes, kept, kappa = middle_call(scalars, exchanged(sent), state, z_fwd, z_inv)
    sent, _ = grid_call((), exchanged(planes), speeds, stats, tuple(grid_tables), False)
    return (final_call(dealias_bound, exchanged(sent), kept, z_fwd)[None], kappa)


def solution(mesh):
    placed = (
        P("scal", None, "fft", None, None),
        P(None, "fft", "scal", None),
        P("scal"),
        P(),
        P("scal"),
    )
    return jax.shard_map(
        body,
        mesh=mesh,
        in_specs=placed,
        out_specs=(P("scal", None, "fft", None, None), P("scal")),
        check_vma=False,
    )
```

```python
import math

import jax
import jax.numpy as jnp
import numpy as np
from jax import lax
from jax.experimental import pallas as pl
from jax.experimental.pallas import tpu as pltpu
from jax.sharding import PartitionSpec as P

N = 256
HALF = 128
PEERS = 32
ROWS = N // PEERS
KEPT = 88
LIMIT = 86
BLOCKS = ROWS * KEPT // HALF
PITCH = 2 * N + 4
STEP = 0.2 * 2.0 * math.pi / N
CELLS = float(N) ** 3
F32 = jnp.float32
BF16 = jnp.bfloat16


def tables():
    def cos_sin(rows, columns):
        angles = (rows[:, None] * columns[None, :] % N).astype(np.float32) * np.float32(2.0 * math.pi / N)
        scale = np.float32(1.0 / math.sqrt(N))
        return np.cos(angles) * scale, np.sin(angles) * scale

    def inverse(rows, columns):
        cos, sin = cos_sin(rows, columns)
        return np.block([[cos, -sin], [sin, cos]])

    def forward(rows, columns):
        cos, sin = cos_sin(rows, columns)
        return np.block([[cos, sin], [-sin, cos]])

    def order(peers):
        return np.arange(2 * peers * ROWS).reshape(2, peers, ROWS).transpose(1, 0, 2).reshape(-1)

    index, low = np.arange(N), np.arange(HALF)
    cos, sin = cos_sin(index, low)
    weight = np.where(low == 0, 1.0, 2.0).astype(np.float32)[:, None]
    keep = (low < LIMIT).astype(np.float32)[None, :]
    halves = order(PEERS // 2)
    listed = {
        "z_inv": np.stack([inverse(2 * low + turn, low) for turn in (0, 1)]),
        "y_inv": np.stack([inverse(2 * low + turn, low)[:, halves] for turn in (0, 1)]),
        "x_inv": np.concatenate([-weight * sin.T, -weight * cos.T], axis=0),
        "x_fwd": np.concatenate([cos * keep, -sin * keep], axis=1),
        "y_fwd": np.stack([forward(low, 2 * low + turn)[halves] for turn in (0, 1)]),
        "z_fwd": forward(np.concatenate([index[:KEPT], index[-KEPT:]]), index)[:, order(PEERS)],
    }
    return {name: jnp.asarray(value.astype(np.float32)).astype(BF16) for name, value in listed.items()}


def both_turns(x):
    low, high = x[: x.shape[0] // 2], x[x.shape[0] // 2 :]
    return low + high, low - high


def dot(left, right):
    return jnp.dot(left, right, preferred_element_type=F32)


def iota(shape, dim):
    return lax.broadcasted_iota(jnp.int32, shape, dim)


def signed(index):
    return jnp.where(index < HALF, index, index - N).astype(F32)


def z_rows(real_part, imag_part, kz_wave):
    columns = [
        [jnp.concatenate(pair, axis=0).astype(BF16) for pair in zip(both_turns(real), both_turns(imag))]
        for real, imag in ((real_part, imag_part), (kz_wave * real_part, kz_wave * imag_part))
    ]
    return [jnp.concatenate(pair, axis=1) for pair in zip(*columns)]


def send_planes(first, count, planes_ref, whole_ref, deriv_ref):
    def some_peers(step, carry):
        for turn in range(UNROLL):
            peer = first + step * UNROLL + turn
            for local in range(ROWS):
                for at, ref in ((0, whole_ref), (HALF, deriv_ref)):
                    start = local % 2 * N + peer * (ROWS // 2) + local // 2
                    real_part = ref[pl.ds(start, ROWS, stride=PITCH), :]
                    imag_part = ref[pl.ds(start + HALF, ROWS, stride=PITCH), :]
                    tile = jnp.concatenate([real_part, imag_part], axis=0).astype(BF16)
                    planes_ref[peer, local, :, at : at + HALF] = tile
        return carry

    lax.fori_loop(0, count // UNROLL, some_peers, 0)


def row_of(block, shift=0):
    return block * PITCH + shift if isinstance(block, int) else pl.multiple_of(block * PITCH + shift, 4)


def z_inverse(local, rows, table_ref, whole_ref, deriv_ref):
    for turn in (0, 1):
        found = dot(table_ref[turn], rows[turn])
        part = pl.ds(row_of(local, turn * N), N)
        whole_ref[part, :] = found[:, :HALF]
        deriv_ref[part, :] = found[:, HALF:]


def waves_of(local):
    ky_wave = signed(lax.axis_index("fft").astype(jnp.int32) * ROWS + local)
    kz_wave = signed(iota((N, HALF), 0))
    kx_wave = iota((N, HALF), 1).astype(F32)
    return kz_wave, kx_wave * kx_wave + ky_wave * ky_wave + kz_wave * kz_wave


def copy_of(source, target, sem):
    return pltpu.make_async_copy(source, target, sem)


def start_kernel(
    state_hbm, table_hbm, out_hbm, stats_ref, state_ref, table_ref, planes_ref, whole_ref, deriv_ref, in_sems, out_sems
):
    loads = [copy_of(table_hbm, table_ref, in_sems.at[ROWS])]
    loads += [copy_of(state_hbm.at[:, k], state_ref.at[:, k], in_sems.at[k]) for k in range(ROWS)]
    for load in loads:
        load.start()
    stats_ref[...] = jnp.zeros_like(stats_ref)
    loads[0].wait()

    def one_row(local, carry):
        copy_of(state_hbm.at[:, local], state_ref.at[:, local], in_sems.at[local]).wait()
        kz_wave, ksquare = waves_of(local)
        real_part = state_ref[0, local]
        imag_part = state_ref[1, local]
        weight = jnp.where(iota((N, HALF), 1) == 0, 1.0, 2.0)
        energy = weight * (real_part * real_part + imag_part * imag_part)
        stats_ref[0] += jnp.sum(energy.reshape(N // 8, 8, HALF), axis=0)
        stats_ref[1] += jnp.sum((ksquare * energy).reshape(N // 8, 8, HALF), axis=0)
        z_inverse(local, z_rows(real_part, imag_part, kz_wave), table_ref, whole_ref, deriv_ref)
        return carry

    lax.fori_loop(0, ROWS, one_row, 0)

    def leaving(k):
        part = pl.ds(k * CHUNK, CHUNK)
        return copy_of(planes_ref.at[part], out_hbm.at[part], out_sems.at[k])

    def one_chunk(k, carry):
        send_planes(k * CHUNK, CHUNK, planes_ref, whole_ref, deriv_ref)
        leaving(k).start()
        return carry

    lax.fori_loop(0, PEERS // CHUNK, one_chunk, 0)
    for k in range(PEERS // CHUNK):
        leaving(k).wait()


def in_three(value):
    high = value.astype(BF16).astype(F32)
    rest = value - high
    middle = rest.astype(BF16).astype(F32)
    return high, middle, (rest - middle).astype(BF16).astype(F32)


def place_of(row):
    return row * KEPT // HALF, row * KEPT % HALF


def packed(parts):
    lane = iota((2 * ROWS, HALF), 1)
    blocks = [None] * (BLOCKS + 1)
    for row, part in enumerate(parts):
        block, shift = place_of(row)
        turned = pltpu.roll(part, shift, 1) if shift else part
        blocks[block] = turned if shift == 0 else jnp.where(lane < shift, blocks[block], turned)
        if shift + KEPT > HALF:
            blocks[block + 1] = turned
    real_part, imag_part = blocks[BLOCKS][:ROWS], blocks[BLOCKS][ROWS:]
    blocks[BLOCKS] = jnp.where(lane[:ROWS] < HALF // 2, real_part, pltpu.roll(imag_part, HALF // 2, 1))
    return blocks


def unpacked(blocks):
    lane = iota(blocks[0].shape, 1)
    parts = []
    for row in range(ROWS):
        block, shift = place_of(row)
        part = blocks[block]
        if shift + KEPT > HALF:
            part = jnp.where(lane >= shift, part, blocks[block + 1])
        parts.append(pltpu.roll(part, HALF - shift, 1) if shift else part)
    return parts


def grid_kernel(scalars, planes_hbm, speed_ref, stats_ref, held, out_ref, passed, sums_ref, peak_ref, *apart):
    count = 2 * N
    if apart:
        planes_ref, planes_sems, sems = apart

        def came_plane(k):
            return copy_of(planes_hbm.at[:, k], planes_ref.at[:, k], planes_sems.at[k])

        loads = [copy_of(source, target, sems.at[k]) for k, (source, target) in enumerate(zip(held, passed))]
        loads[0].start()
        for k in range(PAIR):
            came_plane(k).start()
        for load in loads[1:4]:
            load.start()
        for k in range(PAIR, ROWS):
            came_plane(k).start()
        for load in loads[4:]:
            load.start()
        held = passed
    else:
        planes_ref = planes_hbm
    y_inv_ref, x_inv_ref, x_fwd_ref, y_fwd_ref = held[:4]
    peak_ref[...] = jnp.zeros_like(peak_ref)
    row = iota((count, HALF), 0)
    ky_wave = signed(row // (2 * ROWS) * ROWS + row % ROWS).astype(BF16)
    kx_wave = iota((HALF, HALF), 1).astype(F32)

    def one_pair(step):
        if apart:
            for k in range(PAIR):
                came_plane(step * PAIR + k).wait()
        came = [planes_ref[:, step * PAIR + k].reshape(count, N) for k in range(PAIR)]
        scaled = [ky_wave * part[:, :HALF] for part in came]
        pairs = both_turns(jnp.concatenate(came + scaled, axis=1))
        if apart and step == 0:
            loads[0].wait()
        y_section = [dot(y_inv_ref[turn], pairs[turn]) for turn in (0, 1)]
        x_rows = []
        for k in range(PAIR):
            starts = (k * N, PAIR * N + k * HALF, k * N + HALF)
            for which, at in enumerate(starts):
                for found in y_section:
                    halves = [found[part * HALF : (part + 1) * HALF, at : at + HALF] for part in (0, 1)]
                    if which == 0:
                        halves = [kx_wave * half for half in halves]
                    x_rows.append(jnp.concatenate(halves, axis=1).astype(BF16))
        if apart and step == 0:
            for load in loads[1:4]:
                load.wait()
        gradients = dot(jnp.concatenate(x_rows, axis=0), x_inv_ref[...])
        fields = []
        for k in range(PAIR):
            parts = [gradients[(3 * k + d) * N : (3 * k + d + 1) * N] for d in range(3)]
            total = speed_ref[0, step * PAIR + k].astype(F32) * parts[0]
            total = total + speed_ref[1, step * PAIR + k].astype(F32) * parts[1]
            total = total + speed_ref[2, step * PAIR + k].astype(F32) * parts[2]
            fields.append(total.astype(BF16))
            square = parts[0] * parts[0] + parts[1] * parts[1] + parts[2] * parts[2]
            peak_ref[...] = jnp.maximum(peak_ref[...], jnp.max(square.reshape(N // 8, 8, N), axis=0))
        x_section = dot(jnp.concatenate(fields, axis=0), x_fwd_ref[...]).astype(BF16)
        sums = []
        for turn in (0, 1):
            columns = []
            for k in range(PAIR):
                part = x_section[k * N + turn * HALF : k * N + (turn + 1) * HALF]
                columns.append(jnp.concatenate([part[:, :HALF], part[:, HALF:]], axis=0))
            sums.append(dot(y_fwd_ref[turn], jnp.concatenate(columns, axis=1)))
        for k in range(PAIR):
            even, odd = (found[:, k * HALF : (k + 1) * HALF] for found in sums)
            sums_ref[pl.ds(row_of(step * PAIR + k), N), :] = even + odd
            sums_ref[pl.ds(row_of(step * PAIR + k, N), N), :] = even - odd

    for step in range(ROWS // PAIR):
        one_pair(step)
    shape = (2 * ROWS, HALF)
    peak = jnp.sqrt(jnp.max(peak_ref[...], keepdims=True))
    pieces = []
    for value in (jnp.sum(stats_ref[0], keepdims=True), jnp.sum(stats_ref[1], keepdims=True), peak):
        pieces.extend(in_three(jnp.broadcast_to(value, shape)))
    line = jnp.zeros(shape, F32)
    for k, piece in enumerate(pieces):
        line = jnp.where((iota(shape, 0) == k) & (iota(shape, 1) == LIMIT), piece, line)

    def some_peers(step, carry):
        for turn in range(SENDS):
            peer = step * SENDS + turn
            parts = []
            for row in range(ROWS):
                start = peer * 2 * ROWS + row
                real_part = sums_ref[pl.ds(start, ROWS, stride=PITCH), :]
                imag_part = sums_ref[pl.ds(start + ROWS, ROWS, stride=PITCH), :]
                parts.append(jnp.concatenate([real_part, imag_part], axis=0))
            parts[0] = parts[0] + line
            for k, block in enumerate(packed(parts)):
                at = 2 * ROWS * k
                out_ref[peer, at : at + block.shape[0], :] = block.astype(BF16)
        return carry

    lax.fori_loop(0, PEERS // SENDS, some_peers, 0)
    if apart:
        for load in loads[4:]:
            load.wait()


def tendency(came_ref, table_ref):
    count = 2 * ROWS
    blocks = [came_ref[:, k * count : (k + 1) * count, :] for k in range(BLOCKS)]
    last = came_ref[:, BLOCKS * count :, :].astype(F32)
    blocks.append(jnp.concatenate([last, pltpu.roll(last, HALF // 2, 2)], axis=1).astype(BF16))
    sums = dot(table_ref[...], jnp.concatenate([block.reshape(2 * N, HALF) for block in blocks], axis=1))
    parts = unpacked([sums[:, k * HALF : (k + 1) * HALF] for k in range(BLOCKS + 1)])
    between = jnp.zeros((N - 2 * KEPT, HALF), F32)
    cut = [[part[k * KEPT : (k + 1) * KEPT] for k in range(4)] for part in parts]
    return [tuple(jnp.concatenate([c[k], between, c[k + 1]], axis=0) for k in (0, 2)) for c in cut]


def middle_kernel(
    bound_ref,
    species_ref,
    base_ref,
    came_ref,
    state_ref,
    z_fwd_ref,
    z_inv_ref,
    out_ref,
    kept_ref,
    kappa_ref,
    whole_ref,
    deriv_ref,
):
    shape = (PEERS, 2 * ROWS, HALF)
    found = jnp.where(iota(shape, 2) == LIMIT, came_ref[:, : 2 * ROWS, :].astype(F32), 0.0)
    piece_row = iota(shape, 1)

    def piece(which):
        inside = jnp.where((piece_row >= 3 * which) & (piece_row < 3 * which + 3), found, 0.0)
        return jnp.sum(jnp.sum(inside, axis=1), axis=1, keepdims=True)

    def spread(value):
        return jnp.broadcast_to(value, (8, HALF))

    variance = spread(jnp.sum(piece(0), axis=0, keepdims=True)) / CELLS
    mean_grad = spread(jnp.sum(piece(1), axis=0, keepdims=True)) / CELLS
    peak = spread(jnp.max(piece(2), axis=0, keepdims=True))
    base = base_ref[species_ref[0]]
    found = base * peak * jnp.sqrt(variance) / (mean_grad + 1e-06)
    kappa_ref[0] = jnp.max(found)
    kappa = found[0:1, :]
    bound = (bound_ref[0] * bound_ref[0]).astype(F32)
    for local, (sum_real, sum_imag) in enumerate(tendency(came_ref, z_fwd_ref)):
        kz_wave, ksquare = waves_of(local)
        factor = jnp.exp(-kappa * ksquare * STEP)
        inside = ksquare <= bound
        first = [jnp.where(inside, -part, 0.0) for part in (sum_real, sum_imag)]
        middle = []
        for part in (0, 1):
            start = state_ref[part, local]
            middle.append(factor * (start + STEP * first[part]))
            kept_ref[part, local] = factor * start + (0.5 * STEP) * (factor * first[part])
        z_inverse(local, z_rows(*middle, kz_wave), z_inv_ref, whole_ref, deriv_ref)
    send_planes(0, PEERS, out_ref, whole_ref, deriv_ref)


def final_kernel(bound_ref, came_ref, kept_ref, z_fwd_ref, out_hbm, out_ref, out_sems):
    bound = (bound_ref[0] * bound_ref[0]).astype(F32)
    saves = []
    for local, sums in enumerate(tendency(came_ref, z_fwd_ref)):
        _, ksquare = waves_of(local)
        for part in (0, 1):
            second = jnp.where(ksquare <= bound, -sums[part], 0.0)
            out_ref[part, local] = kept_ref[part, local] + (0.5 * STEP) * second
        saves.append(copy_of(out_ref.at[:, local], out_hbm.at[:, local], out_sems.at[local]))
        saves[-1].start()
    for save in saves:
        save.wait()


SCALARS = pl.BlockSpec(memory_space=pltpu.SMEM)
NEAR = pl.BlockSpec(memory_space=pltpu.VMEM)
FAR = pl.BlockSpec(memory_space=pltpu.HBM)
PLANES = (PEERS, ROWS, 2 * ROWS, N)
SENT = (PEERS, 2 * ROWS * KEPT * ROWS // HALF, HALF)
STATE = (2, ROWS, N, HALF)
PAIR = 4
CHUNK = 8
UNROLL = 4
SENDS = 32


def params(mebibytes):
    return pltpu.CompilerParams(vmem_limit_bytes=mebibytes * 2**20)


def shaped(shape, dtype):
    return jax.ShapeDtypeStruct(shape, dtype)


def near(x):
    return pltpu.with_memory_space_constraint(x, pltpu.VMEM)


def far(x):
    return pltpu.with_memory_space_constraint(x, pltpu.HBM)


def sems(count):
    return pltpu.SemaphoreType.DMA((count,))


def turned():
    return pltpu.VMEM((ROWS * PITCH, HALF), F32)


BIG = pltpu.VMEM((2, N, N), BF16)
HELD = pltpu.VMEM(STATE, F32)


def gathered(velocity):
    groups = lax.axis_size("scal")
    me = lax.axis_index("scal")
    ring = 4
    high, low = me // ring, me % ring
    planes, rows = velocity.shape[1], velocity.shape[2] // 2
    velocity = velocity.reshape(3, planes, rows, 2, N).swapaxes(2, 3)

    def moved(x, change):
        return lax.ppermute(x, "scal", [(s, change(s)) for s in range(groups)])

    def beside(shift):
        return lambda s: s // ring * ring + (s + shift) % ring

    across = moved(velocity, lambda s: (s + ring) % groups)
    out = jnp.zeros((3, planes, 2, HALF, N), velocity.dtype)
    half = planes // 2

    def placed(out, x, owner, first=0):
        return lax.dynamic_update_slice(out, x, (0, first, 0, owner * rows, 0))

    for x, own in ((velocity, high), (across, 1 - high)):
        up = moved(x, beside(1))
        down = moved(x, beside(-1))
        far_up = moved(up[:, :half], beside(1))
        far_down = moved(down[:, half:], beside(-1))
        start = own * ring
        out = placed(out, x, start + low)
        out = placed(out, up, start + (low + ring - 1) % ring)
        out = placed(out, down, start + (low + 1) % ring)
        out = placed(out, far_up, start + (low + 2) % ring)
        out = placed(out, far_down, start + (low + 2) % ring, half)
    return out.reshape(3, planes, N, N)


def exchanged(x):
    return lax.all_to_all(x, "fft", 0, 0, tiled=True)


def start_call(state, table):
    return pl.pallas_call(
        start_kernel,
        in_specs=[FAR, FAR],
        out_specs=[FAR, NEAR],
        out_shape=[pltpu.HBM(PLANES, BF16), pltpu.VMEM((2, 8, HALF), F32)],
        scratch_shapes=[HELD, BIG, pltpu.VMEM(PLANES, BF16), turned(), turned(), sems(ROWS + 1), sems(PEERS // CHUNK)],
        compiler_params=params(24),
        name="start",
    )(far(state), far(table["z_inv"]))


def grid_call(scalars, planes, speeds, stats, held, apart):
    scratch = [turned(), pltpu.VMEM((8, N), F32)]
    passed = held if apart else ()
    if apart:
        scratch += [pltpu.VMEM(PLANES, BF16), sems(ROWS), sems(len(held))]
    spec, place = (FAR, far) if apart else (NEAR, near)
    return pl.pallas_call(
        grid_kernel,
        in_specs=[(SCALARS,) * len(scalars), spec, NEAR, NEAR, (spec,) * len(held)],
        out_specs=[NEAR, (NEAR,) * len(passed)],
        out_shape=[pltpu.VMEM(SENT, BF16), tuple(pltpu.VMEM(x.shape, x.dtype) for x in passed)],
        scratch_shapes=scratch,
        compiler_params=params(24),
        name="grid",
    )(scalars, place(planes), near(speeds), near(stats), tuple(place(x) for x in held))


def middle_call(scalars, came, state, z_fwd, z_inv):
    return pl.pallas_call(
        middle_kernel,
        in_specs=[SCALARS] * 3 + [NEAR] * 4,
        out_specs=[NEAR, NEAR, SCALARS],
        out_shape=[pltpu.VMEM(PLANES, BF16), pltpu.VMEM(STATE, F32), shaped((1,), F32)],
        scratch_shapes=[turned(), turned()],
        compiler_params=params(24),
        name="middle",
    )(*scalars, *(near(x) for x in (came, state, z_fwd, z_inv)))


def final_call(bound, came, kept, z_fwd):
    return pl.pallas_call(
        final_kernel,
        in_specs=[SCALARS, NEAR, NEAR, NEAR],
        out_specs=FAR,
        out_shape=pltpu.HBM(STATE, F32),
        scratch_shapes=[HELD, sems(ROWS)],
        compiler_params=params(24),
        name="final",
    )(bound, near(came), near(kept), near(z_fwd))


def body(scalar_state, velocity, species, kappa_table, dealias_bound):
    table = tables()
    state = scalar_state[0]
    speeds = gathered(velocity)
    planes, stats = start_call(state, table)
    scalars = (dealias_bound, species, kappa_table)
    held = tuple(table[name] for name in ("y_inv", "x_inv", "x_fwd", "y_fwd", "z_fwd", "z_inv")) + (state,)
    sent, held = grid_call(scalars, exchanged(planes), speeds, stats, held, True)
    *grid_tables, z_fwd, z_inv, state = held
    planes, kept, kappa = middle_call(scalars, exchanged(sent), state, z_fwd, z_inv)
    sent, _ = grid_call((), exchanged(planes), speeds, stats, tuple(grid_tables), False)
    return (final_call(dealias_bound, exchanged(sent), kept, z_fwd)[None], kappa)


def solution(mesh):
    placed = (
        P("scal", None, "fft", None, None),
        P(None, "fft", "scal", None),
        P("scal"),
        P(),
        P("scal"),
    )
    return jax.shard_map(
        body,
        mesh=mesh,
        in_specs=placed,
        out_specs=(P("scal", None, "fft", None, None), P("scal")),
        check_vma=False,
    )
```

```python
import math

import jax
import jax.numpy as jnp
import numpy as np
from jax import lax
from jax.experimental import pallas as pl
from jax.experimental.pallas import tpu as pltpu
from jax.sharding import PartitionSpec as P

N = 256
HALF = 128
PEERS = 32
ROWS = N // PEERS
KEPT = 88
LIMIT = 86
BLOCKS = ROWS * KEPT // HALF
PITCH = 2 * N + 4
STEP = 0.2 * 2.0 * math.pi / N
CELLS = float(N) ** 3
F32 = jnp.float32
BF16 = jnp.bfloat16


def tables():
    def cos_sin(rows, columns):
        angles = (rows[:, None] * columns[None, :] % N).astype(np.float32) * np.float32(2.0 * math.pi / N)
        scale = np.float32(1.0 / math.sqrt(N))
        return np.cos(angles) * scale, np.sin(angles) * scale

    def inverse(rows, columns):
        cos, sin = cos_sin(rows, columns)
        return np.block([[cos, -sin], [sin, cos]])

    def forward(rows, columns):
        cos, sin = cos_sin(rows, columns)
        return np.block([[cos, sin], [-sin, cos]])

    def order(peers):
        return np.arange(2 * peers * ROWS).reshape(2, peers, ROWS).transpose(1, 0, 2).reshape(-1)

    index, low = np.arange(N), np.arange(HALF)
    cos, sin = cos_sin(index, low)
    weight = np.where(low == 0, 1.0, 2.0).astype(np.float32)[:, None]
    keep = (low < LIMIT).astype(np.float32)[None, :]
    halves = order(PEERS // 2)
    listed = {
        "z_inv": np.stack([inverse(2 * low + turn, low) for turn in (0, 1)]),
        "y_inv": np.stack([inverse(2 * low + turn, low)[:, halves] for turn in (0, 1)]),
        "x_inv": np.concatenate([-weight * sin.T, -weight * cos.T], axis=0),
        "x_fwd": np.concatenate([cos * keep, -sin * keep], axis=1),
        "y_fwd": np.stack([forward(low, 2 * low + turn)[halves] for turn in (0, 1)]),
        "z_fwd": forward(np.concatenate([index[:KEPT], index[-KEPT:]]), index)[:, order(PEERS)],
    }
    return {name: jnp.asarray(value.astype(np.float32)).astype(BF16) for name, value in listed.items()}


def both_turns(x):
    low, high = x[: x.shape[0] // 2], x[x.shape[0] // 2 :]
    return low + high, low - high


def dot(left, right):
    return jnp.dot(left, right, preferred_element_type=F32)


def iota(shape, dim):
    return lax.broadcasted_iota(jnp.int32, shape, dim)


def signed(index):
    return jnp.where(index < HALF, index, index - N).astype(F32)


def z_rows(real_part, imag_part, kz_wave):
    columns = [
        [jnp.concatenate(pair, axis=0).astype(BF16) for pair in zip(both_turns(real), both_turns(imag))]
        for real, imag in ((real_part, imag_part), (kz_wave * real_part, kz_wave * imag_part))
    ]
    return [jnp.concatenate(pair, axis=1) for pair in zip(*columns)]


def send_planes(first, count, unroll, planes_ref, whole_ref, deriv_ref):
    def some_peers(step, carry):
        for turn in range(unroll):
            peer = first + step * unroll + turn
            for local in range(ROWS):
                for at, ref in ((0, whole_ref), (HALF, deriv_ref)):
                    start = local % 2 * N + peer * (ROWS // 2) + local // 2
                    real_part = ref[pl.ds(start, ROWS, stride=PITCH), :]
                    imag_part = ref[pl.ds(start + HALF, ROWS, stride=PITCH), :]
                    tile = jnp.concatenate([real_part, imag_part], axis=0).astype(BF16)
                    planes_ref[peer, local, :, at : at + HALF] = tile
        return carry

    lax.fori_loop(0, count // unroll, some_peers, 0)


def row_of(block, shift=0):
    return block * PITCH + shift if isinstance(block, int) else pl.multiple_of(block * PITCH + shift, 4)


def z_inverse(local, rows, table_ref, whole_ref, deriv_ref):
    for turn in (0, 1):
        found = dot(table_ref[turn], rows[turn])
        part = pl.ds(row_of(local, turn * N), N)
        whole_ref[part, :] = found[:, :HALF]
        deriv_ref[part, :] = found[:, HALF:]


def across_z(local):
    ky_wave = signed(lax.axis_index("fft").astype(jnp.int32) * ROWS + local)
    kx_wave = iota((1, HALF), 1).astype(F32)
    return kx_wave * kx_wave + ky_wave * ky_wave


def waves_of(local):
    kz_wave = signed(iota((N, HALF), 0))
    return kz_wave, across_z(local) + kz_wave * kz_wave


def copy_of(source, target, sem):
    return pltpu.make_async_copy(source, target, sem)


def start_kernel(
    state_hbm, table_hbm, out_hbm, stats_ref, state_ref, table_ref, planes_ref, whole_ref, deriv_ref, in_sems, out_sems
):
    loads = [copy_of(table_hbm, table_ref, in_sems.at[ROWS])]
    loads += [copy_of(state_hbm.at[:, k], state_ref.at[:, k], in_sems.at[k]) for k in range(ROWS)]
    for load in loads:
        load.start()
    stats_ref[...] = jnp.zeros_like(stats_ref)
    loads[0].wait()

    def one_row(local, carry):
        copy_of(state_hbm.at[:, local], state_ref.at[:, local], in_sems.at[local]).wait()
        kz_wave, ksquare = waves_of(local)
        real_part = state_ref[0, local]
        imag_part = state_ref[1, local]
        weight = jnp.where(iota((N, HALF), 1) == 0, 1.0, 2.0)
        energy = weight * (real_part * real_part + imag_part * imag_part)
        stats_ref[0] += jnp.sum(energy.reshape(N // 8, 8, HALF), axis=0)
        stats_ref[1] += jnp.sum((ksquare * energy).reshape(N // 8, 8, HALF), axis=0)
        z_inverse(local, z_rows(real_part, imag_part, kz_wave), table_ref, whole_ref, deriv_ref)
        return carry

    lax.fori_loop(0, ROWS, one_row, 0, unroll=2)

    def leaving(k):
        part = pl.ds(k * CHUNK, CHUNK)
        return copy_of(planes_ref.at[part], out_hbm.at[part], out_sems.at[k])

    def one_chunk(k, carry):
        send_planes(k * CHUNK, CHUNK, UNROLL, planes_ref, whole_ref, deriv_ref)
        leaving(k).start()
        return carry

    lax.fori_loop(0, PEERS // CHUNK, one_chunk, 0)
    for k in range(PEERS // CHUNK):
        leaving(k).wait()


def in_three(value):
    high = value.astype(BF16).astype(F32)
    rest = value - high
    middle = rest.astype(BF16).astype(F32)
    return high, middle, (rest - middle).astype(BF16).astype(F32)


def place_of(row):
    return row * KEPT // HALF, row * KEPT % HALF


def packed(parts):
    lane = iota((2 * ROWS, HALF), 1)
    blocks = [None] * (BLOCKS + 1)
    for row, part in enumerate(parts):
        block, shift = place_of(row)
        turned = pltpu.roll(part, shift, 1) if shift else part
        blocks[block] = turned if shift == 0 else jnp.where(lane < shift, blocks[block], turned)
        if shift + KEPT > HALF:
            blocks[block + 1] = turned
    real_part, imag_part = blocks[BLOCKS][:ROWS], blocks[BLOCKS][ROWS:]
    blocks[BLOCKS] = jnp.where(lane[:ROWS] < HALF // 2, real_part, pltpu.roll(imag_part, HALF // 2, 1))
    return blocks


def unpacked(blocks):
    lane = iota(blocks[0].shape, 1)
    parts = []
    for row in range(ROWS):
        block, shift = place_of(row)
        part = blocks[block]
        if shift + KEPT > HALF:
            part = jnp.where(lane >= shift, part, blocks[block + 1])
        parts.append(pltpu.roll(part, HALF - shift, 1) if shift else part)
    return parts


def grid_kernel(scalars, planes_hbm, speed_ref, stats_ref, held, out_ref, passed, sums_ref, peak_ref, *apart):
    count = 2 * N
    if apart:
        planes_ref, planes_sems, sems = apart

        def came_plane(k):
            return copy_of(planes_hbm.at[:, k], planes_ref.at[:, k], planes_sems.at[k])

        loads = [copy_of(source, target, sems.at[k]) for k, (source, target) in enumerate(zip(held, passed))]
        loads[0].start()
        for k in range(PAIR):
            came_plane(k).start()
        for load in loads[1:4]:
            load.start()
        for k in range(PAIR, ROWS):
            came_plane(k).start()
        for load in loads[4:]:
            load.start()
        held = passed
    else:
        planes_ref = planes_hbm
    y_inv_ref, x_inv_ref, x_fwd_ref, y_fwd_ref = held[:4]
    peak_ref[...] = jnp.zeros_like(peak_ref)
    row = iota((count, HALF), 0)
    ky_wave = signed(row // (2 * ROWS) * ROWS + row % ROWS).astype(BF16)
    kx_wave = iota((HALF, HALF), 1).astype(F32)

    def one_pair(step):
        if apart:
            for k in range(PAIR):
                came_plane(step * PAIR + k).wait()
        came = [planes_ref[:, step * PAIR + k].reshape(count, N) for k in range(PAIR)]
        scaled = [ky_wave * part[:, :HALF] for part in came]
        pairs = both_turns(jnp.concatenate(came + scaled, axis=1))
        if apart and step == 0:
            loads[0].wait()
        y_section = [dot(y_inv_ref[turn], pairs[turn]) for turn in (0, 1)]
        x_rows = []
        for k in range(PAIR):
            starts = (k * N, PAIR * N + k * HALF, k * N + HALF)
            for which, at in enumerate(starts):
                for found in y_section:
                    halves = [found[part * HALF : (part + 1) * HALF, at : at + HALF] for part in (0, 1)]
                    if which == 0:
                        halves = [kx_wave * half for half in halves]
                    x_rows.append(jnp.concatenate(halves, axis=1).astype(BF16))
        if apart and step == 0:
            for load in loads[1:4]:
                load.wait()
        gradients = dot(jnp.concatenate(x_rows, axis=0), x_inv_ref[...])
        fields = []
        for k in range(PAIR):
            parts = [gradients[(3 * k + d) * N : (3 * k + d + 1) * N] for d in range(3)]
            total = speed_ref[0, step * PAIR + k].astype(F32) * parts[0]
            total = total + speed_ref[1, step * PAIR + k].astype(F32) * parts[1]
            total = total + speed_ref[2, step * PAIR + k].astype(F32) * parts[2]
            fields.append(total.astype(BF16))
            if apart:
                square = parts[0] * parts[0] + parts[1] * parts[1] + parts[2] * parts[2]
                peak_ref[...] = jnp.maximum(peak_ref[...], jnp.max(square.reshape(N // 8, 8, N), axis=0))
        x_section = dot(jnp.concatenate(fields, axis=0), x_fwd_ref[...]).astype(BF16)
        sums = []
        for turn in (0, 1):
            columns = []
            for k in range(PAIR):
                part = x_section[k * N + turn * HALF : k * N + (turn + 1) * HALF]
                columns.append(jnp.concatenate([part[:, :HALF], part[:, HALF:]], axis=0))
            sums.append(dot(y_fwd_ref[turn], jnp.concatenate(columns, axis=1)))
        for k in range(PAIR):
            even, odd = (found[:, k * HALF : (k + 1) * HALF] for found in sums)
            sums_ref[pl.ds(row_of(step * PAIR + k), N), :] = even + odd
            sums_ref[pl.ds(row_of(step * PAIR + k, N), N), :] = even - odd

    for step in range(ROWS // PAIR):
        one_pair(step)
    if apart:
        shape = (2 * ROWS, HALF)
        peak = jnp.sqrt(jnp.max(peak_ref[...], keepdims=True))
        pieces = []
        for value in (jnp.sum(stats_ref[0], keepdims=True), jnp.sum(stats_ref[1], keepdims=True), peak):
            pieces.extend(in_three(jnp.broadcast_to(value, shape)))
        line = jnp.zeros(shape, F32)
        for k, piece in enumerate(pieces):
            line = jnp.where((iota(shape, 0) == k) & (iota(shape, 1) == LIMIT), piece, line)

    def some_peers(step, carry):
        for turn in range(SENDS):
            peer = step * SENDS + turn
            parts = []
            for row in range(ROWS):
                start = peer * 2 * ROWS + row
                real_part = sums_ref[pl.ds(start, ROWS, stride=PITCH), :]
                imag_part = sums_ref[pl.ds(start + ROWS, ROWS, stride=PITCH), :]
                parts.append(jnp.concatenate([real_part, imag_part], axis=0))
            if apart:
                parts[0] = parts[0] + line
            for k, block in enumerate(packed(parts)):
                at = 2 * ROWS * k
                out_ref[peer, at : at + block.shape[0], :] = block.astype(BF16)
        return carry

    lax.fori_loop(0, PEERS // SENDS, some_peers, 0)
    if apart:
        for load in loads[4:]:
            load.wait()


def tendency(came_ref, table_ref):
    count = 2 * ROWS
    blocks = [came_ref[:, k * count : (k + 1) * count, :] for k in range(BLOCKS)]
    last = came_ref[:, BLOCKS * count :, :].astype(F32)
    blocks.append(jnp.concatenate([last, pltpu.roll(last, HALF // 2, 2)], axis=1).astype(BF16))
    sums = dot(table_ref[...], jnp.concatenate([block.reshape(2 * N, HALF) for block in blocks], axis=1))
    parts = unpacked([sums[:, k * HALF : (k + 1) * HALF] for k in range(BLOCKS + 1)])
    between = jnp.zeros((N - 2 * KEPT, HALF), F32)
    cut = [[part[k * KEPT : (k + 1) * KEPT] for k in range(4)] for part in parts]
    return [tuple(jnp.concatenate([c[k], between, c[k + 1]], axis=0) for k in (0, 2)) for c in cut]


def middle_kernel(
    bound_ref,
    species_ref,
    base_ref,
    came_ref,
    state_ref,
    z_fwd_ref,
    z_inv_ref,
    out_ref,
    kept_ref,
    kappa_ref,
    whole_ref,
    deriv_ref,
):
    shape = (PEERS, 2 * ROWS, HALF)
    found = jnp.where(iota(shape, 2) == LIMIT, came_ref[:, : 2 * ROWS, :].astype(F32), 0.0)
    piece_row = iota(shape, 1)

    def piece(which):
        inside = jnp.where((piece_row >= 3 * which) & (piece_row < 3 * which + 3), found, 0.0)
        return jnp.sum(jnp.sum(inside, axis=1), axis=1, keepdims=True)

    def spread(value):
        return jnp.broadcast_to(value, (8, HALF))

    variance = spread(jnp.sum(piece(0), axis=0, keepdims=True)) / CELLS
    mean_grad = spread(jnp.sum(piece(1), axis=0, keepdims=True)) / CELLS
    peak = spread(jnp.max(piece(2), axis=0, keepdims=True))
    base = base_ref[species_ref[0]]
    found = base * peak * jnp.sqrt(variance) / (mean_grad + 1e-06)
    kappa_ref[0] = jnp.max(found)
    kappa = found[0:1, :]
    bound = (bound_ref[0] * bound_ref[0]).astype(F32)
    kz_wave = signed(iota((N, HALF), 0))
    along_z = jnp.exp(-kappa * (kz_wave * kz_wave) * STEP)
    for local, sums in enumerate(tendency(came_ref, z_fwd_ref)):
        _, ksquare = waves_of(local)
        factor = along_z * jnp.exp(-kappa * across_z(local) * STEP)
        scaled = STEP * factor
        inside = ksquare <= bound
        middle = []
        for part in (0, 1):
            start = factor * state_ref[part, local]
            change = jnp.where(inside, scaled * sums[part], 0.0)
            middle.append(start - change)
            kept_ref[part, local] = start - 0.5 * change
        z_inverse(local, z_rows(*middle, kz_wave), z_inv_ref, whole_ref, deriv_ref)
    send_planes(0, PEERS, PEERS, out_ref, whole_ref, deriv_ref)


def final_kernel(bound_ref, came_ref, kept_ref, z_fwd_ref, out_hbm, out_ref, out_sems):
    bound = (bound_ref[0] * bound_ref[0]).astype(F32)
    saves = []
    for local, sums in enumerate(tendency(came_ref, z_fwd_ref)):
        _, ksquare = waves_of(local)
        for part in (0, 1):
            change = jnp.where(ksquare <= bound, (0.5 * STEP) * sums[part], 0.0)
            out_ref[part, local] = kept_ref[part, local] - change
        saves.append(copy_of(out_ref.at[:, local], out_hbm.at[:, local], out_sems.at[local]))
        saves[-1].start()
    for save in saves:
        save.wait()


SCALARS = pl.BlockSpec(memory_space=pltpu.SMEM)
NEAR = pl.BlockSpec(memory_space=pltpu.VMEM)
FAR = pl.BlockSpec(memory_space=pltpu.HBM)
PLANES = (PEERS, ROWS, 2 * ROWS, N)
SENT = (PEERS, 2 * ROWS * KEPT * ROWS // HALF, HALF)
STATE = (2, ROWS, N, HALF)
PAIR = 4
CHUNK = 8
UNROLL = 4
SENDS = 32


def params(mebibytes):
    return pltpu.CompilerParams(vmem_limit_bytes=mebibytes * 2**20)


def shaped(shape, dtype):
    return jax.ShapeDtypeStruct(shape, dtype)


def near(x):
    return pltpu.with_memory_space_constraint(x, pltpu.VMEM)


def far(x):
    return pltpu.with_memory_space_constraint(x, pltpu.HBM)


def sems(count):
    return pltpu.SemaphoreType.DMA((count,))


def turned():
    return pltpu.VMEM((ROWS * PITCH, HALF), F32)


BIG = pltpu.VMEM((2, N, N), BF16)
HELD = pltpu.VMEM(STATE, F32)


def gathered(velocity):
    groups = lax.axis_size("scal")
    me = lax.axis_index("scal")
    ring = 4
    high, low = me // ring, me % ring
    planes, rows = velocity.shape[1], velocity.shape[2] // 2
    velocity = velocity.reshape(3, planes, rows, 2, N).swapaxes(2, 3)

    def moved(x, change):
        return lax.ppermute(x, "scal", [(s, change(s)) for s in range(groups)])

    def beside(shift):
        return lambda s: s // ring * ring + (s + shift) % ring

    across = moved(velocity, lambda s: (s + ring) % groups)
    out = jnp.zeros((3, planes, 2, HALF, N), velocity.dtype)
    half = planes // 2

    def placed(out, x, owner, first=0):
        return lax.dynamic_update_slice(out, x, (0, first, 0, owner * rows, 0))

    for x, own in ((velocity, high), (across, 1 - high)):
        up = moved(x, beside(1))
        down = moved(x, beside(-1))
        far_up = moved(up[:, :half], beside(1))
        far_down = moved(down[:, half:], beside(-1))
        start = own * ring
        out = placed(out, x, start + low)
        out = placed(out, up, start + (low + ring - 1) % ring)
        out = placed(out, down, start + (low + 1) % ring)
        out = placed(out, far_up, start + (low + 2) % ring)
        out = placed(out, far_down, start + (low + 2) % ring, half)
    return out.reshape(3, planes, N, N)


def exchanged(x):
    return lax.all_to_all(x, "fft", 0, 0, tiled=True)


def start_call(state, table):
    return pl.pallas_call(
        start_kernel,
        in_specs=[FAR, FAR],
        out_specs=[FAR, NEAR],
        out_shape=[pltpu.HBM(PLANES, BF16), pltpu.VMEM((2, 8, HALF), F32)],
        scratch_shapes=[HELD, BIG, pltpu.VMEM(PLANES, BF16), turned(), turned(), sems(ROWS + 1), sems(PEERS // CHUNK)],
        compiler_params=params(24),
        name="start",
    )(far(state), far(table["z_inv"]))


def grid_call(scalars, planes, speeds, stats, held, apart):
    scratch = [turned(), pltpu.VMEM((8, N), F32)]
    passed = held if apart else ()
    if apart:
        scratch += [pltpu.VMEM(PLANES, BF16), sems(ROWS), sems(len(held))]
    spec, place = (FAR, far) if apart else (NEAR, near)
    return pl.pallas_call(
        grid_kernel,
        in_specs=[(SCALARS,) * len(scalars), spec, NEAR, NEAR, (spec,) * len(held)],
        out_specs=[NEAR, (NEAR,) * len(passed)],
        out_shape=[pltpu.VMEM(SENT, BF16), tuple(pltpu.VMEM(x.shape, x.dtype) for x in passed)],
        scratch_shapes=scratch,
        compiler_params=params(24),
        name="grid",
    )(scalars, place(planes), near(speeds), near(stats), tuple(place(x) for x in held))


def middle_call(scalars, came, state, z_fwd, z_inv):
    return pl.pallas_call(
        middle_kernel,
        in_specs=[SCALARS] * 3 + [NEAR] * 4,
        out_specs=[NEAR, NEAR, SCALARS],
        out_shape=[pltpu.VMEM(PLANES, BF16), pltpu.VMEM(STATE, F32), shaped((1,), F32)],
        scratch_shapes=[turned(), turned()],
        compiler_params=params(24),
        name="middle",
    )(*scalars, *(near(x) for x in (came, state, z_fwd, z_inv)))


def final_call(bound, came, kept, z_fwd):
    return pl.pallas_call(
        final_kernel,
        in_specs=[SCALARS, NEAR, NEAR, NEAR],
        out_specs=FAR,
        out_shape=pltpu.HBM(STATE, F32),
        scratch_shapes=[HELD, sems(ROWS)],
        compiler_params=params(24),
        name="final",
    )(bound, near(came), near(kept), near(z_fwd))


def body(scalar_state, velocity, species, kappa_table, dealias_bound):
    table = tables()
    state = scalar_state[0]
    speeds = gathered(velocity)
    planes, stats = start_call(state, table)
    scalars = (dealias_bound, species, kappa_table)
    held = tuple(table[name] for name in ("y_inv", "x_inv", "x_fwd", "y_fwd", "z_fwd", "z_inv")) + (state,)
    sent, held = grid_call(scalars, exchanged(planes), speeds, stats, held, True)
    *grid_tables, z_fwd, z_inv, state = held
    planes, kept, kappa = middle_call(scalars, exchanged(sent), state, z_fwd, z_inv)
    sent, _ = grid_call((), exchanged(planes), speeds, stats, tuple(grid_tables), False)
    return (final_call(dealias_bound, exchanged(sent), kept, z_fwd)[None], kappa)


def solution(mesh):
    placed = (
        P("scal", None, "fft", None, None),
        P(None, "fft", "scal", None),
        P("scal"),
        P(),
        P("scal"),
    )
    return jax.shard_map(
        body,
        mesh=mesh,
        in_specs=placed,
        out_specs=(P("scal", None, "fft", None, None), P("scal")),
        check_vma=False,
    )
```

```python
import math

import jax
import jax.numpy as jnp
import numpy as np
from jax import lax
from jax.experimental import pallas as pl
from jax.experimental.pallas import tpu as pltpu
from jax.sharding import PartitionSpec as P

N = 256
HALF = 128
PEERS = 32
ROWS = N // PEERS
KEPT = 88
LIMIT = 86
BLOCKS = ROWS * KEPT // HALF
PITCH = 2 * N + 4
STEP = 0.2 * 2.0 * math.pi / N
CELLS = float(N) ** 3
F32 = jnp.float32
BF16 = jnp.bfloat16


def tables():
    def cos_sin(rows, columns):
        angles = (rows[:, None] * columns[None, :] % N).astype(np.float32) * np.float32(2.0 * math.pi / N)
        scale = np.float32(1.0 / math.sqrt(N))
        return np.cos(angles) * scale, np.sin(angles) * scale

    def inverse(rows, columns):
        cos, sin = cos_sin(rows, columns)
        return np.block([[cos, -sin], [sin, cos]])

    def forward(rows, columns):
        cos, sin = cos_sin(rows, columns)
        return np.block([[cos, sin], [-sin, cos]])

    def order(peers):
        return np.arange(2 * peers * ROWS).reshape(2, peers, ROWS).transpose(1, 0, 2).reshape(-1)

    index, low = np.arange(N), np.arange(HALF)
    cos, sin = cos_sin(index, low)
    weight = np.where(low == 0, 1.0, 2.0).astype(np.float32)[:, None]
    keep = (low < LIMIT).astype(np.float32)[None, :]
    halves = order(PEERS // 2)
    listed = {
        "z_inv": np.stack([inverse(2 * low + turn, low) for turn in (0, 1)]),
        "y_inv": np.stack([inverse(2 * low + turn, low)[:, halves] for turn in (0, 1)]),
        "x_inv": np.concatenate([-weight * sin.T, -weight * cos.T], axis=0),
        "x_fwd": np.concatenate([cos * keep, -sin * keep], axis=1),
        "y_fwd": np.stack([forward(low, 2 * low + turn)[halves] for turn in (0, 1)]),
        "z_fwd": forward(np.concatenate([index[:KEPT], index[-KEPT:]]), index)[:, order(PEERS)],
    }
    return {name: jnp.asarray(value.astype(np.float32)).astype(BF16) for name, value in listed.items()}


def both_turns(x):
    low, high = x[: x.shape[0] // 2], x[x.shape[0] // 2 :]
    return low + high, low - high


def dot(left, right):
    return jnp.dot(left, right, preferred_element_type=F32)


def iota(shape, dim):
    return lax.broadcasted_iota(jnp.int32, shape, dim)


def signed(index):
    return jnp.where(index < HALF, index, index - N).astype(F32)


def z_rows(real_part, imag_part, kz_wave):
    columns = [
        [jnp.concatenate(pair, axis=0).astype(BF16) for pair in zip(both_turns(real), both_turns(imag))]
        for real, imag in ((real_part, imag_part), (kz_wave * real_part, kz_wave * imag_part))
    ]
    return [jnp.concatenate(pair, axis=1) for pair in zip(*columns)]


def send_planes(first, count, unroll, planes_ref, whole_ref, deriv_ref):
    def some_peers(step, carry):
        for turn in range(unroll):
            peer = first + step * unroll + turn
            for local in range(ROWS):
                for at, ref in ((0, whole_ref), (HALF, deriv_ref)):
                    start = local % 2 * N + peer * (ROWS // 2) + local // 2
                    real_part = ref[pl.ds(start, ROWS, stride=PITCH), :]
                    imag_part = ref[pl.ds(start + HALF, ROWS, stride=PITCH), :]
                    tile = jnp.concatenate([real_part, imag_part], axis=0).astype(BF16)
                    planes_ref[peer, local, :, at : at + HALF] = tile
        return carry

    lax.fori_loop(0, count // unroll, some_peers, 0)


def row_of(block, shift=0):
    return block * PITCH + shift if isinstance(block, int) else pl.multiple_of(block * PITCH + shift, 4)


def z_inverse(local, rows, table_ref, whole_ref, deriv_ref):
    for turn in (0, 1):
        found = dot(table_ref[turn], rows[turn])
        part = pl.ds(row_of(local, turn * N), N)
        whole_ref[part, :] = found[:, :HALF]
        deriv_ref[part, :] = found[:, HALF:]


def across_z(local):
    ky_wave = signed(lax.axis_index("fft").astype(jnp.int32) * ROWS + local)
    kx_wave = iota((1, HALF), 1).astype(F32)
    return kx_wave * kx_wave + ky_wave * ky_wave


def waves_of(local):
    kz_wave = signed(iota((N, HALF), 0))
    return kz_wave, across_z(local) + kz_wave * kz_wave


def copy_of(source, target, sem):
    return pltpu.make_async_copy(source, target, sem)


def start_kernel(
    state_hbm, table_hbm, out_hbm, stats_ref, state_ref, table_ref, planes_ref, whole_ref, deriv_ref, in_sems, out_sems
):
    loads = [copy_of(table_hbm, table_ref, in_sems.at[ROWS])]
    loads += [copy_of(state_hbm.at[:, k], state_ref.at[:, k], in_sems.at[k]) for k in range(ROWS)]
    for load in loads:
        load.start()
    stats_ref[...] = jnp.zeros_like(stats_ref)
    loads[0].wait()

    for first in range(0, ROWS, AT_ONCE):
        for local in range(first, first + AT_ONCE):
            loads[1 + local].wait()
        for local in range(first, first + AT_ONCE):
            kz_wave, ksquare = waves_of(local)
            real_part = state_ref[0, local]
            imag_part = state_ref[1, local]
            weight = jnp.where(iota((N, HALF), 1) == 0, 1.0, 2.0)
            energy = weight * (real_part * real_part + imag_part * imag_part)
            stats_ref[0] += jnp.sum(energy.reshape(N // 8, 8, HALF), axis=0)
            stats_ref[1] += jnp.sum((ksquare * energy).reshape(N // 8, 8, HALF), axis=0)
            z_inverse(local, z_rows(real_part, imag_part, kz_wave), table_ref, whole_ref, deriv_ref)

    def leaving(k):
        part = pl.ds(k * CHUNK, CHUNK)
        return copy_of(planes_ref.at[part], out_hbm.at[part], out_sems.at[k])

    def one_chunk(k, carry):
        send_planes(k * CHUNK, CHUNK, UNROLL, planes_ref, whole_ref, deriv_ref)
        leaving(k).start()
        return carry

    lax.fori_loop(0, PEERS // CHUNK, one_chunk, 0)
    for k in range(PEERS // CHUNK):
        leaving(k).wait()


def in_three(value):
    high = value.astype(BF16).astype(F32)
    rest = value - high
    middle = rest.astype(BF16).astype(F32)
    return high, middle, (rest - middle).astype(BF16).astype(F32)


def place_of(row):
    return row * KEPT // HALF, row * KEPT % HALF


def packed(parts):
    lane = iota((2 * ROWS, HALF), 1)
    blocks = [None] * (BLOCKS + 1)
    for row, part in enumerate(parts):
        block, shift = place_of(row)
        turned = pltpu.roll(part, shift, 1) if shift else part
        blocks[block] = turned if shift == 0 else jnp.where(lane < shift, blocks[block], turned)
        if shift + KEPT > HALF:
            blocks[block + 1] = turned
    real_part, imag_part = blocks[BLOCKS][:ROWS], blocks[BLOCKS][ROWS:]
    blocks[BLOCKS] = jnp.where(lane[:ROWS] < HALF // 2, real_part, pltpu.roll(imag_part, HALF // 2, 1))
    return blocks


def unpacked(blocks):
    lane = iota(blocks[0].shape, 1)
    parts = []
    for row in range(ROWS):
        block, shift = place_of(row)
        part = blocks[block]
        if shift + KEPT > HALF:
            part = jnp.where(lane >= shift, part, blocks[block + 1])
        parts.append(pltpu.roll(part, HALF - shift, 1) if shift else part)
    return parts


def grid_kernel(scalars, planes_hbm, speed_ref, stats_ref, held, out_ref, passed, sums_ref, peak_ref, *apart):
    count = 2 * N
    if apart:
        planes_ref, planes_sems, sems = apart

        def came_plane(k):
            return copy_of(planes_hbm.at[:, k], planes_ref.at[:, k], planes_sems.at[k])

        loads = [copy_of(source, target, sems.at[k]) for k, (source, target) in enumerate(zip(held, passed))]
        loads[0].start()
        for k in range(PAIR):
            came_plane(k).start()
        for load in loads[1:4]:
            load.start()
        for k in range(PAIR, ROWS):
            came_plane(k).start()
        for load in loads[4:]:
            load.start()
        held = passed
    else:
        planes_ref = planes_hbm
    y_inv_ref, x_inv_ref, x_fwd_ref, y_fwd_ref = held[:4]
    peak_ref[...] = jnp.zeros_like(peak_ref)
    row = iota((count, HALF), 0)
    ky_wave = signed(row // (2 * ROWS) * ROWS + row % ROWS).astype(BF16)
    kx_wave = iota((HALF, HALF), 1).astype(F32)

    def one_pair(step):
        if apart:
            for k in range(PAIR):
                came_plane(step * PAIR + k).wait()
        if apart and step == 0:
            for load in loads[:4]:
                load.wait()
        came = [planes_ref[:, step * PAIR + k].reshape(count, N) for k in range(PAIR)]
        scaled = [ky_wave * part[:, :HALF] for part in came]
        pairs = both_turns(jnp.concatenate(came + scaled, axis=1))
        y_section = [dot(y_inv_ref[turn], pairs[turn]) for turn in (0, 1)]
        x_rows = []
        for k in range(PAIR):
            starts = (k * N, PAIR * N + k * HALF, k * N + HALF)
            for which, at in enumerate(starts):
                for found in y_section:
                    halves = [found[part * HALF : (part + 1) * HALF, at : at + HALF] for part in (0, 1)]
                    if which == 0:
                        halves = [kx_wave * half for half in halves]
                    x_rows.append(jnp.concatenate(halves, axis=1).astype(BF16))
        gradients = dot(jnp.concatenate(x_rows, axis=0), x_inv_ref[...])
        fields = []
        for k in range(PAIR):
            parts = [gradients[(3 * k + d) * N : (3 * k + d + 1) * N] for d in range(3)]
            total = speed_ref[0, step * PAIR + k].astype(F32) * parts[0]
            total = total + speed_ref[1, step * PAIR + k].astype(F32) * parts[1]
            total = total + speed_ref[2, step * PAIR + k].astype(F32) * parts[2]
            fields.append(total.astype(BF16))
            if apart:
                square = parts[0] * parts[0] + parts[1] * parts[1] + parts[2] * parts[2]
                peak_ref[...] = jnp.maximum(peak_ref[...], jnp.max(square.reshape(N // 8, 8, N), axis=0))
        x_section = dot(jnp.concatenate(fields, axis=0), x_fwd_ref[...]).astype(BF16)
        sums = []
        for turn in (0, 1):
            columns = []
            for k in range(PAIR):
                part = x_section[k * N + turn * HALF : k * N + (turn + 1) * HALF]
                columns.append(jnp.concatenate([part[:, :HALF], part[:, HALF:]], axis=0))
            sums.append(dot(y_fwd_ref[turn], jnp.concatenate(columns, axis=1)))
        for k in range(PAIR):
            even, odd = (found[:, k * HALF : (k + 1) * HALF] for found in sums)
            sums_ref[pl.ds(row_of(step * PAIR + k), N), :] = even + odd
            sums_ref[pl.ds(row_of(step * PAIR + k, N), N), :] = even - odd

    for step in range(ROWS // PAIR):
        one_pair(step)
    if apart:
        shape = (2 * ROWS, HALF)
        peak = jnp.sqrt(jnp.max(peak_ref[...], keepdims=True))
        pieces = []
        for value in (jnp.sum(stats_ref[0], keepdims=True), jnp.sum(stats_ref[1], keepdims=True), peak):
            pieces.extend(in_three(jnp.broadcast_to(value, shape)))
        line = jnp.zeros(shape, F32)
        for k, piece in enumerate(pieces):
            line = jnp.where((iota(shape, 0) == k) & (iota(shape, 1) == LIMIT), piece, line)

    def some_peers(step, carry):
        for turn in range(SENDS):
            peer = step * SENDS + turn
            parts = []
            for row in range(ROWS):
                start = peer * 2 * ROWS + row
                real_part = sums_ref[pl.ds(start, ROWS, stride=PITCH), :]
                imag_part = sums_ref[pl.ds(start + ROWS, ROWS, stride=PITCH), :]
                parts.append(jnp.concatenate([real_part, imag_part], axis=0))
            if apart:
                parts[0] = parts[0] + line
            for k, block in enumerate(packed(parts)):
                at = 2 * ROWS * k
                out_ref[peer, at : at + block.shape[0], :] = block.astype(BF16)
        return carry

    lax.fori_loop(0, PEERS // SENDS, some_peers, 0)
    if apart:
        for load in loads[4:]:
            load.wait()


def tendency(came_ref, table_ref):
    count = 2 * ROWS
    blocks = [came_ref[:, k * count : (k + 1) * count, :] for k in range(BLOCKS)]
    last = came_ref[:, BLOCKS * count :, :].astype(F32)
    blocks.append(jnp.concatenate([last, pltpu.roll(last, HALF // 2, 2)], axis=1).astype(BF16))
    sums = dot(table_ref[...], jnp.concatenate([block.reshape(2 * N, HALF) for block in blocks], axis=1))
    parts = unpacked([sums[:, k * HALF : (k + 1) * HALF] for k in range(BLOCKS + 1)])
    between = jnp.zeros((N - 2 * KEPT, HALF), F32)
    cut = [[part[k * KEPT : (k + 1) * KEPT] for k in range(4)] for part in parts]
    return [tuple(jnp.concatenate([c[k], between, c[k + 1]], axis=0) for k in (0, 2)) for c in cut]


def middle_kernel(
    bound_ref,
    species_ref,
    base_ref,
    came_ref,
    state_ref,
    z_fwd_ref,
    z_inv_ref,
    out_ref,
    kept_ref,
    kappa_ref,
    whole_ref,
    deriv_ref,
):
    shape = (PEERS, 2 * ROWS, HALF)
    found = jnp.where(iota(shape, 2) == LIMIT, came_ref[:, : 2 * ROWS, :].astype(F32), 0.0)
    piece_row = iota(shape, 1)

    def piece(which):
        inside = jnp.where((piece_row >= 3 * which) & (piece_row < 3 * which + 3), found, 0.0)
        return jnp.sum(jnp.sum(inside, axis=1), axis=1, keepdims=True)

    def spread(value):
        return jnp.broadcast_to(value, (8, HALF))

    variance = spread(jnp.sum(piece(0), axis=0, keepdims=True)) / CELLS
    mean_grad = spread(jnp.sum(piece(1), axis=0, keepdims=True)) / CELLS
    peak = spread(jnp.max(piece(2), axis=0, keepdims=True))
    base = base_ref[species_ref[0]]
    found = base * peak * jnp.sqrt(variance) / (mean_grad + 1e-06)
    kappa_ref[0] = jnp.max(found)
    kappa = found[0:1, :]
    bound = (bound_ref[0] * bound_ref[0]).astype(F32)
    kz_wave = signed(iota((N, HALF), 0))
    along_z = jnp.exp(-kappa * (kz_wave * kz_wave) * STEP)
    for local, sums in enumerate(tendency(came_ref, z_fwd_ref)):
        _, ksquare = waves_of(local)
        factor = along_z * jnp.exp(-kappa * across_z(local) * STEP)
        scaled = STEP * factor
        inside = ksquare <= bound
        middle = []
        for part in (0, 1):
            start = factor * state_ref[part, local]
            change = jnp.where(inside, scaled * sums[part], 0.0)
            middle.append(start - change)
            kept_ref[part, local] = start - 0.5 * change
        z_inverse(local, z_rows(*middle, kz_wave), z_inv_ref, whole_ref, deriv_ref)
    send_planes(0, PEERS, PEERS, out_ref, whole_ref, deriv_ref)


def final_kernel(bound_ref, came_ref, kept_ref, z_fwd_ref, out_hbm, out_ref, out_sems):
    bound = (bound_ref[0] * bound_ref[0]).astype(F32)
    saves = []
    for local, sums in enumerate(tendency(came_ref, z_fwd_ref)):
        _, ksquare = waves_of(local)
        for part in (0, 1):
            change = jnp.where(ksquare <= bound, (0.5 * STEP) * sums[part], 0.0)
            out_ref[part, local] = kept_ref[part, local] - change
        saves.append(copy_of(out_ref.at[:, local], out_hbm.at[:, local], out_sems.at[local]))
        saves[-1].start()
    for save in saves:
        save.wait()


SCALARS = pl.BlockSpec(memory_space=pltpu.SMEM)
NEAR = pl.BlockSpec(memory_space=pltpu.VMEM)
FAR = pl.BlockSpec(memory_space=pltpu.HBM)
PLANES = (PEERS, ROWS, 2 * ROWS, N)
SENT = (PEERS, 2 * ROWS * KEPT * ROWS // HALF, HALF)
STATE = (2, ROWS, N, HALF)
PAIR = 4
AT_ONCE = 4
CHUNK = 8
UNROLL = 4
SENDS = 32


def params(mebibytes):
    return pltpu.CompilerParams(vmem_limit_bytes=mebibytes * 2**20)


def shaped(shape, dtype):
    return jax.ShapeDtypeStruct(shape, dtype)


def near(x):
    return pltpu.with_memory_space_constraint(x, pltpu.VMEM)


def far(x):
    return pltpu.with_memory_space_constraint(x, pltpu.HBM)


def sems(count):
    return pltpu.SemaphoreType.DMA((count,))


def turned():
    return pltpu.VMEM((ROWS * PITCH, HALF), F32)


BIG = pltpu.VMEM((2, N, N), BF16)
HELD = pltpu.VMEM(STATE, F32)


def gathered(velocity):
    groups = lax.axis_size("scal")
    me = lax.axis_index("scal")
    ring = 4
    high, low = me // ring, me % ring
    planes, rows = velocity.shape[1], velocity.shape[2] // 2
    velocity = velocity.reshape(3, planes, rows, 2, N).swapaxes(2, 3)

    def moved(x, change):
        return lax.ppermute(x, "scal", [(s, change(s)) for s in range(groups)])

    def beside(shift):
        return lambda s: s // ring * ring + (s + shift) % ring

    across = moved(velocity, lambda s: (s + ring) % groups)
    out = jnp.zeros((3, planes, 2, HALF, N), velocity.dtype)
    half = planes // 2

    def placed(out, x, owner, first=0):
        return lax.dynamic_update_slice(out, x, (0, first, 0, owner * rows, 0))

    for x, own in ((velocity, high), (across, 1 - high)):
        up = moved(x, beside(1))
        down = moved(x, beside(-1))
        far_up = moved(up[:, :half], beside(1))
        far_down = moved(down[:, half:], beside(-1))
        start = own * ring
        out = placed(out, x, start + low)
        out = placed(out, up, start + (low + ring - 1) % ring)
        out = placed(out, down, start + (low + 1) % ring)
        out = placed(out, far_up, start + (low + 2) % ring)
        out = placed(out, far_down, start + (low + 2) % ring, half)
    return out.reshape(3, planes, N, N)


def exchanged(x):
    return lax.all_to_all(x, "fft", 0, 0, tiled=True)


def start_call(state, table):
    return pl.pallas_call(
        start_kernel,
        in_specs=[FAR, FAR],
        out_specs=[FAR, NEAR],
        out_shape=[pltpu.HBM(PLANES, BF16), pltpu.VMEM((2, 8, HALF), F32)],
        scratch_shapes=[HELD, BIG, pltpu.VMEM(PLANES, BF16), turned(), turned(), sems(ROWS + 1), sems(PEERS // CHUNK)],
        compiler_params=params(24),
        name="start",
    )(far(state), far(table["z_inv"]))


def grid_call(scalars, planes, speeds, stats, held, apart):
    scratch = [turned(), pltpu.VMEM((8, N), F32)]
    passed = held if apart else ()
    if apart:
        scratch += [pltpu.VMEM(PLANES, BF16), sems(ROWS), sems(len(held))]
    spec, place = (FAR, far) if apart else (NEAR, near)
    return pl.pallas_call(
        grid_kernel,
        in_specs=[(SCALARS,) * len(scalars), spec, NEAR, NEAR, (spec,) * len(held)],
        out_specs=[NEAR, (NEAR,) * len(passed)],
        out_shape=[pltpu.VMEM(SENT, BF16), tuple(pltpu.VMEM(x.shape, x.dtype) for x in passed)],
        scratch_shapes=scratch,
        compiler_params=params(24),
        name="grid",
    )(scalars, place(planes), near(speeds), near(stats), tuple(place(x) for x in held))


def middle_call(scalars, came, state, z_fwd, z_inv):
    return pl.pallas_call(
        middle_kernel,
        in_specs=[SCALARS] * 3 + [NEAR] * 4,
        out_specs=[NEAR, NEAR, SCALARS],
        out_shape=[pltpu.VMEM(PLANES, BF16), pltpu.VMEM(STATE, F32), shaped((1,), F32)],
        scratch_shapes=[turned(), turned()],
        compiler_params=params(24),
        name="middle",
    )(*scalars, *(near(x) for x in (came, state, z_fwd, z_inv)))


def final_call(bound, came, kept, z_fwd):
    return pl.pallas_call(
        final_kernel,
        in_specs=[SCALARS, NEAR, NEAR, NEAR],
        out_specs=FAR,
        out_shape=pltpu.HBM(STATE, F32),
        scratch_shapes=[HELD, sems(ROWS)],
        compiler_params=params(24),
        name="final",
    )(bound, near(came), near(kept), near(z_fwd))


def body(scalar_state, velocity, species, kappa_table, dealias_bound):
    table = tables()
    state = scalar_state[0]
    speeds = gathered(velocity)
    planes, stats = start_call(state, table)
    scalars = (dealias_bound, species, kappa_table)
    held = tuple(table[name] for name in ("y_inv", "x_inv", "x_fwd", "y_fwd", "z_fwd", "z_inv")) + (state,)
    sent, held = grid_call(scalars, exchanged(planes), speeds, stats, held, True)
    *grid_tables, z_fwd, z_inv, state = held
    planes, kept, kappa = middle_call(scalars, exchanged(sent), state, z_fwd, z_inv)
    sent, _ = grid_call((), exchanged(planes), speeds, stats, tuple(grid_tables), False)
    return (final_call(dealias_bound, exchanged(sent), kept, z_fwd)[None], kappa)


def solution(mesh):
    placed = (
        P("scal", None, "fft", None, None),
        P(None, "fft", "scal", None),
        P("scal"),
        P(),
        P("scal"),
    )
    return jax.shard_map(
        body,
        mesh=mesh,
        in_specs=placed,
        out_specs=(P("scal", None, "fft", None, None), P("scal")),
        check_vma=False,
    )
```

```python
import math

import jax
import jax.numpy as jnp
import numpy as np
from jax import lax
from jax.experimental import pallas as pl
from jax.experimental.pallas import tpu as pltpu
from jax.sharding import PartitionSpec as P

N = 256
HALF = 128
PEERS = 32
ROWS = N // PEERS
KEPT = 88
LIMIT = 86
BLOCKS = ROWS * KEPT // HALF
PITCH = 2 * N + 4
STEP = 0.2 * 2.0 * math.pi / N
CELLS = float(N) ** 3
F32 = jnp.float32
BF16 = jnp.bfloat16


def tables():
    def cos_sin(rows, columns):
        angles = (rows[:, None] * columns[None, :] % N).astype(np.float32) * np.float32(2.0 * math.pi / N)
        scale = np.float32(1.0 / math.sqrt(N))
        return np.cos(angles) * scale, np.sin(angles) * scale

    def inverse(rows, columns):
        cos, sin = cos_sin(rows, columns)
        return np.block([[cos, -sin], [sin, cos]])

    def forward(rows, columns):
        cos, sin = cos_sin(rows, columns)
        return np.block([[cos, sin], [-sin, cos]])

    def order(peers):
        return np.arange(2 * peers * ROWS).reshape(2, peers, ROWS).transpose(1, 0, 2).reshape(-1)

    index, low = np.arange(N), np.arange(HALF)
    cos, sin = cos_sin(index, low)
    weight = np.where(low == 0, 1.0, 2.0).astype(np.float32)[:, None]
    keep = (low < LIMIT).astype(np.float32)[None, :]
    halves = order(PEERS // 2)
    listed = {
        "z_inv": np.stack([inverse(2 * low + turn, low) for turn in (0, 1)]),
        "y_inv": np.stack([inverse(2 * low + turn, low)[:, halves] for turn in (0, 1)]),
        "x_inv": np.concatenate([-weight * sin.T, -weight * cos.T], axis=0),
        "x_fwd": np.concatenate([cos * keep, -sin * keep], axis=1),
        "y_fwd": np.stack([forward(low, 2 * low + turn)[halves] for turn in (0, 1)]),
        "z_fwd": forward(np.concatenate([index[:KEPT], index[-KEPT:]]), index)[:, order(PEERS)],
    }
    return {name: jnp.asarray(value.astype(np.float32)).astype(BF16) for name, value in listed.items()}


def both_turns(x):
    low, high = x[: x.shape[0] // 2], x[x.shape[0] // 2 :]
    return low + high, low - high


def dot(left, right):
    return jnp.dot(left, right, preferred_element_type=F32)


def iota(shape, dim):
    return lax.broadcasted_iota(jnp.int32, shape, dim)


def signed(index):
    return jnp.where(index < HALF, index, index - N).astype(F32)


def z_rows(real_part, imag_part, kz_wave):
    columns = [
        [jnp.concatenate(pair, axis=0).astype(BF16) for pair in zip(both_turns(real), both_turns(imag))]
        for real, imag in ((real_part, imag_part), (kz_wave * real_part, kz_wave * imag_part))
    ]
    return [jnp.concatenate(pair, axis=1) for pair in zip(*columns)]


def send_planes(first, count, unroll, planes_ref, whole_ref, deriv_ref):
    def some_peers(step, carry):
        for turn in range(unroll):
            peer = first + step * unroll + turn
            for local in range(ROWS):
                for at, ref in ((0, whole_ref), (HALF, deriv_ref)):
                    start = local % 2 * N + peer * (ROWS // 2) + local // 2
                    real_part = ref[pl.ds(start, ROWS, stride=PITCH), :]
                    imag_part = ref[pl.ds(start + HALF, ROWS, stride=PITCH), :]
                    tile = jnp.concatenate([real_part, imag_part], axis=0).astype(BF16)
                    planes_ref[peer, local, :, at : at + HALF] = tile
        return carry

    lax.fori_loop(0, count // unroll, some_peers, 0)


def row_of(block, shift=0):
    return block * PITCH + shift if isinstance(block, int) else pl.multiple_of(block * PITCH + shift, 4)


def z_inverse(local, rows, table_ref, whole_ref, deriv_ref):
    for turn in (0, 1):
        found = dot(table_ref[turn], rows[turn])
        part = pl.ds(row_of(local, turn * N), N)
        whole_ref[part, :] = found[:, :HALF]
        deriv_ref[part, :] = found[:, HALF:]


def across_z(local):
    ky_wave = signed(lax.axis_index("fft").astype(jnp.int32) * ROWS + local)
    kx_wave = iota((1, HALF), 1).astype(F32)
    return kx_wave * kx_wave + ky_wave * ky_wave


def waves_of(local):
    kz_wave = signed(iota((N, HALF), 0))
    return kz_wave, across_z(local) + kz_wave * kz_wave


def copy_of(source, target, sem):
    return pltpu.make_async_copy(source, target, sem)


def start_kernel(
    state_hbm, table_hbm, out_hbm, stats_ref, state_ref, table_ref, planes_ref, whole_ref, deriv_ref, in_sems, out_sems
):
    loads = [copy_of(table_hbm, table_ref, in_sems.at[ROWS])]
    loads += [copy_of(state_hbm.at[:, k], state_ref.at[:, k], in_sems.at[k]) for k in range(ROWS)]
    for load in loads:
        load.start()
    stats_ref[...] = jnp.zeros_like(stats_ref)
    loads[0].wait()

    for first in range(0, ROWS, AT_ONCE):
        for local in range(first, first + AT_ONCE):
            loads[1 + local].wait()
        for local in range(first, first + AT_ONCE):
            kz_wave, ksquare = waves_of(local)
            real_part = state_ref[0, local]
            imag_part = state_ref[1, local]
            weight = jnp.where(iota((N, HALF), 1) == 0, 1.0, 2.0)
            energy = weight * (real_part * real_part + imag_part * imag_part)
            stats_ref[0] += jnp.sum(energy.reshape(N // 8, 8, HALF), axis=0)
            stats_ref[1] += jnp.sum((ksquare * energy).reshape(N // 8, 8, HALF), axis=0)
            z_inverse(local, z_rows(real_part, imag_part, kz_wave), table_ref, whole_ref, deriv_ref)

    def leaving(k):
        part = pl.ds(k * CHUNK, CHUNK)
        return copy_of(planes_ref.at[part], out_hbm.at[part], out_sems.at[k])

    def one_chunk(k, carry):
        send_planes(k * CHUNK, CHUNK, UNROLL, planes_ref, whole_ref, deriv_ref)
        leaving(k).start()
        return carry

    lax.fori_loop(0, PEERS // CHUNK, one_chunk, 0)
    for k in range(PEERS // CHUNK):
        leaving(k).wait()


def in_three(value):
    high = value.astype(BF16).astype(F32)
    rest = value - high
    middle = rest.astype(BF16).astype(F32)
    return high, middle, (rest - middle).astype(BF16).astype(F32)


def place_of(row):
    return row * KEPT // HALF, row * KEPT % HALF


def packed(parts):
    lane = iota((2 * ROWS, HALF), 1)
    blocks = [None] * (BLOCKS + 1)
    for row, part in enumerate(parts):
        block, shift = place_of(row)
        turned = pltpu.roll(part, shift, 1) if shift else part
        blocks[block] = turned if shift == 0 else jnp.where(lane < shift, blocks[block], turned)
        if shift + KEPT > HALF:
            blocks[block + 1] = turned
    real_part, imag_part = blocks[BLOCKS][:ROWS], blocks[BLOCKS][ROWS:]
    blocks[BLOCKS] = jnp.where(lane[:ROWS] < HALF // 2, real_part, pltpu.roll(imag_part, HALF // 2, 1))
    return blocks


def unpacked(blocks):
    lane = iota(blocks[0].shape, 1)
    parts = []
    for row in range(ROWS):
        block, shift = place_of(row)
        part = blocks[block]
        if shift + KEPT > HALF:
            part = jnp.where(lane >= shift, part, blocks[block + 1])
        parts.append(pltpu.roll(part, HALF - shift, 1) if shift else part)
    return parts


def grid_kernel(scalars, planes_hbm, speed_ref, stats_ref, held, out_ref, passed, sums_ref, peak_ref, *apart):
    count = 2 * N
    if apart:
        planes_ref, planes_sems, sems = apart

        def came_plane(k):
            return copy_of(planes_hbm.at[:, k], planes_ref.at[:, k], planes_sems.at[k])

        loads = [copy_of(source, target, sems.at[k]) for k, (source, target) in enumerate(zip(held, passed))]
        loads[0].start()
        for k in range(PAIR):
            came_plane(k).start()
        for load in loads[1:4]:
            load.start()
        for k in range(PAIR, ROWS):
            came_plane(k).start()
        for load in loads[4:]:
            load.start()
        held = passed
    else:
        planes_ref = planes_hbm
    y_inv_ref, x_inv_ref, x_fwd_ref, y_fwd_ref = held[:4]
    peak_ref[...] = jnp.zeros_like(peak_ref)
    row = iota((count, HALF), 0)
    ky_wave = signed(row // (2 * ROWS) * ROWS + row % ROWS).astype(BF16)
    kx_wave = iota((HALF, HALF), 1).astype(F32)

    def one_pair(step):
        if apart:
            for k in range(PAIR):
                came_plane(step * PAIR + k).wait()
        if apart and step == 0:
            for load in loads[:4]:
                load.wait()
        came = [planes_ref[:, step * PAIR + k].reshape(count, N) for k in range(PAIR)]
        scaled = [ky_wave * part[:, :HALF] for part in came]
        pairs = both_turns(jnp.concatenate(came + scaled, axis=1))
        y_section = [dot(y_inv_ref[turn], pairs[turn]) for turn in (0, 1)]
        x_rows = []
        for k in range(PAIR):
            starts = (k * N, PAIR * N + k * HALF, k * N + HALF)
            for which, at in enumerate(starts):
                for found in y_section:
                    halves = [found[part * HALF : (part + 1) * HALF, at : at + HALF] for part in (0, 1)]
                    if which == 0:
                        halves = [kx_wave * half for half in halves]
                    x_rows.append(jnp.concatenate(halves, axis=1).astype(BF16))
        gradients = dot(jnp.concatenate(x_rows, axis=0), x_inv_ref[...])
        fields = []
        for k in range(PAIR):
            parts = [gradients[(3 * k + d) * N : (3 * k + d + 1) * N] for d in range(3)]
            total = speed_ref[0, step * PAIR + k].astype(F32) * parts[0]
            total = total + speed_ref[1, step * PAIR + k].astype(F32) * parts[1]
            total = total + speed_ref[2, step * PAIR + k].astype(F32) * parts[2]
            fields.append(total.astype(BF16))
            if apart:
                square = parts[0] * parts[0] + parts[1] * parts[1] + parts[2] * parts[2]
                peak_ref[...] = jnp.maximum(peak_ref[...], jnp.max(square.reshape(N // 8, 8, N), axis=0))
        x_section = dot(jnp.concatenate(fields, axis=0), x_fwd_ref[...]).astype(BF16)
        sums = []
        for turn in (0, 1):
            columns = []
            for k in range(PAIR):
                part = x_section[k * N + turn * HALF : k * N + (turn + 1) * HALF]
                columns.append(jnp.concatenate([part[:, :HALF], part[:, HALF:]], axis=0))
            sums.append(dot(y_fwd_ref[turn], jnp.concatenate(columns, axis=1)))
        for k in range(PAIR):
            even, odd = (found[:, k * HALF : (k + 1) * HALF] for found in sums)
            sums_ref[pl.ds(row_of(step * PAIR + k), N), :] = even + odd
            sums_ref[pl.ds(row_of(step * PAIR + k, N), N), :] = even - odd

    for step in range(ROWS // PAIR):
        one_pair(step)
    if apart:
        shape = (2 * ROWS, HALF)
        peak = jnp.sqrt(jnp.max(peak_ref[...], keepdims=True))
        pieces = []
        for value in (jnp.sum(stats_ref[0], keepdims=True), jnp.sum(stats_ref[1], keepdims=True), peak):
            pieces.extend(in_three(jnp.broadcast_to(value, shape)))
        line = jnp.zeros(shape, F32)
        for k, piece in enumerate(pieces):
            line = jnp.where((iota(shape, 0) == k) & (iota(shape, 1) == LIMIT), piece, line)

    def some_peers(step, carry):
        for turn in range(SENDS):
            peer = step * SENDS + turn
            parts = []
            for row in range(ROWS):
                start = peer * 2 * ROWS + row
                real_part = sums_ref[pl.ds(start, ROWS, stride=PITCH), :]
                imag_part = sums_ref[pl.ds(start + ROWS, ROWS, stride=PITCH), :]
                parts.append(jnp.concatenate([real_part, imag_part], axis=0))
            if apart:
                parts[0] = parts[0] + line
            for k, block in enumerate(packed(parts)):
                at = 2 * ROWS * k
                out_ref[peer, at : at + block.shape[0], :] = block.astype(BF16)
        return carry

    lax.fori_loop(0, PEERS // SENDS, some_peers, 0)
    if apart:
        for load in loads[4:]:
            load.wait()


def tendency(came_ref, table_ref):
    count = 2 * ROWS
    blocks = [came_ref[:, k * count : (k + 1) * count, :] for k in range(BLOCKS)]
    last = came_ref[:, BLOCKS * count :, :].astype(F32)
    blocks.append(jnp.concatenate([last, pltpu.roll(last, HALF // 2, 2)], axis=1).astype(BF16))
    sums = dot(table_ref[...], jnp.concatenate([block.reshape(2 * N, HALF) for block in blocks], axis=1))
    parts = unpacked([sums[:, k * HALF : (k + 1) * HALF] for k in range(BLOCKS + 1)])
    between = jnp.zeros((N - 2 * KEPT, HALF), F32)
    cut = [[part[k * KEPT : (k + 1) * KEPT] for k in range(4)] for part in parts]
    return [tuple(jnp.concatenate([c[k], between, c[k + 1]], axis=0) for k in (0, 2)) for c in cut]


def middle_kernel(
    bound_ref,
    species_ref,
    base_ref,
    came_ref,
    state_ref,
    z_fwd_ref,
    z_inv_ref,
    out_ref,
    kept_ref,
    kappa_ref,
    whole_ref,
    deriv_ref,
):
    shape = (PEERS, 2 * ROWS, HALF)
    found = jnp.where(iota(shape, 2) == LIMIT, came_ref[:, : 2 * ROWS, :].astype(F32), 0.0)
    piece_row = iota(shape, 1)

    def piece(which):
        inside = jnp.where((piece_row >= 3 * which) & (piece_row < 3 * which + 3), found, 0.0)
        return jnp.sum(jnp.sum(inside, axis=1), axis=1, keepdims=True)

    def spread(value):
        return jnp.broadcast_to(value, (8, HALF))

    variance = spread(jnp.sum(piece(0), axis=0, keepdims=True)) / CELLS
    mean_grad = spread(jnp.sum(piece(1), axis=0, keepdims=True)) / CELLS
    peak = spread(jnp.max(piece(2), axis=0, keepdims=True))
    base = base_ref[species_ref[0]]
    found = base * peak * jnp.sqrt(variance) / (mean_grad + 1e-06)
    kappa_ref[0] = jnp.max(found)
    kappa = found[0:1, :]
    bound = (bound_ref[0] * bound_ref[0]).astype(F32)
    kz_wave = signed(iota((N, HALF), 0))
    along_z = jnp.exp(-kappa * (kz_wave * kz_wave) * STEP)
    for local, sums in enumerate(tendency(came_ref, z_fwd_ref)):
        _, ksquare = waves_of(local)
        factor = along_z * jnp.exp(-kappa * across_z(local) * STEP)
        scaled = STEP * factor
        inside = ksquare <= bound
        middle = []
        for part in (0, 1):
            start = factor * state_ref[part, local]
            change = jnp.where(inside, scaled * sums[part], 0.0)
            middle.append(start - change)
            kept_ref[part, local] = start - 0.5 * change
        z_inverse(local, z_rows(*middle, kz_wave), z_inv_ref, whole_ref, deriv_ref)
    send_planes(0, PEERS, PEERS, out_ref, whole_ref, deriv_ref)


def final_kernel(bound_ref, came_ref, kept_ref, z_fwd_ref, out_hbm, out_ref, out_sems):
    bound = (bound_ref[0] * bound_ref[0]).astype(F32)
    bands = (slice(0, KEPT), slice(N - KEPT, N))
    between = slice(KEPT, N - KEPT)
    saves = [copy_of(kept_ref.at[:, :, between], out_hbm.at[:, :, between], out_sems.at[0])]
    saves[0].start()
    for local, sums in enumerate(tendency(came_ref, z_fwd_ref)):
        _, ksquare = waves_of(local)
        for band in bands:
            for part in (0, 1):
                change = jnp.where(ksquare[band] <= bound, (0.5 * STEP) * sums[part][band], 0.0)
                out_ref[part, local, band] = kept_ref[part, local, band] - change
            saves.append(copy_of(out_ref.at[:, local, band], out_hbm.at[:, local, band], out_sems.at[len(saves)]))
            saves[-1].start()
    for save in saves:
        save.wait()


SCALARS = pl.BlockSpec(memory_space=pltpu.SMEM)
NEAR = pl.BlockSpec(memory_space=pltpu.VMEM)
FAR = pl.BlockSpec(memory_space=pltpu.HBM)
PLANES = (PEERS, ROWS, 2 * ROWS, N)
SENT = (PEERS, 2 * ROWS * KEPT * ROWS // HALF, HALF)
STATE = (2, ROWS, N, HALF)
PAIR = 4
AT_ONCE = 4
CHUNK = 8
UNROLL = 4
SENDS = 32


def params(mebibytes):
    return pltpu.CompilerParams(vmem_limit_bytes=mebibytes * 2**20)


def shaped(shape, dtype):
    return jax.ShapeDtypeStruct(shape, dtype)


def near(x):
    return pltpu.with_memory_space_constraint(x, pltpu.VMEM)


def far(x):
    return pltpu.with_memory_space_constraint(x, pltpu.HBM)


def sems(count):
    return pltpu.SemaphoreType.DMA((count,))


def turned():
    return pltpu.VMEM((ROWS * PITCH, HALF), F32)


BIG = pltpu.VMEM((2, N, N), BF16)
HELD = pltpu.VMEM(STATE, F32)


def gathered(velocity):
    groups = lax.axis_size("scal")
    me = lax.axis_index("scal")
    ring = 4
    high, low = me // ring, me % ring
    planes, rows = velocity.shape[1], velocity.shape[2] // 2
    velocity = velocity.reshape(3, planes, rows, 2, N).swapaxes(2, 3)

    def moved(x, change):
        return lax.ppermute(x, "scal", [(s, change(s)) for s in range(groups)])

    def beside(shift):
        return lambda s: s // ring * ring + (s + shift) % ring

    across = moved(velocity, lambda s: (s + ring) % groups)
    out = jnp.zeros((3, planes, 2, HALF, N), velocity.dtype)
    half = planes // 2

    def placed(out, x, owner, first=0):
        return lax.dynamic_update_slice(out, x, (0, first, 0, owner * rows, 0))

    for x, own in ((velocity, high), (across, 1 - high)):
        up = moved(x, beside(1))
        down = moved(x, beside(-1))
        far_up = moved(up[:, :half], beside(1))
        far_down = moved(down[:, half:], beside(-1))
        start = own * ring
        out = placed(out, x, start + low)
        out = placed(out, up, start + (low + ring - 1) % ring)
        out = placed(out, down, start + (low + 1) % ring)
        out = placed(out, far_up, start + (low + 2) % ring)
        out = placed(out, far_down, start + (low + 2) % ring, half)
    return out.reshape(3, planes, N, N)


def exchanged(x):
    return lax.all_to_all(x, "fft", 0, 0, tiled=True)


def start_call(state, table):
    return pl.pallas_call(
        start_kernel,
        in_specs=[FAR, FAR],
        out_specs=[FAR, NEAR],
        out_shape=[pltpu.HBM(PLANES, BF16), pltpu.VMEM((2, 8, HALF), F32)],
        scratch_shapes=[HELD, BIG, pltpu.VMEM(PLANES, BF16), turned(), turned(), sems(ROWS + 1), sems(PEERS // CHUNK)],
        compiler_params=params(24),
        name="start",
    )(far(state), far(table["z_inv"]))


def grid_call(scalars, planes, speeds, stats, held, apart):
    scratch = [turned(), pltpu.VMEM((8, N), F32)]
    passed = held if apart else ()
    if apart:
        scratch += [pltpu.VMEM(PLANES, BF16), sems(ROWS), sems(len(held))]
    spec, place = (FAR, far) if apart else (NEAR, near)
    return pl.pallas_call(
        grid_kernel,
        in_specs=[(SCALARS,) * len(scalars), spec, NEAR, NEAR, (spec,) * len(held)],
        out_specs=[NEAR, (NEAR,) * len(passed)],
        out_shape=[pltpu.VMEM(SENT, BF16), tuple(pltpu.VMEM(x.shape, x.dtype) for x in passed)],
        scratch_shapes=scratch,
        compiler_params=params(24),
        name="grid",
    )(scalars, place(planes), near(speeds), near(stats), tuple(place(x) for x in held))


def middle_call(scalars, came, state, z_fwd, z_inv):
    return pl.pallas_call(
        middle_kernel,
        in_specs=[SCALARS] * 3 + [NEAR] * 4,
        out_specs=[NEAR, NEAR, SCALARS],
        out_shape=[pltpu.VMEM(PLANES, BF16), pltpu.VMEM(STATE, F32), shaped((1,), F32)],
        scratch_shapes=[turned(), turned()],
        compiler_params=params(24),
        name="middle",
    )(*scalars, *(near(x) for x in (came, state, z_fwd, z_inv)))


def final_call(bound, came, kept, z_fwd):
    return pl.pallas_call(
        final_kernel,
        in_specs=[SCALARS, NEAR, NEAR, NEAR],
        out_specs=FAR,
        out_shape=pltpu.HBM(STATE, F32),
        scratch_shapes=[HELD, sems(2 * ROWS + 1)],
        compiler_params=params(24),
        name="final",
    )(bound, near(came), near(kept), near(z_fwd))


def body(scalar_state, velocity, species, kappa_table, dealias_bound):
    table = tables()
    state = scalar_state[0]
    speeds = gathered(velocity)
    planes, stats = start_call(state, table)
    scalars = (dealias_bound, species, kappa_table)
    held = tuple(table[name] for name in ("y_inv", "x_inv", "x_fwd", "y_fwd", "z_fwd", "z_inv")) + (state,)
    sent, held = grid_call(scalars, exchanged(planes), speeds, stats, held, True)
    *grid_tables, z_fwd, z_inv, state = held
    planes, kept, kappa = middle_call(scalars, exchanged(sent), state, z_fwd, z_inv)
    sent, _ = grid_call((), exchanged(planes), speeds, stats, tuple(grid_tables), False)
    return (final_call(dealias_bound, exchanged(sent), kept, z_fwd)[None], kappa)


def solution(mesh):
    placed = (
        P("scal", None, "fft", None, None),
        P(None, "fft", "scal", None),
        P("scal"),
        P(),
        P("scal"),
    )
    return jax.shard_map(
        body,
        mesh=mesh,
        in_specs=placed,
        out_specs=(P("scal", None, "fft", None, None), P("scal")),
        check_vma=False,
    )
```
